256 devices in a mesh: batch: 32 (over x, z_hi, core), hidden: 8 (over z_lo, y).
Axes of the slice: x: 4, y: 4, z: 8 (z_hi: 4, z_lo: 2; z = z_hi * 2 + z_lo), core: 2. Of those that a mesh axis runs over, the one named last changes fastest.
Arguments:
- features: bfloat16 [12288, 512], P('batch'), may hold values from -6 to 6
- w_first: bfloat16 [512, 8192], P('batch', 'hidden'), may hold values from -0.25 to 0.25
- w_second: bfloat16 [8192, 4096], P('hidden', 'batch'), may hold values from -0.0625 to 0.0625
- w_head: bfloat16 [4096, 8], P('hidden'), may hold values from -0.09375 to 0.09375
- rewards: float32 [8, 12288], P(None, 'batch'), may hold values from -1.75 to 1.75
- discount: float32 [8], replicated, as said below
- trace: float32 [8], replicated, as said below
- episode: int32 [12288], P('batch'), may hold values from 0 to 32, as said below
Outputs:
- advantages: float32 [8, 12288], P(None, 'batch')
- loss: float32 [], replicated
- grad_first: float32 [512, 8192], P('batch', 'hidden')
- grad_second: float32 [8192, 4096], P('hidden', 'batch')
- grad_head: float32 [4096, 8], P('hidden')
The draws below stay inside these ranges and needn't reach their ends.
Inputs may be any that keep to these rules, and one draw needn't show every extreme that they name: Each discount lies between 0.875 and 1. Each trace factor lies between 0.875 and 1. episode numbers never fall along the rollout and rise by one at each episode start; each block of 384 timesteps of one index of batch holds exactly one episode start besides the rollout's own start at timestep 0, and that start never falls on the block's first timestep; the rollout begins with episode 0.
All inputs are finite; a program needn't handle non-finite values.
Results may differ from the reference program's by a relative error of at most 0.018.
Values may be sent and summed in bfloat16 or wider, within the bound.
A program may use at most 128 MiB of HBM per device.

```python
import jax
import jax.numpy as jnp
from jax import lax

D_IN = 512
H = 8192
HW = 4096
NH = 8
TOK_DEV = 384
TIMESTEPS = 12288
N_BATCH = 32


def horizon_factor(key):
    lowest = jnp.log(8.0)
    highest = jnp.log(8.0 * TOK_DEV)
    spread = jax.random.uniform(key, (NH,), jnp.float32)
    horizon = jnp.exp(lowest + spread * (highest - lowest))
    return 1.0 - 1.0 / horizon


def draw_discount(key, part):
    return horizon_factor(jax.random.fold_in(key, 11))


def draw_trace(key, part):
    return horizon_factor(jax.random.fold_in(key, 23))


def draw_episode(key, part):
    blocks = TIMESTEPS // TOK_DEV
    offsets = jax.random.randint(jax.random.fold_in(key, 37), (blocks,), 1, TOK_DEV).astype(jnp.int32)
    steps = jnp.arange(TIMESTEPS, dtype=jnp.int32)
    owner = steps // TOK_DEV
    within = steps % TOK_DEV
    return (owner + (within >= offsets[owner]).astype(jnp.int32)).astype(jnp.int32)


def block_scale(own_key, shape, pieces, smallest, high):
    gain, own = 1.0, jax.random.fold_in(own_key, 6)
    for position, parts in pieces:
        draws = jnp.exp(jax.random.uniform(jax.random.fold_in(own, position), (parts,), jnp.float32, smallest / len(pieces), high / len(pieces)))
        gain = gain * jnp.repeat(draws, shape[position] // parts).reshape([-1 if axis == position else 1 for axis in range(len(shape))])
    return gain


def scatter_about(rng, shape, scale, limit, split=(), kind=jnp.bfloat16):
    values = jax.random.normal(rng, shape, jnp.float32) * scale
    if len(split) > 0:
        values = block_scale(rng, shape, split, -0.22, 0.18) * values
    return jnp.clip(values, min=-limit, max=limit).astype(kind)


def setup_inputs(seed: int = 0) -> dict:
    streams_of = jax.random.split(jax.random.key(seed), 9)
    return {
        "features": scatter_about(streams_of[0], (TIMESTEPS, D_IN), 1.0, 6.0, ((0, 32),)),
        "w_first": scatter_about(streams_of[1], (D_IN, H), D_IN ** -0.5, 0.25, ((0, 32), (1, 8))),
        "w_second": scatter_about(streams_of[2], (H, HW), H ** -0.5, 0.0625, ((0, 8), (1, 32))),
        "w_head": scatter_about(streams_of[3], (HW, NH), HW ** -0.5, 0.09375, ((0, 8),)),
        "rewards": scatter_about(streams_of[4], (NH, TIMESTEPS), 0.3, 1.75, ((1, 32),), jnp.float32),
        "discount": draw_discount(jax.random.fold_in(streams_of[8], 71), 0),
        "trace": draw_trace(jax.random.fold_in(streams_of[8], 71), 0),
        "episode": draw_episode(jax.random.fold_in(streams_of[8], 71), 0),
    }


def chain_maps(farther, nearer):
    return (farther[0] * nearer[0], nearer[1] + nearer[0] * farther[1])


def silu_slope(value):
    sigmoid_value = jax.nn.sigmoid(value)
    return sigmoid_value * (1.0 + value * (1.0 - sigmoid_value))


def widen(array):
    return array.astype(jnp.float32)


def reference(features, w_first, w_second, w_head, rewards, discount, trace, episode):
    highest = lax.Precision.HIGHEST
    pre_first = jnp.dot(widen(features), widen(w_first), precision=highest)
    hidden_first = jax.nn.silu(pre_first).astype(jnp.bfloat16)
    pre_second = jnp.dot(widen(hidden_first), widen(w_second), precision=highest)
    hidden_second = jax.nn.silu(pre_second).astype(jnp.bfloat16)
    values = jnp.dot(widen(hidden_second), widen(w_head), precision=highest)
    values_t = values.T
    heads = values_t.shape[0]
    steps_all = values_t.shape[1]
    following = jnp.concatenate([episode[1:], jnp.full((1,), -1, jnp.int32)])
    keep = (following == episode).astype(jnp.float32)
    value_after = jnp.concatenate([values_t[:, 1:], jnp.zeros((heads, 1), jnp.float32)], axis=1)
    delta = rewards + discount[:, None] * keep[None, :] * value_after - values_t
    factor = discount[:, None] * trace[:, None] * keep[None, :]
    _, advantages = lax.associative_scan(chain_maps, (factor, delta), reverse=True, axis=1)
    loss = 0.5 * jnp.sum(advantages * advantages) / (steps_all * heads)
    slope_value = (-advantages.T).astype(jnp.bfloat16)
    slope_second = (jnp.dot(widen(slope_value), widen(w_head).T, precision=highest) * silu_slope(pre_second)).astype(jnp.bfloat16)
    slope_first = (jnp.dot(widen(slope_second), widen(w_second).T, precision=highest) * silu_slope(pre_first)).astype(jnp.bfloat16)
    grad_head = jnp.dot(widen(hidden_second).T, widen(slope_value), precision=highest)

    def accumulate(carry, block):
        feat_block, first_block, hidden_block, second_block = block
        part_first = jnp.dot(widen(feat_block).T, widen(first_block), precision=highest).astype(jnp.bfloat16)
        part_second = jnp.dot(widen(hidden_block).T, widen(second_block), precision=highest).astype(jnp.bfloat16)
        part_first, part_second = lax.optimization_barrier((part_first, part_second))
        return (carry[0] + widen(part_first), carry[1] + widen(part_second)), None

    blocks = (features.reshape(N_BATCH, TOK_DEV, -1), slope_first.reshape(N_BATCH, TOK_DEV, -1),
              hidden_first.reshape(N_BATCH, TOK_DEV, -1), slope_second.reshape(N_BATCH, TOK_DEV, -1))
    start_sums = (jnp.zeros((features.shape[1], w_first.shape[1]), jnp.float32),
                  jnp.zeros((w_second.shape[0], w_second.shape[1]), jnp.float32))
    (grad_first, grad_second), _ = lax.scan(accumulate, start_sums, blocks)
    return advantages, loss, grad_first, grad_second, grad_head
```

```python
import functools

import jax
import jax.numpy as jnp
from jax import lax
from jax.experimental import pallas as pl
from jax.experimental.pallas import tpu as pltpu
from jax.sharding import PartitionSpec as P

BF16, F32 = jnp.bfloat16, jnp.float32
MESH = pl.DeviceIdType.MESH
SLOTS = 240
LOW, HIGH = pl.ds(0, 512), pl.ds(512, 512)


def dot(left, right, dims=((1,), (0,))):
    return lax.dot_general(left, right, (dims, ((), ())), preferred_element_type=F32)


def mod(value, count):
    return lax.rem(value + count, count)


def lane(dx):
    return pl.ds(dx * 128, 128)


class Links:
    def __init__(self, sent, came):
        self.sent, self.came, self.used, self.open = sent, came, 0, []

    def take(self):
        self.used += 1
        return self.used - 1

    def make(self, src, dst, to, k, k_came=None):
        return pltpu.make_async_remote_copy(
            src_ref=src,
            dst_ref=dst,
            send_sem=self.sent.at[k],
            recv_sem=self.came.at[k if k_came is None else k_came],
            device_id=to,
            device_id_type=MESH,
        )

    def push(self, src, dst, to, land=None):
        k = self.take()
        copy = self.make(src, dst, to, k)
        copy.start()
        self.open.append(copy)
        return copy if land is None else self.make(land, land, to, k)

    def drain(self):
        for copy in self.open:
            copy.wait_send()
        self.open = []


def kernel(
    feat, w1in, w2in, whin, rein, dt,
    adv_o, loss_o, g1_o, g2_o, gh_o,
    F, FT, W1, W2, WHB, WH, RE, HF, HFT, SP, PS, RA, RB, RL, RR, RZ, PRE, SL2, H2,
    V, ADV, S, BACK, G2, XA, XB, XL, XR, ZA, ZB, ZL, ZR, BKS, BKR, SF,
    G1, YA, YB, YL, YR, UA, UB, UL, UR, GF, GT, GHP, GR, GS, GZ, GX, GY, GC, GH,
    sent, came,
):
    b, j = lax.axis_index("batch"), lax.axis_index("hidden")
    c, m = lax.rem(b, 2), lax.div(b, 2)
    zh, x = lax.rem(m, 4), lax.div(m, 4)
    y, zl = lax.rem(j, 4), lax.div(j, 4)
    r = y * 2 + zl
    link = Links(sent, came)
    push = link.push

    def at(dx=0, dz=0, dc=0, dy=0, dl=0):
        bb = (mod(x + dx, 4) * 4 + mod(zh + dz, 4)) * 2 + mod(c + dc, 2)
        return bb, mod(zl + dl, 2) * 4 + mod(y + dy, 4)

    def beside(step, dc, dy, dl):
        bb = mod(m + step, 16) * 2 + mod(c + dc, 2)
        return bb, mod(zl + dl, 2) * 4 + mod(y + dy, 4)

    peers = [(dc, dy, dl) for dc in range(2) for dy in range(4) for dl in range(2)]

    F[c] = feat[...]
    W1[x, zh, c] = w1in[...]
    W2[0, :, lane(0)] = w2in[...]
    WHB[j] = whin[...]
    RE[c] = rein[...]

    barrier = pltpu.get_barrier_semaphore()
    partners = [at(dc=dc, dy=dy, dl=dl) for dc, dy, dl in peers[1:]]
    partners += [at(dx=d) for d in (1, 2, 3)] + [at(dz=d) for d in (1, 2, 3)]
    partners += [beside(step, *peer) for step in (1, -1) for peer in peers]
    for partner in partners:
        pl.semaphore_signal(barrier, inc=1, device_id=partner, device_id_type=MESH)
    pl.semaphore_wait(barrier, len(partners))

    w1z = {
        dz: push(w1in, W1.at[x, zh, c], at(dz=dz), W1.at[x, mod(zh - dz, 4), c])
        for dz in (1, 3, 2)
    }

    def w1_sides(zs):
        own = W1.at[x, zs, c]
        return [
            push(own, own, at(dx=dx), W1.at[mod(x - dx, 4), zs, c]) for dx in (1, 3)
        ]

    def w1_across(zs, sides):
        out = []
        for dx, half, side in ((1, LOW, sides[0]), (3, HIGH, sides[1])):
            side.wait_recv()
            part = W1.at[mod(x - dx, 4), zs, c, :, half]
            out.append(push(part, part, at(dx=dx), W1.at[mod(x + 2, 4), zs, c, :, half]))
        return out

    w1x = {0: w1_sides(zh)}
    feat_in = push(feat, F.at[c], at(dc=1), F.at[1 - c])
    first = [
        push(w2in.at[LOW], W2.at[3, LOW, lane(0)], at(dz=1)),
        push(w2in.at[HIGH], W2.at[1, HIGH, lane(0)], at(dz=3)),
    ]
    w2x = {}

    def w2_side(dz, half):
        src = W2.at[dz, half, lane(0)]
        right = lambda: push(src, W2.at[dz, half, lane(3)], at(dx=1))
        left = lambda: push(src, W2.at[dz, half, lane(1)], at(dx=3))
        if half is LOW:
            w2x[dz, 3, 0] = right()
            w2x[dz, 1, 0] = left()
        else:
            w2x[dz, 1, 1] = left()
            w2x[dz, 3, 1] = right()

    def w2_across(dz):
        w2x[dz, 3, 0].wait_recv()
        w2x[dz, 2, 0] = push(
            W2.at[dz, LOW, lane(3)], W2.at[dz, LOW, lane(2)], at(dx=1)
        )
        w2x[dz, 1, 1].wait_recv()
        w2x[dz, 2, 1] = push(
            W2.at[dz, HIGH, lane(1)], W2.at[dz, HIGH, lane(2)], at(dx=3)
        )

    def w2_rest(dz):
        for key in ((3, 1), (1, 0), (2, 0), (2, 1)):
            w2x[(dz, *key)].wait_recv()

    second = [
        push(w2in.at[HIGH], W2.at[3, HIGH, lane(0)], at(dz=1)),
        push(w2in.at[LOW], W2.at[1, LOW, lane(0)], at(dz=3)),
    ]
    for dz in (1, 3, 2):
        w1z[dz].wait_recv()
        w1x[dz] = w1_sides(mod(zh - dz, 4))
    w2_side(0, LOW)
    w2_side(0, HIGH)
    re_in = push(rein, RE.at[c], at(dc=1), RE.at[1 - c])
    re_sem = [link.take() for _ in range(2)]
    re_to = [
        link.make(rein, RE.at[2], beside(-1, dc, 0, 0), re_sem[dc], re_sem[0])
        for dc in range(2)
    ]

    @pl.when(c == 0)
    def _():
        for copy in re_to:
            copy.start()

    wh_in = [
        push(whin, WHB.at[j], at(dy=dy, dl=dl), WHB.at[mod(zl - dl, 2) * 4 + mod(y - dy, 4)])
        for dc, dy, dl in peers[1:8]
    ]

    w1far = {0: w1_across(zh, w1x[0])}
    for dz in (1, 3, 2):
        w1far[dz] = w1_across(mod(zh - dz, 4), w1x[dz])
    w2_across(0)
    w1core = []
    for dz in (0, 1, 3, 2):
        for copy in w1far[dz]:
            copy.wait_recv()
        zs = mod(zh - dz, 4)
        w1core.append(
            push(W1.at[:, zs, c], W1.at[:, zs, c], at(dc=1), W1.at[:, zs, 1 - c])
        )
    first[0].wait_recv()
    w2_z2 = [push(W2.at[3, LOW, lane(0)], W2.at[2, LOW, lane(0)], at(dz=1))]
    w2_side(3, LOW)
    first[1].wait_recv()
    w2_z2.append(push(W2.at[1, HIGH, lane(0)], W2.at[2, HIGH, lane(0)], at(dz=3)))
    w2_side(1, HIGH)

    feat_in.wait_recv()
    for copy in w1core:
        copy.wait_recv()

    @pl.loop(0, 4)
    def _(n):
        cols = pl.ds(pl.multiple_of(n * 256, 256), 256)
        weights = W1[:, :, :, :, cols].reshape(512, 256)
        SP[:, cols] = dot(F[...].reshape(768, 512), weights)

        @pl.loop(0, 12)
        def _(i):
            rows = pl.ds(pl.multiple_of(i * 64, 64), 64)
            value = SP[rows, cols]
            gate = 1.0 / (1.0 + jnp.exp(-value))
            HF[rows, cols] = (value * gate).astype(BF16)
            SP[rows, cols] = gate * (1.0 + value * (1.0 - gate))

    def product(dz):
        @pl.loop(0, 2)
        def _(n):
            start = pl.multiple_of(n * 256, 256)
            part = dot(HF[...], W2[dz, :, pl.ds(start, 256)])
            into = pl.ds(pl.multiple_of(dz * 512 + n * 256, 256), 256)
            PS[:, :, into] = part.astype(BF16).reshape(8, 96, 256)

    up, down, over = mod(y + 1, 4), mod(y - 1, 4), mod(y + 2, 4)
    came_rs = {}

    def scatter_a(dz):
        at_dz = pl.ds(dz * 512, 512)
        came_rs[dz] = [
            push(PS.at[over * 2, :, at_dz], RA.at[dz], at(dy=1)),
            push(PS.at[over * 2 + 1, :, at_dz], RB.at[dz], at(dy=3)),
            push(PS.at[up * 2 + 1, :, at_dz], RL.at[dz, 1], at(dy=1)),
            push(PS.at[down * 2, :, at_dz], RR.at[dz, 0], at(dy=3)),
        ]

    def scatter_b(dz):
        at_dz = pl.ds(dz * 512, 512)
        for got, buf, row, dst, dy in (
            (came_rs[dz][0], RA, up * 2, RL.at[dz, 0], 1),
            (came_rs[dz][1], RB, down * 2 + 1, RR.at[dz, 1], 3),
        ):
            got.wait_recv()
            total = PS[row, :, at_dz].astype(F32) + buf[dz].astype(F32)
            PS[row, :, at_dz] = total.astype(BF16)
            came_rs[dz].append(push(PS.at[row, :, at_dz], dst, at(dy=dy)))

    def scatter_c(dz):
        at_dz = pl.ds(dz * 512, 512)
        for got in came_rs[dz][2:]:
            got.wait_recv()

        def total(side):
            return (
                PS[y * 2 + side, :, at_dz].astype(F32)
                + RL[dz, side].astype(F32)
                + RR[dz, side].astype(F32)
            )

        PS[y * 2 + 1 - zl, :, at_dz] = total(1 - zl).astype(BF16)
        came_rs[dz].append(
            push(PS.at[y * 2 + 1 - zl, :, at_dz], RZ.at[dz], at(dl=1))
        )
        PRE[:, at_dz] = total(zl)

    def scatter_d(dz):
        at_dz = pl.ds(dz * 512, 512)
        came_rs[dz][-1].wait_recv()

        @pl.loop(0, 3)
        def _(i):
            rows = pl.ds(pl.multiple_of(i * 32, 32), 32)
            value = PRE[rows, at_dz] + RZ[dz, rows, :].astype(F32)
            gate = 1.0 / (1.0 + jnp.exp(-value))
            H2[rows, at_dz] = (value * gate).astype(BF16)
            SL2[rows, at_dz] = gate * (1.0 + value * (1.0 - gate))

    w2_rest(0)
    product(0)
    scatter_a(0)
    second[0].wait_recv()
    w2_side(3, HIGH)
    second[1].wait_recv()
    w2_side(1, LOW)
    w2_across(3)
    w2_across(1)
    scatter_b(0)
    w2_z2[0].wait_recv()
    w2_side(2, LOW)
    w2_z2[1].wait_recv()
    w2_side(2, HIGH)

    @pl.loop(0, 4)
    def _(n):
        cols = pl.ds(pl.multiple_of(n * 256, 256), 256)
        HFT[cols, :] = HF[:, cols].astype(F32).T.astype(BF16)

    w2_rest(3)
    product(3)
    scatter_a(3)
    scatter_c(0)

    @pl.loop(0, 2)
    def _(n):
        cols = pl.ds(pl.multiple_of(n * 256, 256), 256)
        FT[cols, :] = F[:, :, cols].reshape(768, 256).astype(F32).T.astype(BF16)

    for copy in wh_in:
        copy.wait_recv()
    for dz in range(4):
        for dx in range(4):
            mm = mod(x + dx, 4) * 4 + mod(zh + dz, 4)
            group, pair = lax.div(mm, 2), lax.rem(mm, 2)
            even, odd = (
                jnp.where(c == 0, WHB[group, :, lane(2 * p)], WHB[group, :, lane(2 * p + 1)])
                for p in (0, 1)
            )
            WH[:, lane(dz * 4 + dx)] = jnp.where(pair == 0, even, odd).astype(BF16)

    scatter_b(3)
    w2_rest(1)
    product(1)
    scatter_a(1)
    w2_across(2)
    scatter_d(0)
    scatter_c(3)
    scatter_b(1)
    scatter_d(3)
    scatter_c(1)
    w2_rest(2)
    product(2)
    scatter_a(2)
    scatter_d(1)
    scatter_b(2)
    scatter_c(2)
    scatter_d(2)

    wide = jnp.zeros((8, 32), F32)
    own_values = dot(WH[...], H2[...], ((1,), (1,)))
    V[c, r] = jnp.concatenate([own_values, wide], axis=1)
    v_in = []
    for dc, dy, dl in peers[1:]:
        src_r = mod(y - dy, 4) * 2 + mod(zl - dl, 2)
        v_in.append(
            push(V.at[c, r], V.at[c, r], at(dc=dc, dy=dy, dl=dl), V.at[mod(c - dc, 2), src_r])
        )
    v_out, v_next = [], []
    for dc, dy, dl in peers:
        k = link.take()
        src_r = mod(y - dy, 4) * 2 + mod(zl - dl, 2)
        v_out.append(
            link.make(V.at[c, r], V.at[c, 8 + lax.rem(r, 4)], beside(-1, dc, dy, dl), k)
        )
        land = V.at[mod(c - dc, 2), 8 + lax.rem(src_r, 4)]
        v_next.append((src_r, link.make(land, land, beside(-1, dc, dy, dl), k)))

    @pl.when(r < 4)
    def _():
        for copy in v_out:
            copy.start()

    re_in.wait_recv()
    link.make(RE.at[2], RE.at[2], at(dc=1), re_sem[0], re_sem[0]).wait_recv()
    shape = (8, 12 * 128)
    place = lax.rem(lax.broadcasted_iota(jnp.int32, shape, 1), 128)

    def ahead(array, steps):
        return pltpu.roll(array, shape[1] - steps, 1)

    def following(array):
        return jnp.where(place == 95, ahead(array, 33), ahead(array, 1))

    def row_of(kind):
        return jnp.concatenate([RE[i // 4, kind, i % 4] for i in range(12)], axis=1)

    reward, number = row_of(0), row_of(1)
    discount = jnp.concatenate([dt[0]] * 12, axis=1)
    both = jnp.concatenate([dt[0] * dt[1]] * 12, axis=1)
    keep = jnp.where(following(number) == number, 1.0, 0.0)
    real = place < 96
    factor = jnp.where(real, both * keep, 1.0)
    scale = discount * keep

    for copy in v_in:
        copy.wait_recv()
    for src_r, copy in v_next:

        @pl.when(src_r < 4)
        def _():
            copy.wait_recv()

    value = jnp.concatenate([V[0, i] + V[1, i] for i in range(12)], axis=1)
    total = jnp.where(real, reward + scale * following(value) - value, 0.0)
    step = 1
    while step < shape[1]:
        total = total + factor * ahead(total, step)
        factor = factor * ahead(factor, step)
        step *= 2
    for i in range(12):
        ADV[i] = total[:, i * 128 : (i + 1) * 128]

    own = ADV[r]
    slope_t = (-own[:, :96]).astype(BF16)
    slope = (-own).T[:96, :].astype(BF16)
    own_rows = S.at[r]

    def slope_chunk(dz):
        at_dz = pl.ds(dz * 512, 512)
        own_rows[:, at_dz] = (dot(slope, WH[:, at_dz]) * SL2[:, at_dz]).astype(BF16)

    ag = {}
    pair_r = y * 2 + 1 - zl

    def gather_a(dz):
        at_dz = pl.ds(dz * 512, 512)
        src = S.at[r, :, at_dz]
        ag[dz] = {
            "pair": push(src, src, at(dl=1), S.at[pair_r, :, at_dz]),
            "down": push(src, src, at(dy=1), S.at[down * 2 + zl, :, at_dz]),
            "up": push(src, src, at(dy=3), S.at[up * 2 + zl, :, at_dz]),
        }

    def gather_b(dz):
        at_dz = pl.ds(dz * 512, 512)
        ag[dz]["pair"].wait_recv()
        src = S.at[pair_r, :, at_dz]
        ag[dz]["down2"] = push(src, src, at(dy=1), S.at[down * 2 + 1 - zl, :, at_dz])
        ag[dz]["up2"] = push(src, src, at(dy=3), S.at[up * 2 + 1 - zl, :, at_dz])

    def gather_c(dz):
        at_dz = pl.ds(dz * 512, 512)
        for name in ("down", "up", "down2", "up2"):
            ag[dz][name].wait_recv()
        low, high = S.at[down * 2, :, at_dz], S.at[up * 2 + 1, :, at_dz]
        ag[dz]["far"] = [
            push(low, low, at(dy=1), S.at[over * 2, :, at_dz]),
            push(high, high, at(dy=3), S.at[over * 2 + 1, :, at_dz]),
        ]

    def gather_d(dz):
        for got in ag[dz]["far"]:
            got.wait_recv()

    def grad_second(dz):
        at_dz = pl.ds(dz * 512, 512)

        @pl.loop(0, 4)
        def _(n):
            rows = pl.ds(pl.multiple_of(n * 256, 256), 256)
            G2[dz, rows, :] = dot(HFT[rows, :], S[:, :, at_dz].reshape(768, 512)).astype(BF16)

    def back_first(dz, start):
        at_dz = pl.ds(dz * 512, 512)

        @pl.loop(0, 4)
        def _(n):
            cols = pl.ds(pl.multiple_of(n * 256, 256), 256)
            part = dot(S[:, :, at_dz].reshape(768, 512), W2[dz, cols, :], ((1,), (1,)))
            BACK[:, cols] = part if start else BACK[:, cols] + part

    gx = {}

    def reduce_a(dz):
        gx[dz] = [
            push(G2.at[dz, LOW, lane(2)], XA.at[dz], at(dx=1)),
            push(G2.at[dz, HIGH, lane(2)], XB.at[dz], at(dx=3)),
            push(G2.at[dz, HIGH, lane(1)], XL.at[dz, 1], at(dx=1)),
            push(G2.at[dz, LOW, lane(3)], XR.at[dz, 0], at(dx=3)),
        ]

    def reduce_b(dz):
        for got, buf, half, dx, dst in (
            (gx[dz][0], XA, LOW, 1, XL.at[dz, 0]),
            (gx[dz][1], XB, HIGH, 3, XR.at[dz, 1]),
        ):
            got.wait_recv()
            block = G2[dz, half, lane(dx)].astype(F32) + buf[dz].astype(F32)
            G2[dz, half, lane(dx)] = block.astype(BF16)
            gx[dz].append(push(G2.at[dz, half, lane(dx)], dst, at(dx=dx)))

    def reduce_c(dz, into=None):
        for got in gx[dz][2:]:
            got.wait_recv()
        for side, half in ((0, LOW), (1, HIGH)):
            block = (
                G2[dz, half, lane(0)].astype(F32)
                + XL[dz, side].astype(F32)
                + XR[dz, side].astype(F32)
            )
            if into is None:
                G2[dz, half, lane(0)] = block.astype(BF16)
            else:
                into[half, :] = block

    slope_chunk(2)
    gather_a(2)
    slope_chunk(1)
    gather_a(1)
    slope_chunk(3)
    slope_chunk(0)
    gather_b(2)

    for i in range(4):
        adv_o[i] = ADV[4 * c + i]
    small = lax.broadcasted_iota(jnp.int32, (8, 128), 1) < 96
    own_loss = jnp.where(small, own * own, 0.0)
    head = dot(slope_t, H2[...])
    for dz in range(4):
        for dx in range(4):
            mm = mod(x + dx, 4) * 4 + mod(zh + dz, 4)
            GHP[lax.div(mm, 2), lax.rem(mm, 2)] = head[:, (dz * 4 + dx) * 128 :][:, :128]
    for g in range(8):
        GHP[g, 2] = own_loss
    gather_c(2)
    gh_in = []
    for dc, dy, dl in peers[1:8]:
        to_j = mod(zl + dl, 2) * 4 + mod(y + dy, 4)
        from_j = mod(zl - dl, 2) * 4 + mod(y - dy, 4)
        gh_in.append(push(GHP.at[to_j], GR.at[j], at(dy=dy, dl=dl), GR.at[from_j]))
    GR[j] = GHP[j]
    gather_b(1)
    gather_a(3)
    gather_d(2)
    grad_second(2)
    reduce_a(2)
    gather_c(1)
    gather_b(3)
    back_first(2, True)
    gather_a(0)
    reduce_b(2)
    gather_d(1)
    grad_second(1)
    reduce_a(1)
    gather_c(3)
    gather_b(0)
    back_first(1, False)
    reduce_b(1)
    for got in gh_in:
        got.wait_recv()
    GS[...] = functools.reduce(jnp.add, [GR[i] for i in range(8)])
    gz_in = [push(GS, GZ.at[d - 1], at(dz=d)) for d in (1, 2, 3)]
    gather_d(3)
    grad_second(3)
    reduce_a(3)
    gather_c(0)
    reduce_c(2)
    z_in = [
        push(G2.at[2, LOW, lane(0)], ZA, at(dz=1)),
        push(G2.at[2, HIGH, lane(0)], ZB, at(dz=3)),
    ]
    back_first(3, False)
    reduce_b(3)
    gather_d(0)
    back_first(0, False)

    @pl.loop(0, 12)
    def _(i):
        rows = pl.ds(pl.multiple_of(i * 64, 64), 64)
        other = pl.ds(pl.multiple_of((1 - c) * 512, 512), 512)
        BKS[rows, :] = BACK[rows, other].astype(BF16)

    back_in = push(BKS, BKR, at(dc=1))
    grad_second(0)
    reduce_a(0)
    for got in gz_in:
        got.wait_recv()
    GY[...] = GS[...] + GZ[0] + GZ[1] + GZ[2]
    gxs_in = [push(GY, GX.at[d - 1], at(dx=d)) for d in (1, 2, 3)]
    back_in.wait_recv()

    @pl.loop(0, 12)
    def _(i):
        rows = pl.ds(pl.multiple_of(i * 64, 64), 64)
        mine = pl.ds(pl.multiple_of(c * 512, 512), 512)
        back = BACK[rows, mine] + BKR[rows, :].astype(F32)
        SF[rows, :] = (back * SP[rows, mine]).astype(BF16)

    @pl.loop(0, 2)
    def _(n):
        rows = pl.ds(pl.multiple_of(n * 256, 256), 256)
        part = dot(FT[rows, :], SF[...]).astype(BF16)
        G1[pl.ds(2 * n, 2)] = part.reshape(2, 4, 32, 512)

    lo, hi = pl.ds(0, 16), pl.ds(16, 16)
    x1, x3, x2 = mod(x + 1, 4), mod(x - 1, 4), mod(x + 2, 4)
    z1, z3, z2 = mod(zh + 1, 4), mod(zh - 1, 4), mod(zh + 2, 4)
    yin = [
        push(G1.at[x2, :, lo], YA, at(dx=1)),
        push(G1.at[x2, :, hi], YB, at(dx=3)),
        push(G1.at[x1, :, hi], YL.at[1], at(dx=1)),
        push(G1.at[x3, :, lo], YR.at[0], at(dx=3)),
    ]
    reduce_c(1)
    reduce_c(3)
    z_in += [
        push(G2.at[1, HIGH, lane(0)], ZL.at[1], at(dz=1)),
        push(G2.at[3, LOW, lane(0)], ZR.at[0], at(dz=3)),
    ]
    for got, buf, dz, half, dst in (
        (z_in[0], ZA, 1, LOW, ZL.at[0]),
        (z_in[1], ZB, 3, HIGH, ZR.at[1]),
    ):
        got.wait_recv()
        block = G2[dz, half, lane(0)].astype(F32) + buf[...].astype(F32)
        G2[dz, half, lane(0)] = block.astype(BF16)
        z_in.append(push(G2.at[dz, half, lane(0)], dst, at(dz=dz)))
    reduce_b(0)
    for got, buf, row, half, dst, dx in (
        (yin[0], YA, x1, lo, YL.at[0], 1),
        (yin[1], YB, x3, hi, YR.at[1], 3),
    ):
        got.wait_recv()
        block = G1[row, :, half].astype(F32) + buf[...].astype(F32)
        G1[row, :, half] = block.astype(BF16)
        yin.append(push(G1.at[row, :, half], dst, at(dx=dx)))
    for got in gxs_in:
        got.wait_recv()
    heads = GY[...] + GX[0] + GX[1] + GX[2]
    GH[...] = heads
    gc_in = push(GH, GC, at(dc=1))
    for got in yin[2:]:
        got.wait_recv()
    for side, half in ((0, lo), (1, hi)):
        block = G1[x, :, half].astype(F32) + YL[side].astype(F32) + YR[side].astype(F32)
        G1[x, :, half] = block.astype(BF16)
    uin = [
        push(G1.at[x, z2, lo], UA, at(dz=1)),
        push(G1.at[x, z2, hi], UB, at(dz=3)),
        push(G1.at[x, z1, hi], UL.at[1], at(dz=1)),
        push(G1.at[x, z3, lo], UR.at[0], at(dz=3)),
    ]
    gc_in.wait_recv()
    other = GC[...]
    loss_o[...] = jnp.broadcast_to(jnp.sum(heads[2]), (8, 128))
    for i in range(2):
        gh_o[:, lane(2 * i)] = jnp.where(c == 0, heads[i], other[i])
        gh_o[:, lane(2 * i + 1)] = jnp.where(c == 0, other[i], heads[i])
    for got, buf, row, half, dst, dz in (
        (uin[0], UA, z1, lo, UL.at[0], 1),
        (uin[1], UB, z3, hi, UR.at[1], 3),
    ):
        got.wait_recv()
        block = G1[x, row, half].astype(F32) + buf[...].astype(F32)
        G1[x, row, half] = block.astype(BF16)
        uin.append(push(G1.at[x, row, half], dst, at(dz=dz)))
    reduce_c(0, g2_o)
    for got in uin[2:]:
        got.wait_recv()
    for side, half in ((0, lo), (1, hi)):
        GF[side] = (
            G1[x, zh, half].astype(F32) + UL[side].astype(F32) + UR[side].astype(F32)
        )
    gt_in = push(GF.at[1 - c], GT, at(dc=1))
    for got in z_in[2:]:
        got.wait_recv()
    for side, half in ((0, LOW), (1, HIGH)):
        g2_o[half, :] = g2_o[half, :] + ZL[side].astype(F32) + ZR[side].astype(F32)
    gt_in.wait_recv()
    mine, theirs = GF[c], GT[...]
    g1_o[:, LOW] = jnp.where(c == 0, mine, theirs)
    g1_o[:, HIGH] = jnp.where(c == 0, theirs, mine)

    link.drain()

    @pl.when(c == 0)
    def _():
        for copy in re_to:
            copy.wait_send()

    @pl.when(r < 4)
    def _():
        for copy in v_out:
            copy.wait_send()


SCRATCH = [
    ((2, 384, 512), BF16), ((512, 768), BF16), ((4, 4, 2, 16, 1024), BF16),
    ((4, 1024, 512), BF16), ((8, 8, 512), F32), ((8, 2048), BF16), ((3, 2, 4, 8, 128), F32),
    ((768, 1024), BF16), ((1024, 768), BF16), ((768, 1024), F32), ((8, 96, 2048), BF16),
    ((4, 96, 512), BF16), ((4, 96, 512), BF16), ((4, 2, 96, 512), BF16),
    ((4, 2, 96, 512), BF16), ((4, 96, 512), BF16), ((96, 2048), F32), ((96, 2048), F32),
    ((96, 2048), BF16), ((2, 12, 8, 128), F32), ((12, 8, 128), F32), ((8, 96, 2048), BF16),
    ((768, 1024), F32), ((4, 1024, 512), BF16), ((4, 512, 128), BF16), ((4, 512, 128), BF16),
    ((4, 2, 512, 128), BF16), ((4, 2, 512, 128), BF16), ((512, 128), BF16),
    ((512, 128), BF16), ((2, 512, 128), BF16), ((2, 512, 128), BF16), ((768, 512), BF16),
    ((768, 512), BF16), ((768, 512), BF16), ((4, 4, 32, 512), BF16), ((4, 16, 512), BF16),
    ((4, 16, 512), BF16), ((2, 4, 16, 512), BF16), ((2, 4, 16, 512), BF16), ((16, 512), BF16),
    ((16, 512), BF16), ((2, 16, 512), BF16), ((2, 16, 512), BF16), ((2, 16, 512), F32),
    ((16, 512), F32), ((8, 3, 8, 128), F32), ((8, 3, 8, 128), F32), ((3, 8, 128), F32),
    ((3, 3, 8, 128), F32), ((3, 3, 8, 128), F32), ((3, 8, 128), F32), ((3, 8, 128), F32),
    ((3, 8, 128), F32),
]


def shards(features, w_first, w_second, w_head, rewards, discount, trace, episode):
    pad = ((0, 0), (0, 0), (0, 32))
    pieces = jnp.pad(rewards.reshape(8, 4, 96), pad).transpose(1, 0, 2)
    numbers = jnp.pad(episode.astype(F32).reshape(1, 4, 96), pad).transpose(1, 0, 2)
    rein = jnp.stack([pieces, jnp.broadcast_to(numbers, pieces.shape)])
    rates = jnp.broadcast_to(jnp.stack([discount, trace])[:, :, None], (2, 8, 128))
    heads = w_head.T.astype(F32)
    vmem = pl.BlockSpec(memory_space=pltpu.VMEM)
    advantages, loss, grad_first, grad_second, grad_head = pl.pallas_call(
        kernel,
        out_shape=(
            jax.ShapeDtypeStruct((4, 8, 128), F32),
            jax.ShapeDtypeStruct((8, 128), F32),
            jax.ShapeDtypeStruct((16, 1024), F32),
            jax.ShapeDtypeStruct((1024, 128), F32),
            jax.ShapeDtypeStruct((8, 512), F32),
        ),
        in_specs=[vmem] * 6,
        out_specs=[vmem] * 5,
        scratch_shapes=[pltpu.VMEM(shape, kind) for shape, kind in SCRATCH]
        + [pltpu.SemaphoreType.DMA((SLOTS,)), pltpu.SemaphoreType.DMA((SLOTS,))],
        compiler_params=pltpu.CompilerParams(
            collective_id=0, has_side_effects=True, vmem_limit_bytes=62 * 2**20
        ),
    )(features, w_first, w_second, heads, rein, rates)
    advantages = advantages[:, :, :96].transpose(1, 0, 2).reshape(8, 384)
    count = features.shape[0] * lax.axis_size("batch") * 8
    return advantages, 0.5 * loss[0, 0] / count, grad_first, grad_second, grad_head.T


def solution(mesh):
    placed = (
        P("batch", None),
        P("batch", "hidden"),
        P("hidden", "batch"),
        P("hidden", None),
        P(None, "batch"),
        P(),
        P(),
        P("batch"),
    )
    return jax.shard_map(
        shards,
        mesh=mesh,
        in_specs=placed,
        out_specs=(
            P(None, "batch"),
            P(),
            P("batch", "hidden"),
            P("hidden", "batch"),
            P("hidden", None),
        ),
        check_vma=False,
    )
```

```python
import functools

import jax
import jax.numpy as jnp
from jax import lax
from jax.experimental import pallas as pl
from jax.experimental.pallas import tpu as pltpu
from jax.sharding import PartitionSpec as P

BF16, F32 = jnp.bfloat16, jnp.float32
MESH = pl.DeviceIdType.MESH
SLOTS = 240
LOW, HIGH = pl.ds(0, 512), pl.ds(512, 512)


def dot(left, right, dims=((1,), (0,))):
    return lax.dot_general(left, right, (dims, ((), ())), preferred_element_type=F32)


def mod(value, count):
    return lax.rem(value + count, count)


def lane(dx):
    return pl.ds(dx * 128, 128)


class Links:
    def __init__(self, sent, came):
        self.sent, self.came, self.used, self.open = sent, came, 0, []

    def take(self):
        self.used += 1
        return self.used - 1

    def make(self, src, dst, to, k, k_came=None):
        return pltpu.make_async_remote_copy(
            src_ref=src,
            dst_ref=dst,
            send_sem=self.sent.at[k],
            recv_sem=self.came.at[k if k_came is None else k_came],
            device_id=to,
            device_id_type=MESH,
        )

    def push(self, src, dst, to, land=None):
        k = self.take()
        copy = self.make(src, dst, to, k)
        copy.start()
        self.open.append(copy)
        return copy if land is None else self.make(land, land, to, k)

    def drain(self):
        for copy in self.open:
            copy.wait_send()
        self.open = []


def kernel(
    feat, w1in, w2in, whin, reward_in, number_in, discount_in, trace_in,
    adv_o, loss_o, g1_o, g2_o, gh_o,
    F, FT, W1, W2, WHB, WH, RE, HF, HFT, SP, PS, RA, RB, RL, RR, RZ, PRE, SL2, H2,
    V, ADV, S, BACK, G2, XA, XB, XL, XR, ZA, ZB, ZL, ZR, BKS, BKR, SF,
    G1, YA, YB, YL, YR, UA, UB, UL, UR, GF, GT, GHP, GR, GS, GZ, GX, GY, GC, GH,
    WHS, RWS, EPS, WIN, sent, came, local,
):
    b, j = lax.axis_index("batch"), lax.axis_index("hidden")
    c, m = lax.rem(b, 2), lax.div(b, 2)
    zh, x = lax.rem(m, 4), lax.div(m, 4)
    y, zl = lax.rem(j, 4), lax.div(j, 4)
    r = y * 2 + zl
    link = Links(sent, came)
    push = link.push

    def at(dx=0, dz=0, dc=0, dy=0, dl=0):
        bb = (mod(x + dx, 4) * 4 + mod(zh + dz, 4)) * 2 + mod(c + dc, 2)
        return bb, mod(zl + dl, 2) * 4 + mod(y + dy, 4)

    def beside(step, dc, dy, dl):
        bb = mod(m + step, 16) * 2 + mod(c + dc, 2)
        return bb, mod(zl + dl, 2) * 4 + mod(y + dy, 4)

    peers = [(dc, dy, dl) for dc in range(2) for dy in range(4) for dl in range(2)]

    loads = [
        pltpu.make_async_copy(src, dst, local.at[k])
        for k, (src, dst) in enumerate(
            (
                (w1in, WIN),
                (w2in, W2.at[0, :, lane(0)]),
                (feat, F.at[c]),
                (whin, WHS),
                (reward_in, RWS),
                (number_in, EPS),
            )
        )
    ]
    for load in loads:
        load.start()

    barrier = pltpu.get_barrier_semaphore()
    partners = [at(dc=dc, dy=dy, dl=dl) for dc, dy, dl in peers[1:]]
    partners += [at(dx=d) for d in (1, 2, 3)] + [at(dz=d) for d in (1, 2, 3)]
    partners += [beside(step, *peer) for step in (1, -1) for peer in peers]
    for partner in partners:
        pl.semaphore_signal(barrier, inc=1, device_id=partner, device_id_type=MESH)
    for load in loads:
        load.wait()
    blank = jnp.zeros((8, 32), F32)
    WHB[j] = WHS[...].astype(F32)
    for i in range(4):
        reward = RWS[:, i * 96 : (i + 1) * 96]
        number = jnp.broadcast_to(EPS[:, i * 96 : (i + 1) * 96].astype(F32), (8, 96))
        RE[c, 0, i] = jnp.concatenate([reward, blank], axis=1)
        RE[c, 1, i] = jnp.concatenate([number, blank], axis=1)
    pl.semaphore_wait(barrier, len(partners))

    mine, theirs = (
        pl.ds(pl.multiple_of(side * 512, 512), 512) for side in (c, 1 - c)
    )
    w1pair = push(WIN.at[:, theirs], W1.at[x, zh, c], at(dc=1), W1.at[x, zh, 1 - c])
    W1[x, zh, c] = WIN[:, mine]

    def w1_sides(zs):
        own = W1.at[x, zs]
        return [push(own, own, at(dx=dx), W1.at[mod(x - dx, 4), zs]) for dx in (1, 3)]

    def w1_across(zs, sides):
        out = []
        for dx, side in ((1, 0), (3, 1)):
            sides[side].wait_recv()
            part = W1.at[mod(x - dx, 4), zs, side]
            out.append(push(part, part, at(dx=dx), W1.at[mod(x + 2, 4), zs, side]))
        return out

    w2x = {}

    def w2_to(dz, half, dx):
        key = (dz, 4 - dx, 0 if half is LOW else 1)
        w2x[key] = push(
            W2.at[dz, half, lane(0)], W2.at[dz, half, lane(4 - dx)], at(dx=dx)
        )

    def w2_side(dz, half):
        near = 1 if half is LOW else 3
        w2_to(dz, half, near)
        w2_to(dz, half, 4 - near)

    def w2_across(dz):
        w2x[dz, 3, 0].wait_recv()
        w2x[dz, 2, 0] = push(
            W2.at[dz, LOW, lane(3)], W2.at[dz, LOW, lane(2)], at(dx=1)
        )
        w2x[dz, 1, 1].wait_recv()
        w2x[dz, 2, 1] = push(
            W2.at[dz, HIGH, lane(1)], W2.at[dz, HIGH, lane(2)], at(dx=3)
        )

    def w2_rest(dz, keys=((3, 1), (1, 0), (2, 0), (2, 1))):
        for key in keys:
            w2x[(dz, *key)].wait_recv()

    def w2_z(half, dz):
        return push(W2.at[0, half, lane(0)], W2.at[4 - dz, half, lane(0)], at(dz=dz))

    first, second, w1z, w1x, w1far = [], [], {}, {}, {}

    def w1_start():
        w1pair.wait_recv()
        own = W1.at[x, zh]
        for dz in (1, 3, 2):
            w1z[dz] = push(own, own, at(dz=dz), W1.at[x, mod(zh - dz, 4)])
        w1x[0] = w1_sides(zh)

    def w1_from_z(dz):
        w1z[dz].wait_recv()
        w1x[dz] = w1_sides(mod(zh - dz, 4))

    def w1_far(dz):
        w1far[dz] = w1_across(mod(zh - dz, 4), w1x[dz])

    def w1_done():
        for dz in (0, 1, 3, 2):
            for copy in w1far[dz]:
                copy.wait_recv()

    w1_start()
    w2_to(0, LOW, 1)
    w2_to(0, HIGH, 3)
    first += [w2_z(LOW, 1), w2_z(HIGH, 3)]
    second += [w2_z(HIGH, 1), w2_z(LOW, 3)]
    feat_in = push(F.at[c], F.at[c], at(dc=1), F.at[1 - c])
    w1_from_z(1)
    w1_from_z(3)
    w1_far(0)
    w1_from_z(2)
    w2_to(0, HIGH, 1)
    w2_to(0, LOW, 3)
    re_in = push(RE.at[c], RE.at[c], at(dc=1), RE.at[1 - c])
    re_sem = [link.take() for _ in range(2)]
    re_to = [
        link.make(RE.at[c], RE.at[2], beside(-1, dc, 0, 0), re_sem[dc], re_sem[0])
        for dc in range(2)
    ]

    @pl.when(c == 0)
    def _():
        for copy in re_to:
            copy.start()

    wh_in = [
        push(WHB.at[j], WHB.at[j], at(dy=dy, dl=dl), WHB.at[mod(zl - dl, 2) * 4 + mod(y - dy, 4)])
        for dc, dy, dl in peers[1:8]
    ]

    w1_far(1)
    w1_far(3)
    w1_far(2)
    w2_across(0)
    w2_z2 = []

    def w2_first():
        first[0].wait_recv()
        w2_z2.append(push(W2.at[3, LOW, lane(0)], W2.at[2, LOW, lane(0)], at(dz=1)))
        w2_side(3, LOW)
        first[1].wait_recv()
        w2_z2.append(push(W2.at[1, HIGH, lane(0)], W2.at[2, HIGH, lane(0)], at(dz=3)))
        w2_side(1, HIGH)

    def w2_second():
        second[0].wait_recv()
        w2_side(3, HIGH)
        second[1].wait_recv()
        w2_side(1, LOW)

    def w2_third():
        w2_z2[0].wait_recv()
        w2_side(2, LOW)
        w2_z2[1].wait_recv()
        w2_side(2, HIGH)

    w2_first()
    feat_in.wait_recv()
    w1_done()
    hf_in = []

    def layer_one():
        for n in range(2):
            cols = pl.ds(n * 256, 256)
            into = pl.ds(pl.multiple_of(c * 512 + n * 256, 256), 256)
            there = pl.ds(pl.multiple_of((1 - c) * 512 + n * 256, 256), 256)
            weights = W1[:, :, :, :, cols].reshape(512, 256)
            SP[:, cols] = dot(F[...].reshape(768, 512), weights)

            @pl.loop(0, 12)
            def _(i):
                rows = pl.ds(pl.multiple_of(i * 64, 64), 64)
                value = SP[rows, cols]
                gate = 1.0 / (1.0 + jnp.exp(-value))
                HF[rows, into] = (value * gate).astype(BF16)
                SP[rows, cols] = gate * (1.0 + value * (1.0 - gate))

            src = HF.at[:, into]
            hf_in.append(push(src, src, at(dc=1), HF.at[:, there]))

    layer_one()
    w2_second()

    def product(dz, part=None):
        for n in range(2) if part is None else (part,):
            out = dot(HF[...], W2[dz, :, pl.ds(n * 256, 256)])
            into = pl.ds(dz * 512 + n * 256, 256)
            PS[:, :, into] = out.astype(BF16).reshape(8, 96, 256)

    up, down, over = mod(y + 1, 4), mod(y - 1, 4), mod(y + 2, 4)
    came_rs = {}

    def lanes(dz, part):
        if part is None:
            return pl.ds(dz * 512, 512), pl.ds(0, 512)
        return pl.ds(dz * 512 + part * 256, 256), pl.ds(part * 256, 256)

    def scatter_a(dz, part=None):
        wide, here = lanes(dz, part)
        came_rs[dz, part] = [
            push(PS.at[over * 2, :, wide], RA.at[dz, :, here], at(dy=1)),
            push(PS.at[over * 2 + 1, :, wide], RB.at[dz, :, here], at(dy=3)),
            push(PS.at[up * 2 + 1, :, wide], RL.at[dz, 1, :, here], at(dy=1)),
            push(PS.at[down * 2, :, wide], RR.at[dz, 0, :, here], at(dy=3)),
        ]

    def scatter_b(dz, part=None):
        wide, here = lanes(dz, part)
        for got, buf, row, dst, dy in (
            (came_rs[dz, part][0], RA, up * 2, RL.at[dz, 0, :, here], 1),
            (came_rs[dz, part][1], RB, down * 2 + 1, RR.at[dz, 1, :, here], 3),
        ):
            got.wait_recv()
            total = PS[row, :, wide].astype(F32) + buf[dz, :, here].astype(F32)
            PS[row, :, wide] = total.astype(BF16)
            came_rs[dz, part].append(push(PS.at[row, :, wide], dst, at(dy=dy)))

    def scatter_c(dz, part=None):
        wide, here = lanes(dz, part)
        for got in came_rs[dz, part][2:]:
            got.wait_recv()

        def total(side):
            return (
                PS[y * 2 + side, :, wide].astype(F32)
                + RL[dz, side, :, here].astype(F32)
                + RR[dz, side, :, here].astype(F32)
            )

        PS[y * 2 + 1 - zl, :, wide] = total(1 - zl).astype(BF16)
        came_rs[dz, part].append(
            push(PS.at[y * 2 + 1 - zl, :, wide], RZ.at[dz, :, here], at(dl=1))
        )
        PRE[:, wide] = total(zl)

    def scatter_d(dz, part=None):
        wide, here = lanes(dz, part)
        came_rs[dz, part][-1].wait_recv()

        @pl.loop(0, 3)
        def _(i):
            rows = pl.ds(pl.multiple_of(i * 32, 32), 32)
            value = PRE[rows, wide] + RZ[dz, rows, here].astype(F32)
            gate = 1.0 / (1.0 + jnp.exp(-value))
            H2[rows, wide] = (value * gate).astype(BF16)
            SL2[rows, wide] = gate * (1.0 + value * (1.0 - gate))

    for got in hf_in:
        got.wait_recv()
    w2_rest(0)
    product(0)
    scatter_a(0)
    w2_across(3)
    w2_across(1)
    w2_third()
    scatter_b(0)

    def transposes():
        @pl.loop(0, 4)
        def _(n):
            cols = pl.ds(pl.multiple_of(n * 256, 256), 256)
            HFT[cols, :] = HF[:, cols].astype(F32).T.astype(BF16)

        @pl.loop(0, 2)
        def _(n):
            cols = pl.ds(pl.multiple_of(n * 256, 256), 256)
            FT[cols, :] = F[:, :, cols].reshape(768, 256).astype(F32).T.astype(BF16)

    transposes()
    w2_rest(3)
    product(3)
    scatter_a(3)
    scatter_c(0)
    w2_rest(1)
    product(1)
    scatter_a(1)
    w2_across(2)
    scatter_b(3)
    for copy in wh_in:
        copy.wait_recv()
    for dz in range(4):
        for dx in range(4):
            mm = mod(x + dx, 4) * 4 + mod(zh + dz, 4)
            group, pair = lax.div(mm, 2), lax.rem(mm, 2)
            even, odd = (
                jnp.where(c == 0, WHB[group, :, lane(2 * p)], WHB[group, :, lane(2 * p + 1)])
                for p in (0, 1)
            )
            WH[:, lane(dz * 4 + dx)] = jnp.where(pair == 0, even, odd).astype(BF16)
    scatter_d(0)
    scatter_b(1)
    w2_rest(2, ((1, 0),))
    product(2, 0)
    scatter_a(2, 0)
    w2_rest(2, ((3, 1), (2, 0), (2, 1)))
    product(2, 1)
    scatter_a(2, 1)
    scatter_c(3)
    scatter_c(1)
    scatter_d(3)
    scatter_b(2, 0)
    scatter_b(2, 1)
    scatter_d(1)
    scatter_c(2, 0)
    scatter_c(2, 1)
    scatter_d(2, 0)
    scatter_d(2, 1)

    own_values = dot(WH[...], H2[...], ((1,), (1,)))
    V[c, r] = jnp.concatenate([own_values, blank], axis=1)
    v_in = []
    for dc, dy, dl in peers[1:]:
        src_r = mod(y - dy, 4) * 2 + mod(zl - dl, 2)
        v_in.append(
            push(V.at[c, r], V.at[c, r], at(dc=dc, dy=dy, dl=dl), V.at[mod(c - dc, 2), src_r])
        )
    v_out, v_next = [], []
    for dc, dy, dl in peers:
        k = link.take()
        src_r = mod(y - dy, 4) * 2 + mod(zl - dl, 2)
        v_out.append(
            link.make(V.at[c, r], V.at[c, 8 + lax.rem(r, 4)], beside(-1, dc, dy, dl), k)
        )
        land = V.at[mod(c - dc, 2), 8 + lax.rem(src_r, 4)]
        v_next.append((src_r, link.make(land, land, beside(-1, dc, dy, dl), k)))

    @pl.when(r < 4)
    def _():
        for copy in v_out:
            copy.start()

    re_in.wait_recv()
    link.make(RE.at[2], RE.at[2], at(dc=1), re_sem[0], re_sem[0]).wait_recv()
    shape = (8, 12 * 128)
    place = lax.rem(lax.broadcasted_iota(jnp.int32, shape, 1), 128)

    def ahead(array, steps):
        return pltpu.roll(array, shape[1] - steps, 1)

    def following(array):
        return jnp.where(place == 95, ahead(array, 33), ahead(array, 1))

    def row_of(kind):
        return jnp.concatenate([RE[i // 4, kind, i % 4] for i in range(12)], axis=1)

    reward, number = row_of(0), row_of(1)
    head_row = lax.broadcasted_iota(jnp.int32, (8, 128), 0)

    def spread(array):
        out = jnp.zeros((8, 128), F32)
        for k in range(8):
            out = jnp.where(head_row == k, array[k], out)
        return out

    rate, decay = spread(discount_in), spread(trace_in)
    discount = jnp.concatenate([rate] * 12, axis=1)
    both = jnp.concatenate([rate * decay] * 12, axis=1)
    keep = jnp.where(following(number) == number, 1.0, 0.0)
    real = place < 96
    factor = jnp.where(real, both * keep, 1.0)
    scale = discount * keep

    for copy in v_in:
        copy.wait_recv()
    for src_r, copy in v_next:

        @pl.when(src_r < 4)
        def _():
            copy.wait_recv()

    value = jnp.concatenate([V[0, i] + V[1, i] for i in range(12)], axis=1)
    total = jnp.where(real, reward + scale * following(value) - value, 0.0)
    step = 1
    while step < shape[1]:
        total = total + factor * ahead(total, step)
        factor = factor * ahead(factor, step)
        step *= 2
    for i in range(12):
        ADV[i] = total[:, i * 128 : (i + 1) * 128]

    own = ADV[r]
    slope_t = (-own[:, :96]).astype(BF16)
    slope = (-own).T[:96, :].astype(BF16)
    own_rows = S.at[r]

    def slope_chunk(dz):
        at_dz = pl.ds(dz * 512, 512)
        own_rows[:, at_dz] = (dot(slope, WH[:, at_dz]) * SL2[:, at_dz]).astype(BF16)

    ag = {}
    pair_r = y * 2 + 1 - zl

    def gather_a(dz, part=None):
        wide, _ = lanes(dz, part)
        src = S.at[r, :, wide]
        ag[dz, part] = {
            "pair": push(src, src, at(dl=1), S.at[pair_r, :, wide]),
            "down": push(src, src, at(dy=1), S.at[down * 2 + zl, :, wide]),
            "up": push(src, src, at(dy=3), S.at[up * 2 + zl, :, wide]),
        }

    def gather_b(dz, part=None):
        wide, _ = lanes(dz, part)
        got = ag[dz, part]
        got["pair"].wait_recv()
        src = S.at[pair_r, :, wide]
        got["down2"] = push(src, src, at(dy=1), S.at[down * 2 + 1 - zl, :, wide])
        got["up2"] = push(src, src, at(dy=3), S.at[up * 2 + 1 - zl, :, wide])

    def gather_c(dz, part=None):
        wide, _ = lanes(dz, part)
        got = ag[dz, part]
        for name in ("down", "up", "down2", "up2"):
            got[name].wait_recv()
        low, high = S.at[down * 2, :, wide], S.at[up * 2 + 1, :, wide]
        got["far"] = [
            push(low, low, at(dy=1), S.at[over * 2, :, wide]),
            push(high, high, at(dy=3), S.at[over * 2 + 1, :, wide]),
        ]

    def gather_d(dz, part=None):
        for got in ag[dz, part]["far"]:
            got.wait_recv()

    def grad_part(dz, part):
        wide, here = lanes(dz, part)

        @pl.loop(0, 2)
        def _(n):
            rows = pl.ds(pl.multiple_of(n * 512, 512), 512)
            G2[dz, rows, here] = dot(HFT[rows, :], S[:, :, wide].reshape(768, 256)).astype(BF16)

    def grad_second(dz, side):
        at_dz = pl.ds(dz * 512, 512)

        @pl.loop(0, 2)
        def _(n):
            rows = pl.ds(pl.multiple_of(side * 512 + n * 256, 256), 256)
            G2[dz, rows, :] = dot(HFT[rows, :], S[:, :, at_dz].reshape(768, 512)).astype(BF16)

    def back_first(dz, start):
        at_dz = pl.ds(dz * 512, 512)

        @pl.loop(0, 4)
        def _(n):
            cols = pl.ds(pl.multiple_of(n * 256, 256), 256)
            part = dot(S[:, :, at_dz].reshape(768, 512), W2[dz, cols, :], ((1,), (1,)))
            BACK[:, cols] = part if start else BACK[:, cols] + part

    gx, halves = {}, (LOW, HIGH)

    def reduce_far(dz, side):
        src = G2.at[dz, halves[side], lane(2)]
        gx[dz, side] = [push(src, (XA, XB)[side].at[dz], at(dx=(1, 3)[side]))]

    def reduce_near(dz, side):
        src = G2.at[dz, halves[side], lane((3, 1)[side])]
        gx[dz, side].append(push(src, (XR, XL)[side].at[dz, side], at(dx=(3, 1)[side])))

    def reduce_a(dz, side):
        reduce_far(dz, side)
        reduce_near(dz, side)

    def reduce_b(dz, side):
        gx[dz, side][0].wait_recv()
        dx, half = (1, 3)[side], halves[side]
        block = G2[dz, half, lane(dx)].astype(F32) + (XA, XB)[side][dz].astype(F32)
        G2[dz, half, lane(dx)] = block.astype(BF16)
        src = G2.at[dz, half, lane(dx)]
        gx[dz, side].append(push(src, (XL, XR)[side].at[dz, side], at(dx=dx)))

    def reduce_c(dz, side, into=None):
        half = halves[side]
        for got in gx[dz, side][1:]:
            got.wait_recv()
        block = (
            G2[dz, half, lane(0)].astype(F32)
            + XL[dz, side].astype(F32)
            + XR[dz, side].astype(F32)
        )
        if into is None:
            G2[dz, half, lane(0)] = block.astype(BF16)
        else:
            into[half, :] = block

    z_far, z_in = [], []

    def reduce_z(dz, side):
        half = halves[side]
        src = G2.at[dz, half, lane(0)]
        if dz == 2:
            z_far.append(push(src, (ZA, ZB)[side], at(dz=(1, 3)[side])))
            return
        if (dz, side) in ((1, 0), (3, 1)):
            z_far[side].wait_recv()
            block = G2[dz, half, lane(0)].astype(F32) + (ZA, ZB)[side][...].astype(F32)
            G2[dz, half, lane(0)] = block.astype(BF16)
        z_in.append(push(src, (ZL if dz == 1 else ZR).at[side], at(dz=dz)))

    slope_chunk(2)
    gather_a(2, 1)
    gather_a(2, 0)
    slope_chunk(1)
    gather_a(1)
    slope_chunk(3)
    slope_chunk(0)
    gather_b(2, 1)
    gather_b(2, 0)
    gather_a(3)

    for i in range(4):
        adv_o[i] = ADV[4 * c + i]
    small = lax.broadcasted_iota(jnp.int32, (8, 128), 1) < 96
    own_loss = jnp.where(small, own * own, 0.0)
    head = dot(slope_t, H2[...])
    for dz in range(4):
        for dx in range(4):
            mm = mod(x + dx, 4) * 4 + mod(zh + dz, 4)
            GHP[lax.div(mm, 2), lax.rem(mm, 2)] = head[:, (dz * 4 + dx) * 128 :][:, :128]
    for g in range(8):
        GHP[g, 2] = own_loss
    gather_c(2, 1)
    gather_c(2, 0)
    gather_b(1)
    gather_a(0)
    gh_in = []
    for dc, dy, dl in peers[1:8]:
        to_j = mod(zl + dl, 2) * 4 + mod(y + dy, 4)
        from_j = mod(zl - dl, 2) * 4 + mod(y - dy, 4)
        gh_in.append(push(GHP.at[to_j], GR.at[j], at(dy=dy, dl=dl), GR.at[from_j]))
    GR[j] = GHP[j]
    gather_d(2, 1)
    grad_part(2, 1)
    reduce_far(2, 0)
    reduce_far(2, 1)
    reduce_near(2, 0)
    gather_d(2, 0)
    grad_part(2, 0)
    reduce_near(2, 1)
    gather_c(1)
    gather_b(3)
    gather_b(0)
    back_first(2, True)
    reduce_b(2, 0)
    reduce_b(2, 1)
    gather_d(1)
    grad_second(1, 1)
    reduce_a(1, 1)
    gather_c(3)
    back_first(1, False)
    gather_c(0)
    gather_d(3)
    grad_second(3, 0)
    reduce_a(3, 0)
    reduce_b(1, 1)
    grad_second(3, 1)
    reduce_a(3, 1)
    grad_second(1, 0)
    reduce_a(1, 0)
    reduce_c(2, 0)
    reduce_z(2, 0)
    reduce_c(2, 1)
    reduce_z(2, 1)
    reduce_b(3, 0)
    back_first(3, False)
    gather_d(0)
    back_first(0, False)

    @pl.loop(0, 12)
    def _(i):
        rows = pl.ds(pl.multiple_of(i * 64, 64), 64)
        BKS[rows, :] = BACK[rows, theirs].astype(BF16)

    back_in = push(BKS, BKR, at(dc=1))
    reduce_b(3, 1)
    reduce_c(1, 1)
    reduce_z(1, 1)
    back_in.wait_recv()

    @pl.loop(0, 12)
    def _(i):
        rows = pl.ds(pl.multiple_of(i * 64, 64), 64)
        back = BACK[rows, mine] + BKR[rows, :].astype(F32)
        SF[rows, :] = (back * SP[rows, :]).astype(BF16)

    @pl.loop(0, 2)
    def _(n):
        rows = pl.ds(pl.multiple_of(n * 256, 256), 256)
        part = dot(FT[rows, :], SF[...]).astype(BF16)
        G1[pl.ds(2 * n, 2)] = part.reshape(2, 4, 32, 512)

    lo, hi = pl.ds(0, 16), pl.ds(16, 16)
    x1, x3, x2 = mod(x + 1, 4), mod(x - 1, 4), mod(x + 2, 4)
    z1, z3, z2 = mod(zh + 1, 4), mod(zh - 1, 4), mod(zh + 2, 4)
    yin = [
        push(G1.at[x2, :, lo], YA, at(dx=1)),
        push(G1.at[x2, :, hi], YB, at(dx=3)),
        push(G1.at[x1, :, hi], YL.at[1], at(dx=1)),
        push(G1.at[x3, :, lo], YR.at[0], at(dx=3)),
    ]
    reduce_b(1, 0)
    grad_second(0, 0)
    grad_second(0, 1)
    reduce_c(3, 0)
    reduce_z(3, 0)

    def sums_y():
        for got, buf, row, half, dst, dx in (
            (yin[0], YA, x1, lo, YL.at[0], 1),
            (yin[1], YB, x3, hi, YR.at[1], 3),
        ):
            got.wait_recv()
            block = G1[row, :, half].astype(F32) + buf[...].astype(F32)
            G1[row, :, half] = block.astype(BF16)
            yin.append(push(G1.at[row, :, half], dst, at(dx=dx)))

    sums_y()
    reduce_a(0, 0)
    reduce_a(0, 1)
    for got in gh_in:
        got.wait_recv()
    GS[...] = functools.reduce(jnp.add, [GR[i] for i in range(8)])
    gz_in = [push(GS, GZ.at[d - 1], at(dz=d)) for d in (1, 2, 3)]
    reduce_c(3, 1)
    reduce_z(3, 1)
    reduce_c(1, 0)
    reduce_z(1, 0)
    for got in yin[2:]:
        got.wait_recv()
    for side, half in ((0, lo), (1, hi)):
        block = G1[x, :, half].astype(F32) + YL[side].astype(F32) + YR[side].astype(F32)
        G1[x, :, half] = block.astype(BF16)
    uin = [
        push(G1.at[x, z2, lo], UA, at(dz=1)),
        push(G1.at[x, z2, hi], UB, at(dz=3)),
        push(G1.at[x, z1, hi], UL.at[1], at(dz=1)),
        push(G1.at[x, z3, lo], UR.at[0], at(dz=3)),
    ]
    reduce_b(0, 0)
    reduce_b(0, 1)
    for got in gz_in:
        got.wait_recv()
    GY[...] = GS[...] + GZ[0] + GZ[1] + GZ[2]
    gxs_in = [push(GY, GX.at[d - 1], at(dx=d)) for d in (1, 2, 3)]
    for got, buf, row, half, dst, dz in (
        (uin[0], UA, z1, lo, UL.at[0], 1),
        (uin[1], UB, z3, hi, UR.at[1], 3),
    ):
        got.wait_recv()
        block = G1[x, row, half].astype(F32) + buf[...].astype(F32)
        G1[x, row, half] = block.astype(BF16)
        uin.append(push(G1.at[x, row, half], dst, at(dz=dz)))
    for got in gxs_in:
        got.wait_recv()
    heads = GY[...] + GX[0] + GX[1] + GX[2]
    GH[...] = heads
    gc_in = push(GH, GC, at(dc=1))
    for got in uin[2:]:
        got.wait_recv()
    for side, half in ((0, lo), (1, hi)):
        GF[side] = (
            G1[x, zh, half].astype(F32) + UL[side].astype(F32) + UR[side].astype(F32)
        )
    gt_in = push(GF.at[1 - c], GT, at(dc=1))
    gc_in.wait_recv()
    other = GC[...]
    loss_o[...] = jnp.broadcast_to(jnp.sum(heads[2]), (8, 128))
    for i in range(2):
        gh_o[:, lane(2 * i)] = jnp.where(c == 0, heads[i], other[i])
        gh_o[:, lane(2 * i + 1)] = jnp.where(c == 0, other[i], heads[i])
    reduce_c(0, 0, g2_o)
    reduce_c(0, 1, g2_o)
    for got in z_in:
        got.wait_recv()
    for side, half in ((0, LOW), (1, HIGH)):
        g2_o[half, :] = g2_o[half, :] + ZL[side].astype(F32) + ZR[side].astype(F32)
    gt_in.wait_recv()
    kept, brought = GF[c], GT[...]
    g1_o[:, LOW] = jnp.where(c == 0, kept, brought)
    g1_o[:, HIGH] = jnp.where(c == 0, brought, kept)

    link.drain()

    @pl.when(c == 0)
    def _():
        for copy in re_to:
            copy.wait_send()

    @pl.when(r < 4)
    def _():
        for copy in v_out:
            copy.wait_send()


SCRATCH = [
    ((2, 384, 512), BF16), ((512, 768), BF16), ((4, 4, 2, 16, 512), BF16),
    ((4, 1024, 512), BF16), ((8, 8, 512), F32), ((8, 2048), BF16), ((3, 2, 4, 8, 128), F32),
    ((768, 1024), BF16), ((1024, 768), BF16), ((768, 512), F32), ((8, 96, 2048), BF16),
    ((4, 96, 512), BF16), ((4, 96, 512), BF16), ((4, 2, 96, 512), BF16),
    ((4, 2, 96, 512), BF16), ((4, 96, 512), BF16), ((96, 2048), F32), ((96, 2048), F32),
    ((96, 2048), BF16), ((2, 12, 8, 128), F32), ((12, 8, 128), F32), ((8, 96, 2048), BF16),
    ((768, 1024), F32), ((4, 1024, 512), BF16), ((4, 512, 128), BF16), ((4, 512, 128), BF16),
    ((4, 2, 512, 128), BF16), ((4, 2, 512, 128), BF16), ((512, 128), BF16),
    ((512, 128), BF16), ((2, 512, 128), BF16), ((2, 512, 128), BF16), ((768, 512), BF16),
    ((768, 512), BF16), ((768, 512), BF16), ((4, 4, 32, 512), BF16), ((4, 16, 512), BF16),
    ((4, 16, 512), BF16), ((2, 4, 16, 512), BF16), ((2, 4, 16, 512), BF16), ((16, 512), BF16),
    ((16, 512), BF16), ((2, 16, 512), BF16), ((2, 16, 512), BF16), ((2, 16, 512), F32),
    ((16, 512), F32), ((8, 3, 8, 128), F32), ((8, 3, 8, 128), F32), ((3, 8, 128), F32),
    ((3, 3, 8, 128), F32), ((3, 3, 8, 128), F32), ((3, 8, 128), F32), ((3, 8, 128), F32),
    ((3, 8, 128), F32), ((8, 512), BF16), ((8, 384), F32), ((1, 384), jnp.int32),
    ((16, 1024), BF16),
]


def finish(adv, loss, g1, g2, gh, adv_o, loss_o, g1_o, g2_o, gh_o):
    adv_o[...] = jnp.concatenate([adv[i][:, :96] for i in range(4)], axis=1)
    loss_o[0, 0] = loss[0, 0] * (0.5 / 98304)
    g1_o[...] = g1[...]
    g2_o[...] = g2[...]
    gh_o[...] = gh[...]


def shards(features, w_first, w_second, w_head, rewards, discount, trace, episode):
    vmem = pl.BlockSpec(memory_space=pltpu.VMEM)
    smem = pl.BlockSpec(memory_space=pltpu.SMEM)
    hbm = pl.BlockSpec(memory_space=pltpu.HBM)
    shapes = ((16, 1024), (1024, 128), (8, 512))
    parts = pl.pallas_call(
        kernel,
        out_shape=[
            jax.ShapeDtypeStruct(shape, F32) for shape in ((4, 8, 128), (8, 128), *shapes)
        ],
        in_specs=[hbm] * 6 + [smem] * 2,
        out_specs=[vmem] * 5,
        scratch_shapes=[pltpu.VMEM(shape, kind) for shape, kind in SCRATCH]
        + [pltpu.SemaphoreType.DMA((count,)) for count in (SLOTS, SLOTS, 6)],
        compiler_params=pltpu.CompilerParams(
            collective_id=0, has_side_effects=True, vmem_limit_bytes=62 * 2**20
        ),
    )(
        features, w_first, w_second, w_head.T, rewards, episode.reshape(1, -1),
        discount, trace,
    )
    advantages, loss, grad_first, grad_second, grad_head = pl.pallas_call(
        finish,
        out_shape=[
            jax.ShapeDtypeStruct(shape, F32) for shape in ((8, 384), (1, 1), *shapes)
        ],
        in_specs=[vmem, smem, vmem, vmem, vmem],
        out_specs=[vmem, smem, vmem, vmem, vmem],
    )(*parts)
    return advantages, loss[0, 0], grad_first, grad_second, grad_head.T


def solution(mesh):
    placed = (
        P("batch", None),
        P("batch", "hidden"),
        P("hidden", "batch"),
        P("hidden", None),
        P(None, "batch"),
        P(),
        P(),
        P("batch"),
    )
    return jax.shard_map(
        shards,
        mesh=mesh,
        in_specs=placed,
        out_specs=(
            P(None, "batch"),
            P(),
            P("batch", "hidden"),
            P("hidden", "batch"),
            P("hidden", None),
        ),
        check_vma=False,
    )
```

```python
import functools

import jax
import jax.numpy as jnp
from jax import lax
from jax.experimental import pallas as pl
from jax.experimental.pallas import tpu as pltpu
from jax.sharding import PartitionSpec as P

BF16, F32 = jnp.bfloat16, jnp.float32
MESH = pl.DeviceIdType.MESH
SLOTS = 240
LOW, HIGH = pl.ds(0, 512), pl.ds(512, 512)


def dot(left, right, dims=((1,), (0,))):
    return lax.dot_general(left, right, (dims, ((), ())), preferred_element_type=F32)


def mod(value, count):
    return lax.rem(value + count, count)


def lane(dx):
    return pl.ds(dx * 128, 128)


class Links:
    def __init__(self, sent, came):
        self.sent, self.came, self.used, self.open = sent, came, 0, []

    def take(self):
        self.used += 1
        return self.used - 1

    def make(self, src, dst, to, k, k_came=None):
        return pltpu.make_async_remote_copy(
            src_ref=src,
            dst_ref=dst,
            send_sem=self.sent.at[k],
            recv_sem=self.came.at[k if k_came is None else k_came],
            device_id=to,
            device_id_type=MESH,
        )

    def push(self, src, dst, to, land=None):
        k = self.take()
        copy = self.make(src, dst, to, k)
        copy.start()
        self.open.append(copy)
        return copy if land is None else self.make(land, land, to, k)

    def drain(self):
        for copy in self.open:
            copy.wait_send()
        self.open = []


def kernel(
    feat, w1in, w2in, whin, reward_in, number_in, discount_in, trace_in,
    adv_o, loss_o, g1_o, g2_o, gh_o,
    F, FT, W1, W2, WHB, WH, RE, HF, HFT, SP, PS, RA, RB, RL, RR, RZ, PRE, SL2, H2,
    V, ADV, S, BACK, G2, XA, XB, XL, XR, ZA, ZB, ZL, ZR, BKS, BKR, SF,
    G1, YA, YB, YL, YR, UA, UB, UL, UR, GF, GT, GHP, GR, GS, GZ, GX, GY, GC, GH,
    WHS, RWS, EPS, WIN, sent, came, local,
):
    b, j = lax.axis_index("batch"), lax.axis_index("hidden")
    c, m = lax.rem(b, 2), lax.div(b, 2)
    zh, x = lax.rem(m, 4), lax.div(m, 4)
    y, zl = lax.rem(j, 4), lax.div(j, 4)
    r = y * 2 + zl
    link = Links(sent, came)
    push = link.push

    def at(dx=0, dz=0, dc=0, dy=0, dl=0):
        bb = (mod(x + dx, 4) * 4 + mod(zh + dz, 4)) * 2 + mod(c + dc, 2)
        return bb, mod(zl + dl, 2) * 4 + mod(y + dy, 4)

    def beside(step, dc, dy, dl):
        bb = mod(m + step, 16) * 2 + mod(c + dc, 2)
        return bb, mod(zl + dl, 2) * 4 + mod(y + dy, 4)

    peers = [(dc, dy, dl) for dc in range(2) for dy in range(4) for dl in range(2)]

    loads = [
        pltpu.make_async_copy(src, dst, local.at[k])
        for k, (src, dst) in enumerate(
            (
                (w1in, WIN),
                (w2in, W2.at[0, :, lane(0)]),
                (feat, F.at[c]),
                (whin, WHS),
                (reward_in, RWS),
                (number_in, EPS),
            )
        )
    ]
    for load in loads:
        load.start()

    barrier = pltpu.get_barrier_semaphore()
    partners = [at(dc=dc, dy=dy, dl=dl) for dc, dy, dl in peers[1:]]
    partners += [at(dx=d) for d in (1, 2, 3)] + [at(dz=d) for d in (1, 2, 3)]
    partners += [beside(step, *peer) for step in (1, -1) for peer in peers]
    for partner in partners:
        pl.semaphore_signal(barrier, inc=1, device_id=partner, device_id_type=MESH)
    for load in loads:
        load.wait()
    blank = jnp.zeros((8, 32), F32)
    WHB[j] = WHS[...].astype(F32)
    for i in range(4):
        reward = RWS[:, i * 96 : (i + 1) * 96]
        number = jnp.broadcast_to(EPS[:, i * 96 : (i + 1) * 96].astype(F32), (8, 96))
        RE[c, 0, i] = jnp.concatenate([reward, blank], axis=1)
        RE[c, 1, i] = jnp.concatenate([number, blank], axis=1)
    pl.semaphore_wait(barrier, len(partners))

    mine, theirs = (
        pl.ds(pl.multiple_of(side * 512, 512), 512) for side in (c, 1 - c)
    )
    w1pair = push(WIN.at[:, theirs], W1.at[x, zh, c], at(dc=1), W1.at[x, zh, 1 - c])
    W1[x, zh, c] = WIN[:, mine]

    def w1_sides(zs):
        own = W1.at[x, zs]
        return [push(own, own, at(dx=dx), W1.at[mod(x - dx, 4), zs]) for dx in (1, 3)]

    def w1_across(zs, sides):
        out = []
        for dx, side in ((1, 0), (3, 1)):
            sides[side].wait_recv()
            part = W1.at[mod(x - dx, 4), zs, side]
            out.append(push(part, part, at(dx=dx), W1.at[mod(x + 2, 4), zs, side]))
        return out

    w2x = {}

    def w2_to(dz, half, dx):
        key = (dz, 4 - dx, 0 if half is LOW else 1)
        w2x[key] = push(
            W2.at[dz, half, lane(0)], W2.at[dz, half, lane(4 - dx)], at(dx=dx)
        )

    def w2_side(dz, half):
        near = 1 if half is LOW else 3
        w2_to(dz, half, near)
        w2_to(dz, half, 4 - near)

    def w2_across(dz):
        w2x[dz, 3, 0].wait_recv()
        w2x[dz, 2, 0] = push(
            W2.at[dz, LOW, lane(3)], W2.at[dz, LOW, lane(2)], at(dx=1)
        )
        w2x[dz, 1, 1].wait_recv()
        w2x[dz, 2, 1] = push(
            W2.at[dz, HIGH, lane(1)], W2.at[dz, HIGH, lane(2)], at(dx=3)
        )

    def w2_rest(dz, keys=((3, 1), (1, 0), (2, 0), (2, 1))):
        for key in keys:
            w2x[(dz, *key)].wait_recv()

    def w2_z(half, dz):
        return push(W2.at[0, half, lane(0)], W2.at[4 - dz, half, lane(0)], at(dz=dz))

    first, second, w1z, w1x, w1far = [], [], {}, {}, {}

    def w1_start():
        w1pair.wait_recv()
        own = W1.at[x, zh]
        for dz in (1, 3, 2):
            w1z[dz] = push(own, own, at(dz=dz), W1.at[x, mod(zh - dz, 4)])
        w1x[0] = w1_sides(zh)

    def w1_from_z(dz):
        w1z[dz].wait_recv()
        w1x[dz] = w1_sides(mod(zh - dz, 4))

    def w1_far(dz):
        w1far[dz] = w1_across(mod(zh - dz, 4), w1x[dz])

    def w1_done():
        for dz in (0, 1, 3, 2):
            for copy in w1far[dz]:
                copy.wait_recv()

    w1_start()
    w2_to(0, LOW, 1)
    w2_to(0, HIGH, 3)
    first += [w2_z(LOW, 1), w2_z(HIGH, 3)]
    feat_in = push(F.at[c], F.at[c], at(dc=1), F.at[1 - c])
    w1_from_z(1)
    w2_to(0, HIGH, 1)
    w2_to(0, LOW, 3)
    w1_from_z(3)
    w1_far(0)
    w1_from_z(2)
    second += [w2_z(HIGH, 1), w2_z(LOW, 3)]
    re_in = push(RE.at[c], RE.at[c], at(dc=1), RE.at[1 - c])
    re_sem = [link.take() for _ in range(2)]
    re_to = [
        link.make(RE.at[c], RE.at[2], beside(-1, dc, 0, 0), re_sem[dc], re_sem[0])
        for dc in range(2)
    ]

    @pl.when(c == 0)
    def _():
        for copy in re_to:
            copy.start()

    wh_in = [
        push(WHB.at[j], WHB.at[j], at(dy=dy, dl=dl), WHB.at[mod(zl - dl, 2) * 4 + mod(y - dy, 4)])
        for dc, dy, dl in peers[1:8]
    ]

    w1_far(1)
    w1_far(3)
    w1_far(2)
    w2_across(0)
    w2_z2 = []

    def w2_first():
        first[0].wait_recv()
        w2_z2.append(push(W2.at[3, LOW, lane(0)], W2.at[2, LOW, lane(0)], at(dz=1)))
        w2_side(3, LOW)
        first[1].wait_recv()
        w2_z2.append(push(W2.at[1, HIGH, lane(0)], W2.at[2, HIGH, lane(0)], at(dz=3)))
        w2_side(1, HIGH)

    def w2_second():
        second[0].wait_recv()
        w2_side(3, HIGH)
        second[1].wait_recv()
        w2_side(1, LOW)

    def w2_third():
        w2_z2[0].wait_recv()
        w2_side(2, LOW)
        w2_z2[1].wait_recv()
        w2_side(2, HIGH)

    w2_first()
    feat_in.wait_recv()
    w1_done()
    hf_in = []

    def layer_one():
        for n in range(2):
            cols = pl.ds(n * 256, 256)
            into = pl.ds(pl.multiple_of(c * 512 + n * 256, 256), 256)
            there = pl.ds(pl.multiple_of((1 - c) * 512 + n * 256, 256), 256)
            weights = W1[:, :, :, :, cols].reshape(512, 256)
            SP[:, cols] = dot(F[...].reshape(768, 512), weights)

            @pl.loop(0, 12)
            def _(i):
                rows = pl.ds(pl.multiple_of(i * 64, 64), 64)
                value = SP[rows, cols]
                gate = 1.0 / (1.0 + jnp.exp(-value))
                HF[rows, into] = (value * gate).astype(BF16)
                SP[rows, cols] = gate * (1.0 + value * (1.0 - gate))

            src = HF.at[:, into]
            hf_in.append(push(src, src, at(dc=1), HF.at[:, there]))

    layer_one()
    w2_second()

    def product(dz, part=None):
        for n in range(2) if part is None else (part,):
            out = dot(HF[...], W2[dz, :, pl.ds(n * 256, 256)])
            into = pl.ds(dz * 512 + n * 256, 256)
            PS[:, :, into] = out.astype(BF16).reshape(8, 96, 256)

    up, down, over = mod(y + 1, 4), mod(y - 1, 4), mod(y + 2, 4)
    came_rs = {}

    def lanes(dz, part):
        if part is None:
            return pl.ds(dz * 512, 512), pl.ds(0, 512)
        return pl.ds(dz * 512 + part * 256, 256), pl.ds(part * 256, 256)

    def scatter_a(dz, part=None):
        wide, here = lanes(dz, part)
        came_rs[dz, part] = [
            push(PS.at[over * 2, :, wide], RA.at[dz, :, here], at(dy=1)),
            push(PS.at[over * 2 + 1, :, wide], RB.at[dz, :, here], at(dy=3)),
            push(PS.at[up * 2 + 1, :, wide], RL.at[dz, 1, :, here], at(dy=1)),
            push(PS.at[down * 2, :, wide], RR.at[dz, 0, :, here], at(dy=3)),
        ]

    def scatter_b(dz, part=None):
        wide, here = lanes(dz, part)
        for got, buf, row, dst, dy in (
            (came_rs[dz, part][0], RA, up * 2, RL.at[dz, 0, :, here], 1),
            (came_rs[dz, part][1], RB, down * 2 + 1, RR.at[dz, 1, :, here], 3),
        ):
            got.wait_recv()
            total = PS[row, :, wide].astype(F32) + buf[dz, :, here].astype(F32)
            PS[row, :, wide] = total.astype(BF16)
            came_rs[dz, part].append(push(PS.at[row, :, wide], dst, at(dy=dy)))

    def scatter_c(dz, part=None):
        wide, here = lanes(dz, part)
        for got in came_rs[dz, part][2:]:
            got.wait_recv()

        def total(side):
            return (
                PS[y * 2 + side, :, wide].astype(F32)
                + RL[dz, side, :, here].astype(F32)
                + RR[dz, side, :, here].astype(F32)
            )

        PS[y * 2 + 1 - zl, :, wide] = total(1 - zl).astype(BF16)
        came_rs[dz, part].append(
            push(PS.at[y * 2 + 1 - zl, :, wide], RZ.at[dz, :, here], at(dl=1))
        )
        PRE[:, wide] = total(zl)

    def scatter_d(dz, part=None):
        wide, here = lanes(dz, part)
        came_rs[dz, part][-1].wait_recv()

        @pl.loop(0, 3)
        def _(i):
            rows = pl.ds(pl.multiple_of(i * 32, 32), 32)
            value = PRE[rows, wide] + RZ[dz, rows, here].astype(F32)
            gate = 1.0 / (1.0 + jnp.exp(-value))
            H2[rows, wide] = (value * gate).astype(BF16)
            SL2[rows, wide] = gate * (1.0 + value * (1.0 - gate))

    for got in hf_in:
        got.wait_recv()
    w2_rest(0)
    product(0)
    scatter_a(0)
    w2_across(3)
    w2_across(1)
    w2_third()
    scatter_b(0)

    def transposes():
        @pl.loop(0, 4)
        def _(n):
            cols = pl.ds(pl.multiple_of(n * 256, 256), 256)
            HFT[cols, :] = HF[:, cols].astype(F32).T.astype(BF16)

        @pl.loop(0, 2)
        def _(n):
            cols = pl.ds(pl.multiple_of(n * 256, 256), 256)
            FT[cols, :] = F[:, :, cols].reshape(768, 256).astype(F32).T.astype(BF16)

    transposes()
    w2_rest(3)
    product(3)
    scatter_a(3)
    scatter_c(0)
    w2_rest(1)
    product(1)
    scatter_a(1)
    scatter_b(3)
    w2_across(2)
    for copy in wh_in:
        copy.wait_recv()
    for dz in range(4):
        for dx in range(4):
            mm = mod(x + dx, 4) * 4 + mod(zh + dz, 4)
            group, pair = lax.div(mm, 2), lax.rem(mm, 2)
            even, odd = (
                jnp.where(c == 0, WHB[group, :, lane(2 * p)], WHB[group, :, lane(2 * p + 1)])
                for p in (0, 1)
            )
            WH[:, lane(dz * 4 + dx)] = jnp.where(pair == 0, even, odd).astype(BF16)
    scatter_d(0)
    scatter_b(1)
    w2_rest(2, ((1, 0),))
    product(2, 0)
    scatter_a(2, 0)
    w2_rest(2, ((3, 1), (2, 0), (2, 1)))
    product(2, 1)
    scatter_a(2, 1)
    scatter_c(3)
    scatter_c(1)
    scatter_d(3)
    scatter_b(2, 0)
    scatter_b(2, 1)
    scatter_d(1)
    scatter_c(2, 0)
    scatter_c(2, 1)
    scatter_d(2, 0)
    scatter_d(2, 1)

    own_values = dot(WH[...], H2[...], ((1,), (1,)))
    V[c, r] = jnp.concatenate([own_values, blank], axis=1)
    v_in = []
    for dc, dy, dl in peers[1:]:
        src_r = mod(y - dy, 4) * 2 + mod(zl - dl, 2)
        v_in.append(
            push(V.at[c, r], V.at[c, r], at(dc=dc, dy=dy, dl=dl), V.at[mod(c - dc, 2), src_r])
        )
    v_out, v_next = [], []
    for dc, dy, dl in peers:
        k = link.take()
        src_r = mod(y - dy, 4) * 2 + mod(zl - dl, 2)
        v_out.append(
            link.make(V.at[c, r], V.at[c, 8 + lax.rem(r, 4)], beside(-1, dc, dy, dl), k)
        )
        land = V.at[mod(c - dc, 2), 8 + lax.rem(src_r, 4)]
        v_next.append((src_r, link.make(land, land, beside(-1, dc, dy, dl), k)))

    @pl.when(r < 4)
    def _():
        for copy in v_out:
            copy.start()

    re_in.wait_recv()
    link.make(RE.at[2], RE.at[2], at(dc=1), re_sem[0], re_sem[0]).wait_recv()
    shape = (8, 12 * 128)
    place = lax.rem(lax.broadcasted_iota(jnp.int32, shape, 1), 128)

    def ahead(array, steps):
        return pltpu.roll(array, shape[1] - steps, 1)

    def following(array):
        return jnp.where(place == 95, ahead(array, 33), ahead(array, 1))

    def row_of(kind):
        return jnp.concatenate([RE[i // 4, kind, i % 4] for i in range(12)], axis=1)

    reward, number = row_of(0), row_of(1)
    head_row = lax.broadcasted_iota(jnp.int32, (8, 128), 0)

    def spread(array):
        out = jnp.zeros((8, 128), F32)
        for k in range(8):
            out = jnp.where(head_row == k, array[k], out)
        return out

    rate, decay = spread(discount_in), spread(trace_in)
    discount = jnp.concatenate([rate] * 12, axis=1)
    both = jnp.concatenate([rate * decay] * 12, axis=1)
    keep = jnp.where(following(number) == number, 1.0, 0.0)
    real = place < 96
    factor = jnp.where(real, both * keep, 1.0)
    scale = discount * keep

    for copy in v_in:
        copy.wait_recv()
    for src_r, copy in v_next:

        @pl.when(src_r < 4)
        def _():
            copy.wait_recv()

    value = jnp.concatenate([V[0, i] + V[1, i] for i in range(12)], axis=1)
    total = jnp.where(real, reward + scale * following(value) - value, 0.0)
    step = 1
    while step < shape[1]:
        total = total + factor * ahead(total, step)
        factor = factor * ahead(factor, step)
        step *= 2
    for i in range(12):
        ADV[i] = total[:, i * 128 : (i + 1) * 128]

    own = ADV[r]
    slope_t = (-own[:, :96]).astype(BF16)
    slope = (-own).T[:96, :].astype(BF16)
    own_rows = S.at[r]

    def slope_chunk(dz):
        at_dz = pl.ds(dz * 512, 512)
        own_rows[:, at_dz] = (dot(slope, WH[:, at_dz]) * SL2[:, at_dz]).astype(BF16)

    ag = {}
    pair_r = y * 2 + 1 - zl

    def gather_a(dz, part=None):
        wide, _ = lanes(dz, part)
        src = S.at[r, :, wide]
        ag[dz, part] = {
            "pair": push(src, src, at(dl=1), S.at[pair_r, :, wide]),
            "down": push(src, src, at(dy=1), S.at[down * 2 + zl, :, wide]),
            "up": push(src, src, at(dy=3), S.at[up * 2 + zl, :, wide]),
        }

    def gather_b(dz, part=None):
        wide, _ = lanes(dz, part)
        got = ag[dz, part]
        got["pair"].wait_recv()
        src = S.at[pair_r, :, wide]
        got["down2"] = push(src, src, at(dy=1), S.at[down * 2 + 1 - zl, :, wide])
        got["up2"] = push(src, src, at(dy=3), S.at[up * 2 + 1 - zl, :, wide])

    def gather_c(dz, part=None):
        wide, _ = lanes(dz, part)
        got = ag[dz, part]
        for name in ("down", "up", "down2", "up2"):
            got[name].wait_recv()
        low, high = S.at[down * 2, :, wide], S.at[up * 2 + 1, :, wide]
        got["far"] = [
            push(low, low, at(dy=1), S.at[over * 2, :, wide]),
            push(high, high, at(dy=3), S.at[over * 2 + 1, :, wide]),
        ]

    def gather_d(dz, part=None):
        for got in ag[dz, part]["far"]:
            got.wait_recv()

    def grad_part(dz, part):
        wide, here = lanes(dz, part)

        @pl.loop(0, 2)
        def _(n):
            rows = pl.ds(pl.multiple_of(n * 512, 512), 512)
            G2[dz, rows, here] = dot(HFT[rows, :], S[:, :, wide].reshape(768, 256)).astype(BF16)

    def grad_second(dz, side):
        at_dz = pl.ds(dz * 512, 512)

        @pl.loop(0, 2)
        def _(n):
            rows = pl.ds(pl.multiple_of(side * 512 + n * 256, 256), 256)
            G2[dz, rows, :] = dot(HFT[rows, :], S[:, :, at_dz].reshape(768, 512)).astype(BF16)

    def back_first(dz, start):
        at_dz = pl.ds(dz * 512, 512)

        @pl.loop(0, 4)
        def _(n):
            cols = pl.ds(pl.multiple_of(n * 256, 256), 256)
            part = dot(S[:, :, at_dz].reshape(768, 512), W2[dz, cols, :], ((1,), (1,)))
            BACK[:, cols] = part if start else BACK[:, cols] + part

    gx, halves = {}, (LOW, HIGH)

    def reduce_far(dz, side):
        src = G2.at[dz, halves[side], lane(2)]
        gx[dz, side] = [push(src, (XA, XB)[side].at[dz], at(dx=(1, 3)[side]))]

    def reduce_near(dz, side):
        src = G2.at[dz, halves[side], lane((3, 1)[side])]
        gx[dz, side].append(push(src, (XR, XL)[side].at[dz, side], at(dx=(3, 1)[side])))

    def reduce_a(dz, side):
        reduce_far(dz, side)
        reduce_near(dz, side)

    def reduce_b(dz, side):
        gx[dz, side][0].wait_recv()
        dx, half = (1, 3)[side], halves[side]
        block = G2[dz, half, lane(dx)].astype(F32) + (XA, XB)[side][dz].astype(F32)
        G2[dz, half, lane(dx)] = block.astype(BF16)
        src = G2.at[dz, half, lane(dx)]
        gx[dz, side].append(push(src, (XL, XR)[side].at[dz, side], at(dx=dx)))

    def reduce_c(dz, side, into=None):
        half = halves[side]
        for got in gx[dz, side][1:]:
            got.wait_recv()
        block = (
            G2[dz, half, lane(0)].astype(F32)
            + XL[dz, side].astype(F32)
            + XR[dz, side].astype(F32)
        )
        if into is None:
            G2[dz, half, lane(0)] = block.astype(BF16)
        else:
            into[half, :] = block

    z_far, z_in = [], []

    def reduce_z(dz, side):
        half = halves[side]
        src = G2.at[dz, half, lane(0)]
        if dz == 2:
            z_far.append(push(src, (ZA, ZB)[side], at(dz=(1, 3)[side])))
            return
        if (dz, side) in ((1, 0), (3, 1)):
            z_far[side].wait_recv()
            block = G2[dz, half, lane(0)].astype(F32) + (ZA, ZB)[side][...].astype(F32)
            G2[dz, half, lane(0)] = block.astype(BF16)
        z_in.append(push(src, (ZL if dz == 1 else ZR).at[side], at(dz=dz)))

    slope_chunk(2)
    gather_a(2, 1)
    gather_a(2, 0)
    slope_chunk(1)
    gather_a(1)
    slope_chunk(3)
    slope_chunk(0)
    gather_b(2, 1)
    gather_b(2, 0)
    gather_a(3)

    for i in range(4):
        adv_o[i] = ADV[4 * c + i]
    small = lax.broadcasted_iota(jnp.int32, (8, 128), 1) < 96
    own_loss = jnp.where(small, own * own, 0.0)
    head = dot(slope_t, H2[...])
    for dz in range(4):
        for dx in range(4):
            mm = mod(x + dx, 4) * 4 + mod(zh + dz, 4)
            GHP[lax.div(mm, 2), lax.rem(mm, 2)] = head[:, (dz * 4 + dx) * 128 :][:, :128]
    for g in range(8):
        GHP[g, 2] = own_loss
    gather_c(2, 1)
    gather_c(2, 0)
    gather_b(1)
    gather_a(0)
    gh_in = []
    for dc, dy, dl in peers[1:8]:
        to_j = mod(zl + dl, 2) * 4 + mod(y + dy, 4)
        from_j = mod(zl - dl, 2) * 4 + mod(y - dy, 4)
        gh_in.append(push(GHP.at[to_j], GR.at[j], at(dy=dy, dl=dl), GR.at[from_j]))
    GR[j] = GHP[j]
    gather_d(2, 1)
    grad_part(2, 1)
    reduce_far(2, 0)
    reduce_far(2, 1)
    reduce_near(2, 0)
    gather_d(2, 0)
    grad_part(2, 0)
    reduce_near(2, 1)
    gather_c(1)
    gather_b(3)
    gather_b(0)
    back_first(2, True)
    reduce_b(2, 0)
    reduce_b(2, 1)
    gather_d(1)
    grad_second(1, 1)
    reduce_a(1, 1)
    grad_second(1, 0)
    reduce_a(1, 0)
    gather_c(3)
    back_first(1, False)
    gather_c(0)
    reduce_b(1, 1)
    gather_d(3)
    grad_second(3, 0)
    reduce_a(3, 0)
    grad_second(3, 1)
    reduce_a(3, 1)
    reduce_b(1, 0)
    reduce_c(2, 0)
    reduce_z(2, 0)
    reduce_c(2, 1)
    reduce_z(2, 1)
    back_first(3, False)
    gather_d(0)
    back_first(0, False)

    @pl.loop(0, 12)
    def _(i):
        rows = pl.ds(pl.multiple_of(i * 64, 64), 64)
        BKS[rows, :] = BACK[rows, theirs].astype(BF16)

    back_in = push(BKS, BKR, at(dc=1))
    reduce_b(3, 0)
    reduce_b(3, 1)
    grad_second(0, 0)
    grad_second(0, 1)
    back_in.wait_recv()

    @pl.loop(0, 12)
    def _(i):
        rows = pl.ds(pl.multiple_of(i * 64, 64), 64)
        back = BACK[rows, mine] + BKR[rows, :].astype(F32)
        SF[rows, :] = (back * SP[rows, :]).astype(BF16)

    @pl.loop(0, 2)
    def _(n):
        rows = pl.ds(pl.multiple_of(n * 256, 256), 256)
        part = dot(FT[rows, :], SF[...]).astype(BF16)
        G1[pl.ds(2 * n, 2)] = part.reshape(2, 4, 32, 512)

    lo, hi = pl.ds(0, 16), pl.ds(16, 16)
    x1, x3, x2 = mod(x + 1, 4), mod(x - 1, 4), mod(x + 2, 4)
    z1, z3, z2 = mod(zh + 1, 4), mod(zh - 1, 4), mod(zh + 2, 4)
    yin = [
        push(G1.at[x2, :, lo], YA, at(dx=1)),
        push(G1.at[x2, :, hi], YB, at(dx=3)),
        push(G1.at[x1, :, hi], YL.at[1], at(dx=1)),
        push(G1.at[x3, :, lo], YR.at[0], at(dx=3)),
    ]
    reduce_a(0, 0)
    reduce_a(0, 1)
    reduce_c(1, 1)
    reduce_z(1, 1)
    reduce_c(1, 0)
    reduce_z(1, 0)
    reduce_c(3, 0)
    reduce_z(3, 0)

    def sums_y():
        for got, buf, row, half, dst, dx in (
            (yin[0], YA, x1, lo, YL.at[0], 1),
            (yin[1], YB, x3, hi, YR.at[1], 3),
        ):
            got.wait_recv()
            block = G1[row, :, half].astype(F32) + buf[...].astype(F32)
            G1[row, :, half] = block.astype(BF16)
            yin.append(push(G1.at[row, :, half], dst, at(dx=dx)))

    sums_y()
    for got in gh_in:
        got.wait_recv()
    GS[...] = functools.reduce(jnp.add, [GR[i] for i in range(8)])
    gz_in = [push(GS, GZ.at[d - 1], at(dz=d)) for d in (1, 2, 3)]
    reduce_c(3, 1)
    reduce_z(3, 1)
    for got in yin[2:]:
        got.wait_recv()
    for side, half in ((0, lo), (1, hi)):
        block = G1[x, :, half].astype(F32) + YL[side].astype(F32) + YR[side].astype(F32)
        G1[x, :, half] = block.astype(BF16)
    uin = [
        push(G1.at[x, z2, lo], UA, at(dz=1)),
        push(G1.at[x, z2, hi], UB, at(dz=3)),
        push(G1.at[x, z1, hi], UL.at[1], at(dz=1)),
        push(G1.at[x, z3, lo], UR.at[0], at(dz=3)),
    ]
    reduce_b(0, 0)
    reduce_b(0, 1)
    for got in gz_in:
        got.wait_recv()
    GY[...] = GS[...] + GZ[0] + GZ[1] + GZ[2]
    gxs_in = [push(GY, GX.at[d - 1], at(dx=d)) for d in (1, 2, 3)]
    for got, buf, row, half, dst, dz in (
        (uin[0], UA, z1, lo, UL.at[0], 1),
        (uin[1], UB, z3, hi, UR.at[1], 3),
    ):
        got.wait_recv()
        block = G1[x, row, half].astype(F32) + buf[...].astype(F32)
        G1[x, row, half] = block.astype(BF16)
        uin.append(push(G1.at[x, row, half], dst, at(dz=dz)))
    for got in gxs_in:
        got.wait_recv()
    heads = GY[...] + GX[0] + GX[1] + GX[2]
    GH[...] = heads
    gc_in = push(GH, GC, at(dc=1))
    for got in uin[2:]:
        got.wait_recv()
    for side, half in ((0, lo), (1, hi)):
        GF[side] = (
            G1[x, zh, half].astype(F32) + UL[side].astype(F32) + UR[side].astype(F32)
        )
    gt_in = push(GF.at[1 - c], GT, at(dc=1))
    gc_in.wait_recv()
    other = GC[...]
    loss_o[...] = jnp.broadcast_to(jnp.sum(heads[2]), (8, 128))
    for i in range(2):
        gh_o[:, lane(2 * i)] = jnp.where(c == 0, heads[i], other[i])
        gh_o[:, lane(2 * i + 1)] = jnp.where(c == 0, other[i], heads[i])
    reduce_c(0, 0, g2_o)
    reduce_c(0, 1, g2_o)
    for got in z_in:
        got.wait_recv()
    for side, half in ((0, LOW), (1, HIGH)):
        g2_o[half, :] = g2_o[half, :] + ZL[side].astype(F32) + ZR[side].astype(F32)
    gt_in.wait_recv()
    kept, brought = GF[c], GT[...]
    g1_o[:, LOW] = jnp.where(c == 0, kept, brought)
    g1_o[:, HIGH] = jnp.where(c == 0, brought, kept)

    link.drain()

    @pl.when(c == 0)
    def _():
        for copy in re_to:
            copy.wait_send()

    @pl.when(r < 4)
    def _():
        for copy in v_out:
            copy.wait_send()


SCRATCH = [
    ((2, 384, 512), BF16), ((512, 768), BF16), ((4, 4, 2, 16, 512), BF16),
    ((4, 1024, 512), BF16), ((8, 8, 512), F32), ((8, 2048), BF16), ((3, 2, 4, 8, 128), F32),
    ((768, 1024), BF16), ((1024, 768), BF16), ((768, 512), F32), ((8, 96, 2048), BF16),
    ((4, 96, 512), BF16), ((4, 96, 512), BF16), ((4, 2, 96, 512), BF16),
    ((4, 2, 96, 512), BF16), ((4, 96, 512), BF16), ((96, 2048), F32), ((96, 2048), F32),
    ((96, 2048), BF16), ((2, 12, 8, 128), F32), ((12, 8, 128), F32), ((8, 96, 2048), BF16),
    ((768, 1024), F32), ((4, 1024, 512), BF16), ((4, 512, 128), BF16), ((4, 512, 128), BF16),
    ((4, 2, 512, 128), BF16), ((4, 2, 512, 128), BF16), ((512, 128), BF16),
    ((512, 128), BF16), ((2, 512, 128), BF16), ((2, 512, 128), BF16), ((768, 512), BF16),
    ((768, 512), BF16), ((768, 512), BF16), ((4, 4, 32, 512), BF16), ((4, 16, 512), BF16),
    ((4, 16, 512), BF16), ((2, 4, 16, 512), BF16), ((2, 4, 16, 512), BF16), ((16, 512), BF16),
    ((16, 512), BF16), ((2, 16, 512), BF16), ((2, 16, 512), BF16), ((2, 16, 512), F32),
    ((16, 512), F32), ((8, 3, 8, 128), F32), ((8, 3, 8, 128), F32), ((3, 8, 128), F32),
    ((3, 3, 8, 128), F32), ((3, 3, 8, 128), F32), ((3, 8, 128), F32), ((3, 8, 128), F32),
    ((3, 8, 128), F32), ((8, 512), BF16), ((8, 384), F32), ((1, 384), jnp.int32),
    ((16, 1024), BF16),
]


def finish(adv, loss, g1, g2, gh, adv_o, loss_o, g1_o, g2_o, gh_o):
    adv_o[...] = jnp.concatenate([adv[i][:, :96] for i in range(4)], axis=1)
    loss_o[0, 0] = loss[0, 0] * (0.5 / 98304)
    g1_o[...] = g1[...]
    g2_o[...] = g2[...]
    gh_o[...] = gh[...]


def shards(features, w_first, w_second, w_head, rewards, discount, trace, episode):
    vmem = pl.BlockSpec(memory_space=pltpu.VMEM)
    smem = pl.BlockSpec(memory_space=pltpu.SMEM)
    hbm = pl.BlockSpec(memory_space=pltpu.HBM)
    shapes = ((16, 1024), (1024, 128), (8, 512))
    parts = pl.pallas_call(
        kernel,
        out_shape=[
            jax.ShapeDtypeStruct(shape, F32) for shape in ((4, 8, 128), (8, 128), *shapes)
        ],
        in_specs=[hbm] * 6 + [smem] * 2,
        out_specs=[vmem] * 5,
        scratch_shapes=[pltpu.VMEM(shape, kind) for shape, kind in SCRATCH]
        + [pltpu.SemaphoreType.DMA((count,)) for count in (SLOTS, SLOTS, 6)],
        compiler_params=pltpu.CompilerParams(
            collective_id=0, has_side_effects=True, vmem_limit_bytes=62 * 2**20
        ),
    )(
        features, w_first, w_second, w_head.T, rewards, episode.reshape(1, -1),
        discount, trace,
    )
    advantages, loss, grad_first, grad_second, grad_head = pl.pallas_call(
        finish,
        out_shape=[
            jax.ShapeDtypeStruct(shape, F32) for shape in ((8, 384), (1, 1), *shapes)
        ],
        in_specs=[vmem, smem, vmem, vmem, vmem],
        out_specs=[vmem, smem, vmem, vmem, vmem],
    )(*parts)
    return advantages, loss[0, 0], grad_first, grad_second, grad_head.T


def solution(mesh):
    placed = (
        P("batch", None),
        P("batch", "hidden"),
        P("hidden", "batch"),
        P("hidden", None),
        P(None, "batch"),
        P(),
        P(),
        P("batch"),
    )
    return jax.shard_map(
        shards,
        mesh=mesh,
        in_specs=placed,
        out_specs=(
            P(None, "batch"),
            P(),
            P("batch", "hidden"),
            P("hidden", "batch"),
            P("hidden", None),
        ),
        check_vma=False,
    )
```

```python
import functools

import jax
import jax.numpy as jnp
from jax import lax
from jax.experimental import pallas as pl
from jax.experimental.pallas import tpu as pltpu
from jax.sharding import PartitionSpec as P

BF16, F32 = jnp.bfloat16, jnp.float32
MESH = pl.DeviceIdType.MESH
SLOTS, RING = 195, 64
EDGE = 192
HALF = (1024 - EDGE) // 2
LOW, HIGH = pl.ds(0, HALF), pl.ds(HALF, HALF)
TOP = pl.ds(2 * HALF, EDGE)
TOPS = (pl.ds(2 * HALF, EDGE // 2), pl.ds(2 * HALF + EDGE // 2, EDGE // 2))


def dot(left, right, dims=((1,), (0,))):
    return lax.dot_general(left, right, (dims, ((), ())), preferred_element_type=F32)


def mod(value, count):
    return lax.rem(value + count, count)


def lane(dx):
    return pl.ds(dx * 128, 128)


class Links:
    def __init__(self, sent, came):
        self.sent, self.came, self.used, self.open = sent, came, 0, []

    def take(self):
        self.used += 1
        return self.used - 1

    def make(self, src, dst, to, k, k_sent):
        return pltpu.make_async_remote_copy(
            src_ref=src,
            dst_ref=dst,
            send_sem=self.sent.at[k_sent],
            recv_sem=self.came.at[k],
            device_id=to,
            device_id_type=MESH,
        )

    def push(self, src, dst, to, land=None, k=None):
        k = self.take() if k is None else k
        turn = len(self.open)
        if turn >= RING:
            self.open[turn - RING].wait_send()
        copy = self.make(src, dst, to, k, turn % RING)
        copy.start()
        self.open.append(copy)
        return copy if land is None else self.make(land, land, to, k, 0)

    def drain(self):
        for copy in self.open[-RING:]:
            copy.wait_send()


def kernel(
    feat, w1in, w2in, whin, reward_in, number_in, discount_in, trace_in,
    adv_o, loss_o, g1_o, g2_o, gh_o,
    F, FT, W1, W2, WHB, WH, RE, HF, HFT, SP, PS, RA, RB, RL, RR, RZ, PRE, SL2, H2,
    V, ADV, S, BACK, G2, XA, XB, XL, XR, ZA, ZB, ZL, ZR, BKS, BKR, SF,
    G1, YA, YB, YL, YR, UA, UB, UL, UR, GF, GT, GHP, GR, GS, GZ, GX, GY, GC, GH,
    WHS, RWS, EPS, WIN, EZF, EZL, EZR, EXF, EXL, EXR, sent, came, local,
):
    b, j = lax.axis_index("batch"), lax.axis_index("hidden")
    c, m = lax.rem(b, 2), lax.div(b, 2)
    zh, x = lax.rem(m, 4), lax.div(m, 4)
    y, zl = lax.rem(j, 4), lax.div(j, 4)
    r = y * 2 + zl
    link = Links(sent, came)
    push = link.push

    def at(dx=0, dz=0, dc=0, dy=0, dl=0):
        bb = (mod(x + dx, 4) * 4 + mod(zh + dz, 4)) * 2 + mod(c + dc, 2)
        return bb, mod(zl + dl, 2) * 4 + mod(y + dy, 4)

    def beside(step, dc, dy, dl):
        bb = mod(m + step, 16) * 2 + mod(c + dc, 2)
        return bb, mod(zl + dl, 2) * 4 + mod(y + dy, 4)

    peers = [(dc, dy, dl) for dc in range(2) for dy in range(4) for dl in range(2)]

    loads = [
        pltpu.make_async_copy(src, dst, local.at[k])
        for k, (src, dst) in enumerate(
            (
                (w1in, WIN),
                (w2in, W2.at[0, :, lane(0)]),
                (feat, F.at[c]),
                (whin, WHS),
                (reward_in, RWS),
                (number_in, EPS),
            )
        )
    ]
    for load in loads:
        load.start()

    barrier = pltpu.get_barrier_semaphore()
    partners = [at(dc=dc, dy=dy, dl=dl) for dc, dy, dl in peers[1:]]
    partners += [at(dx=d) for d in (1, 2, 3)] + [at(dz=d) for d in (1, 2, 3)]
    partners += [beside(step, *peer) for step in (1, -1) for peer in peers]
    for partner in partners:
        pl.semaphore_signal(barrier, inc=1, device_id=partner, device_id_type=MESH)
    for load in loads:
        load.wait()
    blank = jnp.zeros((8, 32), F32)
    WHB[j] = WHS[...].astype(F32)
    for i in range(4):
        reward = RWS[:, i * 96 : (i + 1) * 96]
        number = jnp.broadcast_to(EPS[:, i * 96 : (i + 1) * 96].astype(F32), (8, 96))
        RE[c, 0, i] = jnp.concatenate([reward, blank], axis=1)
        RE[c, 1, i] = jnp.concatenate([number, blank], axis=1)
    pl.semaphore_wait(barrier, len(partners))

    mine, theirs = (
        pl.ds(pl.multiple_of(side * 512, 512), 512) for side in (c, 1 - c)
    )
    w1pair = push(WIN.at[:, theirs], W1.at[x, zh, c], at(dc=1), W1.at[x, zh, 1 - c])
    W1[x, zh, c] = WIN[:, mine]

    def w1_sides(zs):
        own = W1.at[x, zs]
        return [push(own, own, at(dx=dx), W1.at[mod(x - dx, 4), zs]) for dx in (1, 3)]

    def w1_across(zs, sides):
        out = []
        for dx, side in ((1, 0), (3, 1)):
            sides[side].wait_recv()
            part = W1.at[mod(x - dx, 4), zs, side]
            out.append(push(part, part, at(dx=dx), W1.at[mod(x + 2, 4), zs, side]))
        return out

    w2x = {}

    def w2_to(dz, half, dx):
        key = (dz, 4 - dx, 0 if half is LOW else 1)
        w2x[key] = push(
            W2.at[dz, half, lane(0)], W2.at[dz, half, lane(4 - dx)], at(dx=dx)
        )

    def w2_side(dz, half):
        near = 1 if half is LOW else 3
        w2_to(dz, half, near)
        w2_to(dz, half, 4 - near)

    def w2_across(dz):
        w2x[dz, 3, 0].wait_recv()
        w2x[dz, 2, 0] = push(
            W2.at[dz, LOW, lane(3)], W2.at[dz, LOW, lane(2)], at(dx=1)
        )
        w2x[dz, 1, 1].wait_recv()
        w2x[dz, 2, 1] = push(
            W2.at[dz, HIGH, lane(1)], W2.at[dz, HIGH, lane(2)], at(dx=3)
        )

    def w2_rest(dz, keys=((3, 1), (1, 0), (2, 0), (2, 1))):
        for key in keys:
            w2x[(dz, *key)].wait_recv()

    def w2_z(half, dz):
        return push(W2.at[0, half, lane(0)], W2.at[4 - dz, half, lane(0)], at(dz=dz))

    first, second, w1z, w1x, w1far = [], [], {}, {}, {}

    def w1_start():
        w1pair.wait_recv()
        own = W1.at[x, zh]
        for dz in (1, 3, 2):
            w1z[dz] = push(own, own, at(dz=dz), W1.at[x, mod(zh - dz, 4)])
        w1x[0] = w1_sides(zh)

    def w1_from_z(dz):
        w1z[dz].wait_recv()
        w1x[dz] = w1_sides(mod(zh - dz, 4))

    def w1_far(dz):
        w1far[dz] = w1_across(mod(zh - dz, 4), w1x[dz])

    def w1_done():
        for dz in (0, 1, 3, 2):
            for copy in w1far[dz]:
                copy.wait_recv()

    edge = {}

    def edge_x1():
        src = W2.at[0, TOP, lane(0)]
        edge["x3"] = push(src, W2.at[0, TOP, lane(3)], at(dx=1))
        edge["x1"] = push(src, W2.at[0, TOP, lane(1)], at(dx=3))

    def edge_x2():
        edge["x3"].wait_recv()
        src = W2.at[0, TOPS[0], lane(3)]
        edge["x2"] = [push(src, W2.at[0, TOPS[0], lane(2)], at(dx=1))]
        edge["x1"].wait_recv()
        src = W2.at[0, TOPS[1], lane(1)]
        edge["x2"].append(push(src, W2.at[0, TOPS[1], lane(2)], at(dx=3)))

    def edge_z1():
        for got in edge["x2"]:
            got.wait_recv()
        src = W2.at[0, TOP]
        edge["z3"] = push(src, W2.at[3, TOP], at(dz=1))
        edge["z1"] = push(src, W2.at[1, TOP], at(dz=3))

    edge["z2"] = []

    def edge_z2(dz):
        edge["z3" if dz == 3 else "z1"].wait_recv()
        half = TOPS[0 if dz == 3 else 1]
        edge["z2"].append(push(W2.at[dz, half], W2.at[2, half], at(dz=4 - dz)))

    w1_start()
    edge_x1()
    w2_to(0, LOW, 1)
    w2_to(0, HIGH, 3)
    first += [w2_z(LOW, 1), w2_z(HIGH, 3)]
    feat_in = push(F.at[c], F.at[c], at(dc=1), F.at[1 - c])
    w1_from_z(1)
    w2_to(0, HIGH, 1)
    w2_to(0, LOW, 3)
    w1_from_z(3)
    w1_far(0)
    edge_x2()
    w1_from_z(2)
    second += [w2_z(HIGH, 1), w2_z(LOW, 3)]
    re_in = push(RE.at[c], RE.at[c], at(dc=1), RE.at[1 - c])
    re_sem = link.take()
    re_to = [
        link.make(RE.at[c], RE.at[2], beside(-1, dc, 0, 0), re_sem, RING + dc)
        for dc in range(2)
    ]

    @pl.when(c == 0)
    def _():
        for copy in re_to:
            copy.start()

    wh_sem = link.take()
    for dc, dy, dl in peers[1:8]:
        push(WHB.at[j], WHB.at[j], at(dy=dy, dl=dl), k=wh_sem)
    wh_all = WHB.at[pl.ds(0, 7)]
    wh_in = [link.make(wh_all, wh_all, at(dc=1), wh_sem, 0)]

    w1_far(1)
    edge_z1()
    w1_far(3)
    w1_far(2)
    w2_across(0)
    w2_z2 = []

    def w2_first():
        first[0].wait_recv()
        w2_z2.append(push(W2.at[3, LOW, lane(0)], W2.at[2, LOW, lane(0)], at(dz=1)))
        w2_side(3, LOW)
        first[1].wait_recv()
        w2_z2.append(push(W2.at[1, HIGH, lane(0)], W2.at[2, HIGH, lane(0)], at(dz=3)))
        w2_side(1, HIGH)

    def w2_second():
        second[0].wait_recv()
        w2_side(3, HIGH)
        second[1].wait_recv()
        w2_side(1, LOW)

    def w2_third():
        w2_z2[0].wait_recv()
        w2_side(2, LOW)
        w2_z2[1].wait_recv()
        w2_side(2, HIGH)

    w2_first()
    feat_in.wait_recv()
    w1_done()
    hf_in = []

    def layer_one():
        for n in range(2):
            cols = pl.ds(n * 256, 256)
            into = pl.ds(pl.multiple_of(c * 512 + n * 256, 256), 256)
            there = pl.ds(pl.multiple_of((1 - c) * 512 + n * 256, 256), 256)
            weights = W1[:, :, :, :, cols].reshape(512, 256)
            SP[:, cols] = dot(F[...].reshape(768, 512), weights)

            @pl.loop(0, 12)
            def _(i):
                rows = pl.ds(pl.multiple_of(i * 64, 64), 64)
                value = SP[rows, cols]
                gate = 1.0 / (1.0 + jnp.exp(-value))
                HF[rows, into] = (value * gate).astype(BF16)
                SP[rows, cols] = gate * (1.0 + value * (1.0 - gate))

            src = HF.at[:, into]
            hf_in.append(push(src, src, at(dc=1), HF.at[:, there]))

    layer_one()
    w2_second()

    def product(dz, part=None):
        for n in range(2) if part is None else (part,):
            out = dot(HF[...], W2[dz, :, pl.ds(n * 256, 256)])
            into = pl.ds(dz * 512 + n * 256, 256)
            PS[:, :, into] = out.astype(BF16).reshape(8, 96, 256)

    up, down, over = mod(y + 1, 4), mod(y - 1, 4), mod(y + 2, 4)
    came_rs = {}

    def lanes(dz, part):
        if part is None:
            return pl.ds(dz * 512, 512), pl.ds(0, 512)
        return pl.ds(dz * 512 + part * 256, 256), pl.ds(part * 256, 256)

    def scatter_a(dz, part=None):
        wide, here = lanes(dz, part)
        came_rs[dz, part] = [
            push(PS.at[over * 2, :, wide], RA.at[dz, :, here], at(dy=1)),
            push(PS.at[over * 2 + 1, :, wide], RB.at[dz, :, here], at(dy=3)),
            push(PS.at[up * 2 + 1, :, wide], RL.at[dz, 1, :, here], at(dy=1)),
            push(PS.at[down * 2, :, wide], RR.at[dz, 0, :, here], at(dy=3)),
        ]

    def scatter_b(dz, part=None):
        wide, here = lanes(dz, part)
        for got, buf, row, dst, dy in (
            (came_rs[dz, part][0], RA, up * 2, RL.at[dz, 0, :, here], 1),
            (came_rs[dz, part][1], RB, down * 2 + 1, RR.at[dz, 1, :, here], 3),
        ):
            got.wait_recv()
            total = PS[row, :, wide].astype(F32) + buf[dz, :, here].astype(F32)
            PS[row, :, wide] = total.astype(BF16)
            came_rs[dz, part].append(push(PS.at[row, :, wide], dst, at(dy=dy)))

    def scatter_c(dz, part=None):
        wide, here = lanes(dz, part)
        for got in came_rs[dz, part][2:]:
            got.wait_recv()

        def total(side):
            return (
                PS[y * 2 + side, :, wide].astype(F32)
                + RL[dz, side, :, here].astype(F32)
                + RR[dz, side, :, here].astype(F32)
            )

        PS[y * 2 + 1 - zl, :, wide] = total(1 - zl).astype(BF16)
        came_rs[dz, part].append(
            push(PS.at[y * 2 + 1 - zl, :, wide], RZ.at[dz, :, here], at(dl=1))
        )
        PRE[:, wide] = total(zl)

    def scatter_d(dz, part=None):
        wide, here = lanes(dz, part)
        came_rs[dz, part][-1].wait_recv()

        @pl.loop(0, 3)
        def _(i):
            rows = pl.ds(pl.multiple_of(i * 32, 32), 32)
            value = PRE[rows, wide] + RZ[dz, rows, here].astype(F32)
            gate = 1.0 / (1.0 + jnp.exp(-value))
            H2[rows, wide] = (value * gate).astype(BF16)
            SL2[rows, wide] = gate * (1.0 + value * (1.0 - gate))

    for got in hf_in:
        got.wait_recv()
    w2_rest(0)
    product(0)
    scatter_a(0)
    w2_across(3)
    w2_across(1)
    scatter_b(0)
    edge_z2(3)
    w2_rest(3)
    product(3)
    scatter_a(3)
    w2_third()
    edge_z2(1)
    w2_rest(1)
    product(1)
    scatter_a(1)
    scatter_c(0)

    def transposes():
        @pl.loop(0, 4)
        def _(n):
            cols = pl.ds(pl.multiple_of(n * 256, 256), 256)
            HFT[cols, :] = HF[:, cols].astype(F32).T.astype(BF16)

        @pl.loop(0, 2)
        def _(n):
            cols = pl.ds(pl.multiple_of(n * 256, 256), 256)
            FT[cols, :] = F[:, :, cols].reshape(768, 256).astype(F32).T.astype(BF16)

    transposes()
    scatter_b(3)
    w2_across(2)
    for copy in wh_in:
        copy.wait_recv()
    for dz in range(4):
        for dx in range(4):
            mm = mod(x + dx, 4) * 4 + mod(zh + dz, 4)
            group, pair = lax.div(mm, 2), lax.rem(mm, 2)
            even, odd = (
                jnp.where(c == 0, WHB[group, :, lane(2 * p)], WHB[group, :, lane(2 * p + 1)])
                for p in (0, 1)
            )
            WH[:, lane(dz * 4 + dx)] = jnp.where(pair == 0, even, odd).astype(BF16)
    scatter_d(0)
    scatter_b(1)
    w2_rest(2, ((1, 0),))
    for got in edge["z2"]:
        got.wait_recv()
    product(2, 0)
    scatter_a(2, 0)
    w2_rest(2, ((3, 1), (2, 0), (2, 1)))
    product(2, 1)
    scatter_a(2, 1)
    scatter_c(3)
    scatter_c(1)
    scatter_d(3)
    scatter_b(2, 0)
    scatter_b(2, 1)
    scatter_d(1)
    scatter_c(2, 0)
    scatter_c(2, 1)
    scatter_d(2, 0)
    scatter_d(2, 1)

    own_values = dot(WH[...], H2[...], ((1,), (1,)))
    own_v = V.at[c * 12 + r]
    V[c * 12 + r] = jnp.concatenate([own_values, blank], axis=1)
    v_sem = link.take()
    for dc, dy, dl in peers[1:]:
        push(own_v, own_v, at(dc=dc, dy=dy, dl=dl), k=v_sem)
    v_out = [
        link.make(
            own_v, V.at[c * 12 + 8 + lax.rem(r, 4)], beside(-1, *peer), v_sem, RING + 2 + k
        )
        for k, peer in enumerate(peers)
    ]

    @pl.when(r < 4)
    def _():
        for copy in v_out:
            copy.start()

    re_in.wait_recv()
    link.make(RE.at[2], RE.at[2], at(dc=1), re_sem, 0).wait_recv()
    shape = (8, 12 * 128)
    place = lax.rem(lax.broadcasted_iota(jnp.int32, shape, 1), 128)

    def ahead(array, steps):
        return pltpu.roll(array, shape[1] - steps, 1)

    def following(array):
        return jnp.where(place == 95, ahead(array, 33), ahead(array, 1))

    def row_of(kind):
        return jnp.concatenate([RE[i // 4, kind, i % 4] for i in range(12)], axis=1)

    reward, number = row_of(0), row_of(1)
    head_row = lax.broadcasted_iota(jnp.int32, (8, 128), 0)

    def spread(array):
        out = jnp.zeros((8, 128), F32)
        for k in range(8):
            out = jnp.where(head_row == k, array[k], out)
        return out

    rate, decay = spread(discount_in), spread(trace_in)
    discount = jnp.concatenate([rate] * 12, axis=1)
    both = jnp.concatenate([rate * decay] * 12, axis=1)
    keep = jnp.where(following(number) == number, 1.0, 0.0)
    real = place < 96
    factor = jnp.where(real, both * keep, 1.0)
    scale = discount * keep

    v_all = V.at[pl.ds(0, 23)]
    v_in = [link.make(v_all, v_all, at(dc=1), v_sem, 0)]
    for copy in v_in:
        copy.wait_recv()
    value = jnp.concatenate([V[i] + V[12 + i] for i in range(12)], axis=1)
    total = jnp.where(real, reward + scale * following(value) - value, 0.0)
    step = 1
    while step < shape[1]:
        total = total + factor * ahead(total, step)
        factor = factor * ahead(factor, step)
        step *= 2
    for i in range(12):
        ADV[i] = total[:, i * 128 : (i + 1) * 128]

    own = ADV[r]
    slope_t = (-own[:, :96]).astype(BF16)
    slope = (-own).T[:96, :].astype(BF16)
    own_rows = S.at[r]

    def slope_chunk(dz):
        at_dz = pl.ds(dz * 512, 512)
        own_rows[:, at_dz] = (dot(slope, WH[:, at_dz]) * SL2[:, at_dz]).astype(BF16)

    ag = {}
    pair_r = y * 2 + 1 - zl

    def gather_a(dz, part=None):
        wide, _ = lanes(dz, part)
        src = S.at[r, :, wide]
        ag[dz, part] = {
            "pair": push(src, src, at(dl=1), S.at[pair_r, :, wide]),
            "down": push(src, src, at(dy=1), S.at[down * 2 + zl, :, wide]),
            "up": push(src, src, at(dy=3), S.at[up * 2 + zl, :, wide]),
        }

    def gather_b(dz, part=None):
        wide, _ = lanes(dz, part)
        got = ag[dz, part]
        got["pair"].wait_recv()
        src = S.at[pair_r, :, wide]
        got["down2"] = push(src, src, at(dy=1), S.at[down * 2 + 1 - zl, :, wide])
        got["up2"] = push(src, src, at(dy=3), S.at[up * 2 + 1 - zl, :, wide])

    def gather_c(dz, part=None):
        wide, _ = lanes(dz, part)
        got = ag[dz, part]
        for name in ("down", "up", "down2", "up2"):
            got[name].wait_recv()
        low, high = S.at[down * 2, :, wide], S.at[up * 2 + 1, :, wide]
        got["far"] = [
            push(low, low, at(dy=1), S.at[over * 2, :, wide]),
            push(high, high, at(dy=3), S.at[over * 2 + 1, :, wide]),
        ]

    def gather_d(dz, part=None):
        for got in ag[dz, part]["far"]:
            got.wait_recv()

    def grad_part(dz, part):
        wide, here = lanes(dz, part)

        @pl.loop(0, 2)
        def _(n):
            rows = pl.ds(pl.multiple_of(n * 512, 512), 512)
            G2[dz, rows, here] = dot(HFT[rows, :], S[:, :, wide].reshape(768, 256)).astype(BF16)

    def grad_second(dz, side):
        at_dz = pl.ds(dz * 512, 512)

        @pl.loop(0, 2)
        def _(n):
            size = (HALF if side == 0 else HALF + EDGE) // 2
            rows = pl.ds(pl.multiple_of(side * HALF + n * size, 16), size)
            G2[dz, rows, :] = dot(HFT[rows, :], S[:, :, at_dz].reshape(768, 512)).astype(BF16)

    def back_first(dz, start):
        at_dz = pl.ds(dz * 512, 512)

        @pl.loop(0, 4)
        def _(n):
            cols = pl.ds(pl.multiple_of(n * 256, 256), 256)
            part = dot(S[:, :, at_dz].reshape(768, 512), W2[dz, cols, :], ((1,), (1,)))
            BACK[:, cols] = part if start else BACK[:, cols] + part

    gx, halves = {}, (LOW, HIGH)

    def reduce_far(dz, side):
        src = G2.at[dz, halves[side], lane(2)]
        gx[dz, side] = [push(src, (XA, XB)[side].at[dz], at(dx=(1, 3)[side]))]

    def reduce_near(dz, side):
        src = G2.at[dz, halves[side], lane((3, 1)[side])]
        gx[dz, side].append(push(src, (XR, XL)[side].at[dz, side], at(dx=(3, 1)[side])))

    def reduce_a(dz, side):
        reduce_far(dz, side)
        reduce_near(dz, side)

    def reduce_b(dz, side):
        gx[dz, side][0].wait_recv()
        dx, half = (1, 3)[side], halves[side]
        block = G2[dz, half, lane(dx)].astype(F32) + (XA, XB)[side][dz].astype(F32)
        G2[dz, half, lane(dx)] = block.astype(BF16)
        src = G2.at[dz, half, lane(dx)]
        gx[dz, side].append(push(src, (XL, XR)[side].at[dz, side], at(dx=dx)))

    def reduce_c(dz, side, into=None):
        half = halves[side]
        for got in gx[dz, side][1:]:
            got.wait_recv()
        block = (
            G2[dz, half, lane(0)].astype(F32)
            + XL[dz, side].astype(F32)
            + XR[dz, side].astype(F32)
        )
        if into is None:
            G2[dz, half, lane(0)] = block.astype(BF16)
        else:
            into[half, :] = block

    e_far, e_in, e_x = [], [], []

    def edge_far():
        for side in (0, 1):
            src = G2.at[2, TOPS[side], :]
            e_far.append(push(src, EZF.at[side], at(dz=(1, 3)[side])))

    def edge_near(dz):
        buf, near, side = (EZL, 1, 0) if dz == 1 else (EZR, 0, 1)
        e_in.append(push(G2.at[dz, TOPS[near], :], buf.at[near], at(dz=dz)))
        e_far[side].wait_recv()
        block = G2[dz, TOPS[side], :].astype(F32) + EZF[side].astype(F32)
        G2[dz, TOPS[side], :] = block.astype(BF16)
        e_in.append(push(G2.at[dz, TOPS[side], :], buf.at[side], at(dz=dz)))

    def edge_sum():
        for got in e_in:
            got.wait_recv()
        for side in (0, 1):
            block = (
                G2[0, TOPS[side], :].astype(F32)
                + EZL[side].astype(F32)
                + EZR[side].astype(F32)
            )
            G2[0, TOPS[side], :] = block.astype(BF16)
            src = G2.at[0, TOPS[side]]
            e_x.append(push(src.at[:, lane(2)], EXF.at[side], at(dx=(1, 3)[side])))
            near = (EXR, EXL)[side].at[side]
            e_x.append(push(src.at[:, lane((3, 1)[side])], near, at(dx=(3, 1)[side])))

    def edge_mid():
        for side in (0, 1):
            e_x[2 * side].wait_recv()
            dx = (1, 3)[side]
            block = G2[0, TOPS[side], lane(dx)].astype(F32) + EXF[side].astype(F32)
            G2[0, TOPS[side], lane(dx)] = block.astype(BF16)
            src = G2.at[0, TOPS[side], lane(dx)]
            e_x.append(push(src, (EXL, EXR)[side].at[side], at(dx=dx)))

    def edge_end():
        for k in (1, 3, 4, 5):
            e_x[k].wait_recv()
        for side in (0, 1):
            g2_o[TOPS[side], :] = (
                G2[0, TOPS[side], lane(0)].astype(F32)
                + EXL[side].astype(F32)
                + EXR[side].astype(F32)
            )

    z_far, z_in = [], []

    def reduce_z(dz, side):
        half = halves[side]
        src = G2.at[dz, half, lane(0)]
        if dz == 2:
            z_far.append(push(src, (ZA, ZB)[side], at(dz=(1, 3)[side])))
            return
        if (dz, side) in ((1, 0), (3, 1)):
            z_far[side].wait_recv()
            block = G2[dz, half, lane(0)].astype(F32) + (ZA, ZB)[side][...].astype(F32)
            G2[dz, half, lane(0)] = block.astype(BF16)
        z_in.append(push(src, (ZL if dz == 1 else ZR).at[side], at(dz=dz)))

    slope_chunk(2)
    gather_a(2, 1)
    gather_a(2, 0)
    slope_chunk(1)
    gather_a(1)
    slope_chunk(3)
    slope_chunk(0)
    gather_b(2, 1)
    gather_b(2, 0)
    gather_a(3)

    for i in range(4):
        adv_o[i] = ADV[4 * c + i]
    small = lax.broadcasted_iota(jnp.int32, (8, 128), 1) < 96
    own_loss = jnp.where(small, own * own, 0.0)
    head = dot(slope_t, H2[...])
    for dz in range(4):
        for dx in range(4):
            mm = mod(x + dx, 4) * 4 + mod(zh + dz, 4)
            GHP[lax.div(mm, 2), lax.rem(mm, 2)] = head[:, (dz * 4 + dx) * 128 :][:, :128]
    for g in range(8):
        GHP[g, 2] = own_loss
    gather_c(2, 1)
    gather_c(2, 0)
    gather_b(1)
    gather_a(0)
    gh_sem, gh_all = link.take(), GR.at[pl.ds(0, 7)]
    for dc, dy, dl in peers[1:8]:
        to_j = mod(zl + dl, 2) * 4 + mod(y + dy, 4)
        push(GHP.at[to_j], GR.at[j], at(dy=dy, dl=dl), k=gh_sem)
    gh_in = [link.make(gh_all, gh_all, at(dc=1), gh_sem, 0)]
    GR[j] = GHP[j]
    gather_d(2, 1)
    grad_part(2, 1)
    reduce_far(2, 0)
    reduce_far(2, 1)
    reduce_near(2, 0)
    gather_d(2, 0)
    grad_part(2, 0)
    reduce_near(2, 1)
    edge_far()
    gather_c(1)
    gather_b(3)
    gather_b(0)
    back_first(2, True)
    reduce_b(2, 0)
    reduce_b(2, 1)
    gather_d(1)
    grad_second(1, 1)
    reduce_a(1, 1)
    grad_second(1, 0)
    reduce_a(1, 0)
    gather_c(3)
    back_first(1, False)
    edge_near(1)
    gather_c(0)
    reduce_b(1, 1)
    gather_d(3)
    grad_second(3, 0)
    reduce_a(3, 0)
    grad_second(3, 1)
    reduce_a(3, 1)
    edge_near(3)
    reduce_b(1, 0)
    reduce_c(2, 0)
    reduce_z(2, 0)
    reduce_c(2, 1)
    reduce_z(2, 1)
    back_first(3, False)
    gather_d(0)
    back_first(0, False)

    @pl.loop(0, 12)
    def _(i):
        rows = pl.ds(pl.multiple_of(i * 64, 64), 64)
        BKS[rows, :] = BACK[rows, theirs].astype(BF16)

    back_in = push(BKS, BKR, at(dc=1))
    reduce_b(3, 0)
    grad_second(0, 0)
    back_in.wait_recv()

    @pl.loop(0, 12)
    def _(i):
        rows = pl.ds(pl.multiple_of(i * 64, 64), 64)
        back = BACK[rows, mine] + BKR[rows, :].astype(F32)
        SF[rows, :] = (back * SP[rows, :]).astype(BF16)

    @pl.loop(0, 2)
    def _(n):
        rows = pl.ds(pl.multiple_of(n * 256, 256), 256)
        part = dot(FT[rows, :], SF[...]).astype(BF16)
        G1[pl.ds(2 * n, 2)] = part.reshape(2, 4, 32, 512)

    lo, hi = pl.ds(0, 16), pl.ds(16, 16)
    x1, x3, x2 = mod(x + 1, 4), mod(x - 1, 4), mod(x + 2, 4)
    z1, z3, z2 = mod(zh + 1, 4), mod(zh - 1, 4), mod(zh + 2, 4)
    yin = [
        push(G1.at[x2, :, lo], YA, at(dx=1)),
        push(G1.at[x2, :, hi], YB, at(dx=3)),
        push(G1.at[x1, :, hi], YL.at[1], at(dx=1)),
        push(G1.at[x3, :, lo], YR.at[0], at(dx=3)),
    ]
    reduce_b(3, 1)
    grad_second(0, 1)
    reduce_c(1, 1)
    reduce_z(1, 1)
    reduce_c(1, 0)
    reduce_z(1, 0)
    reduce_c(3, 0)
    reduce_z(3, 0)

    def sums_y():
        for got, buf, row, half, dst, dx in (
            (yin[0], YA, x1, lo, YL.at[0], 1),
            (yin[1], YB, x3, hi, YR.at[1], 3),
        ):
            got.wait_recv()
            block = G1[row, :, half].astype(F32) + buf[...].astype(F32)
            G1[row, :, half] = block.astype(BF16)
            yin.append(push(G1.at[row, :, half], dst, at(dx=dx)))

    sums_y()
    reduce_a(0, 0)
    reduce_a(0, 1)
    edge_sum()
    for got in gh_in:
        got.wait_recv()
    GS[...] = functools.reduce(jnp.add, [GR[i] for i in range(8)])
    gz_sem, gx_sem = link.take(), link.take()
    for d in (1, 2, 3):
        push(GS, GZ.at[d - 1], at(dz=d), k=gz_sem)
    gz_in = [link.make(GZ, GZ, at(dz=1), gz_sem, 0)]
    reduce_c(3, 1)
    reduce_z(3, 1)
    for got in yin[2:]:
        got.wait_recv()
    for side, half in ((0, lo), (1, hi)):
        block = G1[x, :, half].astype(F32) + YL[side].astype(F32) + YR[side].astype(F32)
        G1[x, :, half] = block.astype(BF16)
    uin = [
        push(G1.at[x, z2, lo], UA, at(dz=1)),
        push(G1.at[x, z2, hi], UB, at(dz=3)),
        push(G1.at[x, z1, hi], UL.at[1], at(dz=1)),
        push(G1.at[x, z3, lo], UR.at[0], at(dz=3)),
    ]
    reduce_b(0, 0)
    reduce_b(0, 1)
    edge_mid()
    for got, buf, row, half, dst, dz in (
        (uin[0], UA, z1, lo, UL.at[0], 1),
        (uin[1], UB, z3, hi, UR.at[1], 3),
    ):
        got.wait_recv()
        block = G1[x, row, half].astype(F32) + buf[...].astype(F32)
        G1[x, row, half] = block.astype(BF16)
        uin.append(push(G1.at[x, row, half], dst, at(dz=dz)))
    for got in gz_in:
        got.wait_recv()
    GY[...] = GS[...] + GZ[0] + GZ[1] + GZ[2]
    for d in (1, 2, 3):
        push(GY, GX.at[d - 1], at(dx=d), k=gx_sem)
    gxs_in = [link.make(GX, GX, at(dx=1), gx_sem, 0)]
    for got in gxs_in:
        got.wait_recv()
    heads = GY[...] + GX[0] + GX[1] + GX[2]
    GH[...] = heads
    gc_in = push(GH, GC, at(dc=1))
    for got in uin[2:]:
        got.wait_recv()
    for side, half in ((0, lo), (1, hi)):
        GF[side] = (
            G1[x, zh, half].astype(F32) + UL[side].astype(F32) + UR[side].astype(F32)
        )
    gt_in = push(GF.at[1 - c], GT, at(dc=1))
    gc_in.wait_recv()
    other = GC[...]
    loss_o[...] = jnp.broadcast_to(jnp.sum(heads[2]), (8, 128))
    for i in range(2):
        gh_o[:, lane(2 * i)] = jnp.where(c == 0, heads[i], other[i])
        gh_o[:, lane(2 * i + 1)] = jnp.where(c == 0, other[i], heads[i])
    reduce_c(0, 0, g2_o)
    reduce_c(0, 1, g2_o)
    edge_end()
    for got in z_in:
        got.wait_recv()
    for side, half in ((0, LOW), (1, HIGH)):
        g2_o[half, :] = g2_o[half, :] + ZL[side].astype(F32) + ZR[side].astype(F32)
    gt_in.wait_recv()
    kept, brought = GF[c], GT[...]
    g1_o[:, pl.ds(0, 512)] = jnp.where(c == 0, kept, brought)
    g1_o[:, pl.ds(512, 512)] = jnp.where(c == 0, brought, kept)

    link.drain()

    @pl.when(c == 0)
    def _():
        for copy in re_to:
            copy.wait_send()

    @pl.when(r < 4)
    def _():
        for copy in v_out:
            copy.wait_send()


SCRATCH = [
    ((2, 384, 512), BF16), ((512, 768), BF16), ((4, 4, 2, 16, 512), BF16),
    ((4, 1024, 512), BF16), ((8, 8, 512), F32), ((8, 2048), BF16), ((3, 2, 4, 8, 128), F32),
    ((768, 1024), BF16), ((1024, 768), BF16), ((768, 512), F32), ((8, 96, 2048), BF16),
    ((4, 96, 512), BF16), ((4, 96, 512), BF16), ((4, 2, 96, 512), BF16),
    ((4, 2, 96, 512), BF16), ((4, 96, 512), BF16), ((96, 2048), F32), ((96, 2048), F32),
    ((96, 2048), BF16), ((24, 8, 128), F32), ((12, 8, 128), F32), ((8, 96, 2048), BF16),
    ((768, 1024), F32), ((4, 1024, 512), BF16), ((4, HALF, 128), BF16), ((4, HALF, 128), BF16),
    ((4, 2, HALF, 128), BF16), ((4, 2, HALF, 128), BF16), ((HALF, 128), BF16),
    ((HALF, 128), BF16), ((2, HALF, 128), BF16), ((2, HALF, 128), BF16), ((768, 512), BF16),
    ((768, 512), BF16), ((768, 512), BF16), ((4, 4, 32, 512), BF16), ((4, 16, 512), BF16),
    ((4, 16, 512), BF16), ((2, 4, 16, 512), BF16), ((2, 4, 16, 512), BF16), ((16, 512), BF16),
    ((16, 512), BF16), ((2, 16, 512), BF16), ((2, 16, 512), BF16), ((2, 16, 512), F32),
    ((16, 512), F32), ((8, 3, 8, 128), F32), ((8, 3, 8, 128), F32), ((3, 8, 128), F32),
    ((3, 3, 8, 128), F32), ((3, 3, 8, 128), F32), ((3, 8, 128), F32), ((3, 8, 128), F32),
    ((3, 8, 128), F32), ((8, 512), BF16), ((8, 384), F32), ((1, 384), jnp.int32),
    ((16, 1024), BF16),
    ((2, EDGE // 2, 512), BF16), ((2, EDGE // 2, 512), BF16), ((2, EDGE // 2, 512), BF16),
    ((2, EDGE // 2, 128), BF16), ((2, EDGE // 2, 128), BF16), ((2, EDGE // 2, 128), BF16),
]


def finish(adv, loss, g1, g2, gh, adv_o, loss_o, g1_o, g2_o, gh_o):
    adv_o[...] = jnp.concatenate([adv[i][:, :96] for i in range(4)], axis=1)
    loss_o[0, 0] = loss[0, 0] * (0.5 / 98304)
    g1_o[...] = g1[...]
    g2_o[...] = g2[...]
    gh_o[...] = gh[...]


def shards(features, w_first, w_second, w_head, rewards, discount, trace, episode):
    vmem = pl.BlockSpec(memory_space=pltpu.VMEM)
    smem = pl.BlockSpec(memory_space=pltpu.SMEM)
    hbm = pl.BlockSpec(memory_space=pltpu.HBM)
    shapes = ((16, 1024), (1024, 128), (8, 512))
    parts = pl.pallas_call(
        kernel,
        out_shape=[
            jax.ShapeDtypeStruct(shape, F32) for shape in ((4, 8, 128), (8, 128), *shapes)
        ],
        in_specs=[hbm] * 6 + [smem] * 2,
        out_specs=[vmem] * 5,
        scratch_shapes=[pltpu.VMEM(shape, kind) for shape, kind in SCRATCH]
        + [pltpu.SemaphoreType.DMA((count,)) for count in (RING + 18, SLOTS, 6)],
        compiler_params=pltpu.CompilerParams(
            collective_id=0, has_side_effects=True, vmem_limit_bytes=62 * 2**20
        ),
    )(
        features, w_first, w_second, w_head.T, rewards, episode.reshape(1, -1),
        discount, trace,
    )
    advantages, loss, grad_first, grad_second, grad_head = pl.pallas_call(
        finish,
        out_shape=[
            jax.ShapeDtypeStruct(shape, F32) for shape in ((8, 384), (1, 1), *shapes)
        ],
        in_specs=[vmem, smem, vmem, vmem, vmem],
        out_specs=[vmem, smem, vmem, vmem, vmem],
    )(*parts)
    return advantages, loss[0, 0], grad_first, grad_second, grad_head.T


def solution(mesh):
    placed = (
        P("batch", None),
        P("batch", "hidden"),
        P("hidden", "batch"),
        P("hidden", None),
        P(None, "batch"),
        P(),
        P(),
        P("batch"),
    )
    return jax.shard_map(
        shards,
        mesh=mesh,
        in_specs=placed,
        out_specs=(
            P(None, "batch"),
            P(),
            P("batch", "hidden"),
            P("hidden", "batch"),
            P("hidden", None),
        ),
        check_vma=False,
    )
```

```python
import functools

import jax
import jax.numpy as jnp
from jax import lax
from jax.experimental import pallas as pl
from jax.experimental.pallas import tpu as pltpu
from jax.sharding import PartitionSpec as P

BF16, F32 = jnp.bfloat16, jnp.float32
MESH = pl.DeviceIdType.MESH
SLOTS, RING = 130, 48
EDGE = 192
HALF = (1024 - EDGE) // 2
LOW, HIGH = pl.ds(0, HALF), pl.ds(HALF, HALF)
TOP = pl.ds(2 * HALF, EDGE)
TOPS = (pl.ds(2 * HALF, EDGE // 2), pl.ds(2 * HALF + EDGE // 2, EDGE // 2))


def dot(left, right, dims=((1,), (0,))):
    return lax.dot_general(left, right, (dims, ((), ())), preferred_element_type=F32)


def mod(value, count):
    return lax.rem(value + count, count)


def lane(dx):
    return pl.ds(dx * 128, 128)


class Links:
    def __init__(self, sent, came):
        self.sent, self.came, self.used, self.open = sent, came, 0, []

    def take(self):
        self.used += 1
        return self.used - 1

    def make(self, src, dst, to, k, k_sent):
        return pltpu.make_async_remote_copy(
            src_ref=src,
            dst_ref=dst,
            send_sem=self.sent.at[k_sent],
            recv_sem=self.came.at[k],
            device_id=to,
            device_id_type=MESH,
        )

    def push(self, src, dst, to, land=None, k=None):
        k = self.take() if k is None else k
        turn = len(self.open)
        if turn >= RING:
            self.open[turn - RING].wait_send()
        copy = self.make(src, dst, to, k, turn % RING)
        copy.start()
        self.open.append(copy)
        return copy if land is None else self.make(land, land, to, k, 0)

    def all_of(self, ref, k):
        return self.make(ref, ref, self.peer, k, 0)

    def drain(self):
        for copy in self.open[-RING:]:
            copy.wait_send()


def kernel(
    feat, w1in, w2in, whin, reward_in, number_in, discount_in, trace_in,
    adv_o, loss_o, g1_o, g2_o, gh_o,
    F, FT, W1, W2, WHB, WH, RE, HF, HFT, SP, PS, RA, RB, RL, RR, RZ, PRE, SL2, H2,
    V, ADV, S, BACK, G2, XA, XB, XL, XR, ZA, ZB, ZL, ZR, BKS, BKR, SF,
    G1, YA, YB, YL, YR, UA, UB, UL, UR, GF, GT, GHP, GR, GS, GZ, GX, GY, GC, GH,
    WHS, RWS, EPS, WIN, EZF, EZL, EZR, EXF, EXL, EXR, sent, came, local,
):
    b, j = lax.axis_index("batch"), lax.axis_index("hidden")
    c, m = lax.rem(b, 2), lax.div(b, 2)
    zh, x = lax.rem(m, 4), lax.div(m, 4)
    y, zl = lax.rem(j, 4), lax.div(j, 4)
    r = y * 2 + zl
    link = Links(sent, came)
    push = link.push

    def at(dx=0, dz=0, dc=0, dy=0, dl=0):
        bb = (mod(x + dx, 4) * 4 + mod(zh + dz, 4)) * 2 + mod(c + dc, 2)
        return bb, mod(zl + dl, 2) * 4 + mod(y + dy, 4)

    def beside(step, dc, dy, dl):
        bb = mod(m + step, 16) * 2 + mod(c + dc, 2)
        return bb, mod(zl + dl, 2) * 4 + mod(y + dy, 4)

    link.peer = at(dc=1)
    peers = [(dc, dy, dl) for dc in range(2) for dy in range(4) for dl in range(2)]

    loads = [
        pltpu.make_async_copy(src, dst, local.at[k])
        for k, (src, dst) in enumerate(
            (
                (w1in, WIN),
                (w2in, W2.at[0, :, lane(0)]),
                (feat, F.at[c]),
                (whin, WHS),
                (reward_in, RWS),
                (number_in, EPS.at[0]),
            )
        )
    ]
    for load in loads:
        load.start()

    barrier = pltpu.get_barrier_semaphore()
    partners = [at(dc=dc, dy=dy, dl=dl) for dc, dy, dl in peers[1:]]
    partners += [at(dx=d) for d in (1, 2, 3)] + [at(dz=d) for d in (1, 2, 3)]
    partners += [beside(step, *peer) for step in (1, -1) for peer in peers]
    for partner in partners:
        pl.semaphore_signal(barrier, inc=1, device_id=partner, device_id_type=MESH)
    for load in loads:
        load.wait()
    blank = jnp.zeros((8, 32), F32)
    WHB[j] = WHS[...].astype(F32)
    for i in range(4):
        reward = RWS[:, i * 96 : (i + 1) * 96]
        number = jnp.broadcast_to(EPS[:, i * 96 : (i + 1) * 96].astype(F32), (8, 96))
        RE[c, 0, i] = jnp.concatenate([reward, blank], axis=1)
        RE[c, 1, i] = jnp.concatenate([number, blank], axis=1)
    pl.semaphore_wait(barrier, len(partners))

    mine, theirs = (
        pl.ds(pl.multiple_of(side * 512, 512), 512) for side in (c, 1 - c)
    )
    w1_sem = link.take()
    w1pair = push(WIN.at[:, theirs], W1.at[x, zh, c], at(dc=1), W1.at[x, zh, 1 - c])
    W1[x, zh, c] = WIN[:, mine]

    def w1_sides(zs):
        own = W1.at[x, zs]
        return [push(own, own, at(dx=dx), W1.at[mod(x - dx, 4), zs]) for dx in (1, 3)]

    def w1_across(zs, sides):
        out = []
        for dx, side in ((1, 0), (3, 1)):
            sides[side].wait_recv()
            part = W1.at[mod(x - dx, 4), zs, side]
            out.append(push(part, part, at(dx=dx), k=w1_sem))
        return out

    w2x = {}

    def w2_to(dz, half, dx):
        key = (dz, 4 - dx, 0 if half is LOW else 1)
        w2x[key] = push(
            W2.at[dz, half, lane(0)], W2.at[dz, half, lane(4 - dx)], at(dx=dx)
        )

    def w2_side(dz, half):
        near = 1 if half is LOW else 3
        w2_to(dz, half, near)
        w2_to(dz, half, 4 - near)

    def w2_across(dz):
        w2x[dz, 3, 0].wait_recv()
        w2x[dz, 2, 0] = push(
            W2.at[dz, LOW, lane(3)], W2.at[dz, LOW, lane(2)], at(dx=1)
        )
        w2x[dz, 1, 1].wait_recv()
        w2x[dz, 2, 1] = push(
            W2.at[dz, HIGH, lane(1)], W2.at[dz, HIGH, lane(2)], at(dx=3)
        )

    def w2_rest(dz, keys=((3, 1), (1, 0), (2, 0), (2, 1))):
        for key in keys:
            w2x[(dz, *key)].wait_recv()

    def w2_z(half, dz):
        return push(W2.at[0, half, lane(0)], W2.at[4 - dz, half, lane(0)], at(dz=dz))

    first, second, w1z, w1x, w1far = [], [], {}, {}, {}

    def w1_start():
        w1pair.wait_recv()
        own = W1.at[x, zh]
        for dz in (1, 3, 2):
            w1z[dz] = push(own, own, at(dz=dz), W1.at[x, mod(zh - dz, 4)])
        w1x[0] = w1_sides(zh)

    def w1_from_z(dz):
        w1z[dz].wait_recv()
        w1x[dz] = w1_sides(mod(zh - dz, 4))

    def w1_far(dz):
        w1far[dz] = w1_across(mod(zh - dz, 4), w1x[dz])

    def w1_done():
        link.all_of(W1.at[0], w1_sem).wait_recv()

    edge = {}

    def edge_x1():
        src = W2.at[0, TOP, lane(0)]
        edge["x3"] = push(src, W2.at[0, TOP, lane(3)], at(dx=1))
        edge["x1"] = push(src, W2.at[0, TOP, lane(1)], at(dx=3))

    def edge_x2():
        edge["x3"].wait_recv()
        src = W2.at[0, TOPS[0], lane(3)]
        edge["x2"] = [push(src, W2.at[0, TOPS[0], lane(2)], at(dx=1))]
        edge["x1"].wait_recv()
        src = W2.at[0, TOPS[1], lane(1)]
        edge["x2"].append(push(src, W2.at[0, TOPS[1], lane(2)], at(dx=3)))

    def edge_z1():
        for got in edge["x2"]:
            got.wait_recv()
        src = W2.at[0, TOP]
        edge["z3"] = push(src, W2.at[3, TOP], at(dz=1))
        edge["z1"] = push(src, W2.at[1, TOP], at(dz=3))

    edge["z2"] = []

    def edge_z2(dz):
        edge["z3" if dz == 3 else "z1"].wait_recv()
        half = TOPS[0 if dz == 3 else 1]
        edge["z2"].append(push(W2.at[dz, half], W2.at[2, half], at(dz=4 - dz)))

    w1_start()
    edge_x1()
    w2_to(0, LOW, 1)
    w2_to(0, HIGH, 3)
    first += [w2_z(LOW, 1), w2_z(HIGH, 3)]
    feat_in = push(F.at[c], F.at[c], at(dc=1), F.at[1 - c])
    w1_from_z(1)
    w2_to(0, HIGH, 1)
    w2_to(0, LOW, 3)
    w1_from_z(3)
    w1_far(0)
    edge_x2()
    w1_from_z(2)
    second += [w2_z(HIGH, 1), w2_z(LOW, 3)]
    re_in = push(RE.at[c], RE.at[c], at(dc=1), RE.at[1 - c])
    re_sem = link.take()
    re_to = [
        link.make(RE.at[c], RE.at[2], beside(-1, dc, 0, 0), re_sem, RING + dc)
        for dc in range(2)
    ]

    @pl.when(c == 0)
    def _():
        for copy in re_to:
            copy.start()

    wh_sem = link.take()
    for dc, dy, dl in peers[1:8]:
        push(WHB.at[j], WHB.at[j], at(dy=dy, dl=dl), k=wh_sem)
    wh_all = WHB.at[pl.ds(0, 7)]
    wh_in = [link.make(wh_all, wh_all, at(dc=1), wh_sem, 0)]

    w1_far(1)
    edge_z1()
    w1_far(3)
    w1_far(2)
    w2_across(0)
    w2_z2 = []

    def w2_first():
        first[0].wait_recv()
        w2_z2.append(push(W2.at[3, LOW, lane(0)], W2.at[2, LOW, lane(0)], at(dz=1)))
        w2_side(3, LOW)
        first[1].wait_recv()
        w2_z2.append(push(W2.at[1, HIGH, lane(0)], W2.at[2, HIGH, lane(0)], at(dz=3)))
        w2_side(1, HIGH)

    def w2_second():
        second[0].wait_recv()
        w2_side(3, HIGH)
        second[1].wait_recv()
        w2_side(1, LOW)

    def w2_third():
        w2_z2[0].wait_recv()
        w2_side(2, LOW)
        w2_z2[1].wait_recv()
        w2_side(2, HIGH)

    w2_first()
    feat_in.wait_recv()
    w1_done()
    hf_in = []

    def layer_one():
        for n in range(2):
            cols = pl.ds(n * 256, 256)
            into = pl.ds(pl.multiple_of(c * 512 + n * 256, 256), 256)
            there = pl.ds(pl.multiple_of((1 - c) * 512 + n * 256, 256), 256)
            weights = W1[:, :, :, :, cols].reshape(512, 256)
            SP[:, cols] = dot(F[...].reshape(768, 512), weights)

            @pl.loop(0, 12)
            def _(i):
                rows = pl.ds(pl.multiple_of(i * 64, 64), 64)
                value = SP[rows, cols]
                gate = 1.0 / (1.0 + jnp.exp(-value))
                HF[rows, into] = (value * gate).astype(BF16)
                SP[rows, cols] = gate * (1.0 + value * (1.0 - gate))

            src = HF.at[:, into]
            hf_in.append(push(src, src, at(dc=1), HF.at[:, there]))

    layer_one()
    w2_second()

    def product(dz, part=None):
        for n in range(2) if part is None else (part,):
            out = dot(HF[...], W2[dz, :, pl.ds(n * 256, 256)])
            into = pl.ds(dz * 512 + n * 256, 256)
            PS[:, :, into] = out.astype(BF16).reshape(8, 96, 256)

    up, down, over = mod(y + 1, 4), mod(y - 1, 4), mod(y + 2, 4)
    came_rs = {}

    def lanes(dz, part):
        if part is None:
            return pl.ds(dz * 512, 512), pl.ds(0, 512)
        return pl.ds(dz * 512 + part * 256, 256), pl.ds(part * 256, 256)

    def scatter_a(dz, part=None):
        wide, here = lanes(dz, part)
        k = link.take()
        came_rs[dz, part] = [
            push(PS.at[over * 2, :, wide], RA.at[dz, :, here], at(dy=1)),
            push(PS.at[over * 2 + 1, :, wide], RB.at[dz, :, here], at(dy=3)),
            link.all_of(PS.at[pl.ds(0, 4), :, wide], k),
            k,
        ]
        push(PS.at[up * 2 + 1, :, wide], RL.at[dz, 1, :, here], at(dy=1), k=k)
        push(PS.at[down * 2, :, wide], RR.at[dz, 0, :, here], at(dy=3), k=k)

    def scatter_b(dz, part=None):
        wide, here = lanes(dz, part)
        for got, buf, row, dst, dy in (
            (came_rs[dz, part][0], RA, up * 2, RL.at[dz, 0, :, here], 1),
            (came_rs[dz, part][1], RB, down * 2 + 1, RR.at[dz, 1, :, here], 3),
        ):
            got.wait_recv()
            total = PS[row, :, wide].astype(F32) + buf[dz, :, here].astype(F32)
            PS[row, :, wide] = total.astype(BF16)
            push(PS.at[row, :, wide], dst, at(dy=dy), k=came_rs[dz, part][3])

    def scatter_c(dz, part=None):
        wide, here = lanes(dz, part)
        came_rs[dz, part][2].wait_recv()

        def total(side):
            return (
                PS[y * 2 + side, :, wide].astype(F32)
                + RL[dz, side, :, here].astype(F32)
                + RR[dz, side, :, here].astype(F32)
            )

        PS[y * 2 + 1 - zl, :, wide] = total(1 - zl).astype(BF16)
        came_rs[dz, part].append(
            push(PS.at[y * 2 + 1 - zl, :, wide], RZ.at[dz, :, here], at(dl=1))
        )
        PRE[:, wide] = total(zl)

    def scatter_d(dz, part=None):
        wide, here = lanes(dz, part)
        came_rs[dz, part][-1].wait_recv()

        @pl.loop(0, 3)
        def _(i):
            rows = pl.ds(pl.multiple_of(i * 32, 32), 32)
            value = PRE[rows, wide] + RZ[dz, rows, here].astype(F32)
            gate = 1.0 / (1.0 + jnp.exp(-value))
            H2[rows, wide] = (value * gate).astype(BF16)
            SL2[rows, wide] = gate * (1.0 + value * (1.0 - gate))

    for got in hf_in:
        got.wait_recv()
    w2_rest(0)
    product(0)
    scatter_a(0)
    w2_across(3)
    w2_across(1)
    scatter_b(0)
    edge_z2(3)
    w2_rest(3)
    product(3)
    scatter_a(3)
    w2_third()
    edge_z2(1)
    w2_rest(1)
    product(1)
    scatter_a(1)
    scatter_c(0)

    def transposes():
        @pl.loop(0, 4)
        def _(n):
            cols = pl.ds(pl.multiple_of(n * 256, 256), 256)
            HFT[cols, :] = HF[:, cols].astype(F32).T.astype(BF16)

        @pl.loop(0, 2)
        def _(n):
            cols = pl.ds(pl.multiple_of(n * 256, 256), 256)
            FT[cols, :] = F[:, :, cols].reshape(768, 256).astype(F32).T.astype(BF16)

    transposes()
    scatter_b(3)
    w2_across(2)
    for copy in wh_in:
        copy.wait_recv()
    for dz in range(4):
        for dx in range(4):
            mm = mod(x + dx, 4) * 4 + mod(zh + dz, 4)
            group, pair = lax.div(mm, 2), lax.rem(mm, 2)
            even, odd = (
                jnp.where(c == 0, WHB[group, :, lane(2 * p)], WHB[group, :, lane(2 * p + 1)])
                for p in (0, 1)
            )
            WH[:, lane(dz * 4 + dx)] = jnp.where(pair == 0, even, odd).astype(BF16)
    scatter_d(0)
    scatter_b(1)
    w2_rest(2, ((1, 0),))
    for got in edge["z2"]:
        got.wait_recv()
    product(2, 0)
    scatter_a(2, 0)
    w2_rest(2, ((3, 1), (2, 0), (2, 1)))
    product(2, 1)
    scatter_a(2, 1)
    scatter_c(3)
    scatter_c(1)
    scatter_d(3)
    scatter_b(2, 0)
    scatter_b(2, 1)
    scatter_d(1)
    scatter_c(2, 0)
    scatter_c(2, 1)
    scatter_d(2, 0)
    scatter_d(2, 1)

    own_values = dot(WH[...], H2[...], ((1,), (1,)))
    own_v = V.at[c * 12 + r]
    V[c * 12 + r] = jnp.concatenate([own_values, blank], axis=1)
    v_sem = link.take()
    for dc, dy, dl in peers[1:]:
        push(own_v, own_v, at(dc=dc, dy=dy, dl=dl), k=v_sem)
    v_out = [
        link.make(
            own_v, V.at[c * 12 + 8 + lax.rem(r, 4)], beside(-1, *peer), v_sem, RING + 2 + k
        )
        for k, peer in enumerate(peers)
    ]

    @pl.when(r < 4)
    def _():
        for copy in v_out:
            copy.start()

    re_in.wait_recv()
    link.make(RE.at[2], RE.at[2], at(dc=1), re_sem, 0).wait_recv()
    shape = (8, 12 * 128)
    place = lax.rem(lax.broadcasted_iota(jnp.int32, shape, 1), 128)

    def ahead(array, steps):
        return pltpu.roll(array, shape[1] - steps, 1)

    def following(array):
        return jnp.where(place == 95, ahead(array, 33), ahead(array, 1))

    def row_of(kind):
        return jnp.concatenate([RE[i // 4, kind, i % 4] for i in range(12)], axis=1)

    reward, number = row_of(0), row_of(1)
    head_row = lax.broadcasted_iota(jnp.int32, (8, 128), 0)

    def spread(array):
        out = jnp.zeros((8, 128), F32)
        for k in range(8):
            out = jnp.where(head_row == k, array[k], out)
        return out

    rate, decay = spread(discount_in), spread(trace_in)
    discount = jnp.concatenate([rate] * 12, axis=1)
    both = jnp.concatenate([rate * decay] * 12, axis=1)
    keep = jnp.where(following(number) == number, 1.0, 0.0)
    real = place < 96
    factor = jnp.where(real, both * keep, 1.0)
    scale = discount * keep

    v_all = V.at[pl.ds(0, 23)]
    v_in = [link.make(v_all, v_all, at(dc=1), v_sem, 0)]
    for copy in v_in:
        copy.wait_recv()
    value = jnp.concatenate([V[i] + V[12 + i] for i in range(12)], axis=1)
    total = jnp.where(real, reward + scale * following(value) - value, 0.0)
    step = 1
    while step < shape[1]:
        total = total + factor * ahead(total, step)
        factor = factor * ahead(factor, step)
        step *= 2
    for i in range(12):
        ADV[i] = total[:, i * 128 : (i + 1) * 128]

    own = ADV[r]
    slope_t = (-own[:, :96]).astype(BF16)
    slope = (-own).T[:96, :].astype(BF16)
    own_rows = S.at[r]

    def slope_chunk(dz):
        at_dz = pl.ds(dz * 512, 512)
        own_rows[:, at_dz] = (dot(slope, WH[:, at_dz]) * SL2[:, at_dz]).astype(BF16)

    ag = {}
    pair_r = y * 2 + 1 - zl

    def gather_a(dz, part=None):
        wide, _ = lanes(dz, part)
        src = S.at[r, :, wide]
        k, far = link.take(), link.take()
        pair = push(src, src, at(dl=1), S.at[pair_r, :, wide])
        push(src, src, at(dy=1), k=k)
        push(src, src, at(dy=3), k=k)
        ag[dz, part] = pair, k, far

    def gather_b(dz, part=None):
        wide, _ = lanes(dz, part)
        pair, k, _ = ag[dz, part]
        pair.wait_recv()
        src = S.at[pair_r, :, wide]
        push(src, src, at(dy=1), k=k)
        push(src, src, at(dy=3), k=k)

    def gather_c(dz, part=None):
        wide, _ = lanes(dz, part)
        _, k, far = ag[dz, part]
        link.all_of(S.at[pl.ds(0, 4), :, wide], k).wait_recv()
        low, high = S.at[down * 2, :, wide], S.at[up * 2 + 1, :, wide]
        push(low, low, at(dy=1), k=far)
        push(high, high, at(dy=3), k=far)

    def gather_d(dz, part=None):
        wide, _ = lanes(dz, part)
        link.all_of(S.at[pl.ds(0, 2), :, wide], ag[dz, part][2]).wait_recv()

    def grad_part(dz, part):
        wide, here = lanes(dz, part)

        @pl.loop(0, 2)
        def _(n):
            rows = pl.ds(pl.multiple_of(n * 512, 512), 512)
            G2[dz, rows, here] = dot(HFT[rows, :], S[:, :, wide].reshape(768, 256)).astype(BF16)

    def grad_second(dz, side):
        at_dz = pl.ds(dz * 512, 512)

        @pl.loop(0, 2)
        def _(n):
            size = (HALF if side == 0 else HALF + EDGE) // 2
            rows = pl.ds(pl.multiple_of(side * HALF + n * size, 16), size)
            G2[dz, rows, :] = dot(HFT[rows, :], S[:, :, at_dz].reshape(768, 512)).astype(BF16)

    def back_first(dz, start):
        at_dz = pl.ds(dz * 512, 512)

        @pl.loop(0, 4)
        def _(n):
            cols = pl.ds(pl.multiple_of(n * 256, 256), 256)
            part = dot(S[:, :, at_dz].reshape(768, 512), W2[dz, cols, :], ((1,), (1,)))
            BACK[:, cols] = part if start else BACK[:, cols] + part

    gx, halves = {}, (LOW, HIGH)

    def reduce_far(dz, side):
        src = G2.at[dz, halves[side], lane(2)]
        gx[dz, side] = push(src, (XA, XB)[side].at[dz], at(dx=(1, 3)[side])), link.take()

    def reduce_near(dz, side):
        src = G2.at[dz, halves[side], lane((3, 1)[side])]
        push(src, (XR, XL)[side].at[dz, side], at(dx=(3, 1)[side]), k=gx[dz, side][1])

    def reduce_a(dz, side):
        reduce_far(dz, side)
        reduce_near(dz, side)

    def reduce_b(dz, side):
        gx[dz, side][0].wait_recv()
        dx, half = (1, 3)[side], halves[side]
        block = G2[dz, half, lane(dx)].astype(F32) + (XA, XB)[side][dz].astype(F32)
        G2[dz, half, lane(dx)] = block.astype(BF16)
        src = G2.at[dz, half, lane(dx)]
        push(src, (XL, XR)[side].at[dz, side], at(dx=dx), k=gx[dz, side][1])

    def reduce_c(dz, side, into=None):
        half = halves[side]
        link.all_of(XL.at[dz], gx[dz, side][1]).wait_recv()
        block = (
            G2[dz, half, lane(0)].astype(F32)
            + XL[dz, side].astype(F32)
            + XR[dz, side].astype(F32)
        )
        if into is None:
            G2[dz, half, lane(0)] = block.astype(BF16)
        else:
            into[half, :] = block

    e_far, e_x, e_sem, ex_sem = [], [], link.take(), link.take()

    def edge_far():
        for side in (0, 1):
            src = G2.at[2, TOPS[side], :]
            e_far.append(push(src, EZF.at[side], at(dz=(1, 3)[side])))

    def edge_near(dz):
        buf, near, side = (EZL, 1, 0) if dz == 1 else (EZR, 0, 1)
        push(G2.at[dz, TOPS[near], :], buf.at[near], at(dz=dz), k=e_sem)
        e_far[side].wait_recv()
        block = G2[dz, TOPS[side], :].astype(F32) + EZF[side].astype(F32)
        G2[dz, TOPS[side], :] = block.astype(BF16)
        push(G2.at[dz, TOPS[side], :], buf.at[side], at(dz=dz), k=e_sem)

    def edge_sum():
        link.all_of(G2.at[0, pl.ds(0, 2 * EDGE), :], e_sem).wait_recv()
        for side in (0, 1):
            block = (
                G2[0, TOPS[side], :].astype(F32)
                + EZL[side].astype(F32)
                + EZR[side].astype(F32)
            )
            G2[0, TOPS[side], :] = block.astype(BF16)
            src = G2.at[0, TOPS[side]]
            e_x.append(push(src.at[:, lane(2)], EXF.at[side], at(dx=(1, 3)[side])))
            near = (EXR, EXL)[side].at[side]
            push(src.at[:, lane((3, 1)[side])], near, at(dx=(3, 1)[side]), k=ex_sem)

    def edge_mid():
        for side in (0, 1):
            e_x[side].wait_recv()
            dx = (1, 3)[side]
            block = G2[0, TOPS[side], lane(dx)].astype(F32) + EXF[side].astype(F32)
            G2[0, TOPS[side], lane(dx)] = block.astype(BF16)
            src = G2.at[0, TOPS[side], lane(dx)]
            push(src, (EXL, EXR)[side].at[side], at(dx=dx), k=ex_sem)

    def edge_end():
        link.all_of(G2.at[0, pl.ds(0, 2 * EDGE), lane(0)], ex_sem).wait_recv()
        for side in (0, 1):
            g2_o[TOPS[side], :] = (
                G2[0, TOPS[side], lane(0)].astype(F32)
                + EXL[side].astype(F32)
                + EXR[side].astype(F32)
            )

    z_far, z_sem = [], link.take()

    def reduce_z(dz, side):
        half = halves[side]
        src = G2.at[dz, half, lane(0)]
        if dz == 2:
            z_far.append(push(src, (ZA, ZB)[side], at(dz=(1, 3)[side])))
            return
        if (dz, side) in ((1, 0), (3, 1)):
            z_far[side].wait_recv()
            block = G2[dz, half, lane(0)].astype(F32) + (ZA, ZB)[side][...].astype(F32)
            G2[dz, half, lane(0)] = block.astype(BF16)
        push(src, (ZL if dz == 1 else ZR).at[side], at(dz=dz), k=z_sem)

    slope_chunk(2)
    gather_a(2, 1)
    gather_a(2, 0)
    slope_chunk(1)
    slope_chunk(3)
    slope_chunk(0)
    gather_b(2, 1)
    gather_b(2, 0)
    gather_a(1)

    for i in range(4):
        adv_o[i] = ADV[4 * c + i]
    small = lax.broadcasted_iota(jnp.int32, (8, 128), 1) < 96
    own_loss = jnp.where(small, own * own, 0.0)
    head = dot(slope_t, H2[...])
    for dz in range(4):
        for dx in range(4):
            mm = mod(x + dx, 4) * 4 + mod(zh + dz, 4)
            GHP[lax.div(mm, 2), lax.rem(mm, 2)] = head[:, (dz * 4 + dx) * 128 :][:, :128]
    for g in range(8):
        GHP[g, 2] = own_loss
    gather_c(2, 1)
    gather_c(2, 0)
    gather_a(3)
    gather_b(1)
    gh_sem, gh_all = link.take(), GR.at[pl.ds(0, 7)]
    for dc, dy, dl in peers[1:8]:
        to_j = mod(zl + dl, 2) * 4 + mod(y + dy, 4)
        push(GHP.at[to_j], GR.at[j], at(dy=dy, dl=dl), k=gh_sem)
    gh_in = [link.make(gh_all, gh_all, at(dc=1), gh_sem, 0)]
    GR[j] = GHP[j]
    gather_d(2, 1)
    grad_part(2, 1)
    reduce_far(2, 0)
    reduce_far(2, 1)
    reduce_near(2, 0)
    gather_d(2, 0)
    grad_part(2, 0)
    reduce_near(2, 1)
    edge_far()
    gather_c(1)
    gather_b(3)
    gather_a(0)
    back_first(2, True)
    reduce_b(2, 0)
    reduce_b(2, 1)
    gather_b(0)
    gather_d(1)
    grad_second(1, 1)
    reduce_a(1, 1)
    grad_second(1, 0)
    reduce_a(1, 0)
    gather_c(3)
    back_first(1, False)
    edge_near(1)
    gather_c(0)
    reduce_b(1, 1)
    gather_d(3)
    grad_second(3, 0)
    reduce_a(3, 0)
    grad_second(3, 1)
    reduce_a(3, 1)
    edge_near(3)
    reduce_b(1, 0)
    reduce_c(2, 0)
    reduce_z(2, 0)
    reduce_c(2, 1)
    reduce_z(2, 1)
    back_first(3, False)
    gather_d(0)
    back_first(0, False)

    @pl.loop(0, 12)
    def _(i):
        rows = pl.ds(pl.multiple_of(i * 64, 64), 64)
        BKS[rows, :] = BACK[rows, theirs].astype(BF16)

    back_in = push(BKS, BKR, at(dc=1))
    reduce_b(3, 0)
    grad_second(0, 0)
    back_in.wait_recv()

    @pl.loop(0, 12)
    def _(i):
        rows = pl.ds(pl.multiple_of(i * 64, 64), 64)
        back = BACK[rows, mine] + BKR[rows, :].astype(F32)
        SF[rows, :] = (back * SP[rows, :]).astype(BF16)

    @pl.loop(0, 2)
    def _(n):
        rows = pl.ds(pl.multiple_of(n * 256, 256), 256)
        part = dot(FT[rows, :], SF[...]).astype(BF16)
        G1[pl.ds(2 * n, 2)] = part.reshape(2, 4, 32, 512)

    lo, hi = pl.ds(0, 16), pl.ds(16, 16)
    x1, x3, x2 = mod(x + 1, 4), mod(x - 1, 4), mod(x + 2, 4)
    z1, z3, z2 = mod(zh + 1, 4), mod(zh - 1, 4), mod(zh + 2, 4)
    yin = [
        push(G1.at[x2, :, lo], YA, at(dx=1)),
        push(G1.at[x2, :, hi], YB, at(dx=3)),
    ]
    y_sem, u_sem = link.take(), link.take()
    push(G1.at[x1, :, hi], YL.at[1], at(dx=1), k=y_sem)
    push(G1.at[x3, :, lo], YR.at[0], at(dx=3), k=y_sem)
    reduce_b(3, 1)
    grad_second(0, 1)
    reduce_c(1, 1)
    reduce_z(1, 1)
    reduce_c(1, 0)
    reduce_z(1, 0)
    reduce_c(3, 0)
    reduce_z(3, 0)

    def sums_y():
        for got, buf, row, half, dst, dx in (
            (yin[0], YA, x1, lo, YL.at[0], 1),
            (yin[1], YB, x3, hi, YR.at[1], 3),
        ):
            got.wait_recv()
            block = G1[row, :, half].astype(F32) + buf[...].astype(F32)
            G1[row, :, half] = block.astype(BF16)
            push(G1.at[row, :, half], dst, at(dx=dx), k=y_sem)

    sums_y()
    reduce_a(0, 0)
    reduce_a(0, 1)
    edge_sum()
    for got in gh_in:
        got.wait_recv()
    GS[...] = functools.reduce(jnp.add, [GR[i] for i in range(8)])
    gz_sem, gx_sem = link.take(), link.take()
    for d in (1, 2, 3):
        push(GS, GZ.at[d - 1], at(dz=d), k=gz_sem)
    gz_in = [link.make(GZ, GZ, at(dz=1), gz_sem, 0)]
    reduce_c(3, 1)
    reduce_z(3, 1)
    link.all_of(G1.at[pl.ds(0, 2)], y_sem).wait_recv()
    for side, half in ((0, lo), (1, hi)):
        block = G1[x, :, half].astype(F32) + YL[side].astype(F32) + YR[side].astype(F32)
        G1[x, :, half] = block.astype(BF16)
    uin = [
        push(G1.at[x, z2, lo], UA, at(dz=1)),
        push(G1.at[x, z2, hi], UB, at(dz=3)),
    ]
    push(G1.at[x, z1, hi], UL.at[1], at(dz=1), k=u_sem)
    push(G1.at[x, z3, lo], UR.at[0], at(dz=3), k=u_sem)
    reduce_b(0, 0)
    reduce_b(0, 1)
    edge_mid()
    for got, buf, row, half, dst, dz in (
        (uin[0], UA, z1, lo, UL.at[0], 1),
        (uin[1], UB, z3, hi, UR.at[1], 3),
    ):
        got.wait_recv()
        block = G1[x, row, half].astype(F32) + buf[...].astype(F32)
        G1[x, row, half] = block.astype(BF16)
        push(G1.at[x, row, half], dst, at(dz=dz), k=u_sem)
    for got in gz_in:
        got.wait_recv()
    GY[...] = GS[...] + GZ[0] + GZ[1] + GZ[2]
    for d in (1, 2, 3):
        push(GY, GX.at[d - 1], at(dx=d), k=gx_sem)
    gxs_in = [link.make(GX, GX, at(dx=1), gx_sem, 0)]
    for got in gxs_in:
        got.wait_recv()
    heads = GY[...] + GX[0] + GX[1] + GX[2]
    GH[...] = heads
    gc_in = push(GH, GC, at(dc=1))
    link.all_of(G1.at[0, pl.ds(0, 2)], u_sem).wait_recv()
    for side, half in ((0, lo), (1, hi)):
        GF[side] = (
            G1[x, zh, half].astype(F32) + UL[side].astype(F32) + UR[side].astype(F32)
        )
    gt_in = push(GF.at[1 - c], GT, at(dc=1))
    gc_in.wait_recv()
    other = GC[...]
    loss_o[...] = jnp.broadcast_to(jnp.sum(heads[2]), (8, 128))
    for i in range(2):
        gh_o[:, lane(2 * i)] = jnp.where(c == 0, heads[i], other[i])
        gh_o[:, lane(2 * i + 1)] = jnp.where(c == 0, other[i], heads[i])
    reduce_c(0, 0, g2_o)
    reduce_c(0, 1, g2_o)
    edge_end()
    link.all_of(XL.at[pl.ds(0, 2)], z_sem).wait_recv()
    for side, half in ((0, LOW), (1, HIGH)):
        g2_o[half, :] = g2_o[half, :] + ZL[side].astype(F32) + ZR[side].astype(F32)
    gt_in.wait_recv()
    kept, brought = GF[c], GT[...]
    g1_o[:, pl.ds(0, 512)] = jnp.where(c == 0, kept, brought)
    g1_o[:, pl.ds(512, 512)] = jnp.where(c == 0, brought, kept)

    link.drain()

    @pl.when(c == 0)
    def _():
        for copy in re_to:
            copy.wait_send()

    @pl.when(r < 4)
    def _():
        for copy in v_out:
            copy.wait_send()


SCRATCH = [
    ((2, 384, 512), BF16), ((512, 768), BF16), ((4, 4, 2, 16, 512), BF16),
    ((4, 1024, 512), BF16), ((8, 8, 512), F32), ((8, 2048), BF16), ((3, 2, 4, 8, 128), F32),
    ((768, 1024), BF16), ((1024, 768), BF16), ((768, 512), F32), ((8, 96, 2048), BF16),
    ((4, 96, 512), BF16), ((4, 96, 512), BF16), ((4, 2, 96, 512), BF16),
    ((4, 2, 96, 512), BF16), ((4, 96, 512), BF16), ((96, 2048), F32), ((96, 2048), F32),
    ((96, 2048), BF16), ((24, 8, 128), F32), ((12, 8, 128), F32), ((8, 96, 2048), BF16),
    ((768, 1024), F32), ((4, 1024, 512), BF16), ((4, HALF, 128), BF16), ((4, HALF, 128), BF16),
    ((4, 2, HALF, 128), BF16), ((4, 2, HALF, 128), BF16), ((HALF, 128), BF16),
    ((HALF, 128), BF16), ((2, HALF, 128), BF16), ((2, HALF, 128), BF16), ((768, 512), BF16),
    ((768, 512), BF16), ((768, 512), BF16), ((4, 4, 32, 512), BF16), ((4, 16, 512), BF16),
    ((4, 16, 512), BF16), ((2, 4, 16, 512), BF16), ((2, 4, 16, 512), BF16), ((16, 512), BF16),
    ((16, 512), BF16), ((2, 16, 512), BF16), ((2, 16, 512), BF16), ((2, 16, 512), F32),
    ((16, 512), F32), ((8, 3, 8, 128), F32), ((8, 3, 8, 128), F32), ((3, 8, 128), F32),
    ((3, 3, 8, 128), F32), ((3, 3, 8, 128), F32), ((3, 8, 128), F32), ((3, 8, 128), F32),
    ((3, 8, 128), F32), ((8, 512), BF16), ((8, 384), F32), ((1, 384), jnp.int32),
    ((16, 1024), BF16),
    ((2, EDGE // 2, 512), BF16), ((2, EDGE // 2, 512), BF16), ((2, EDGE // 2, 512), BF16),
    ((2, EDGE // 2, 128), BF16), ((2, EDGE // 2, 128), BF16), ((2, EDGE // 2, 128), BF16),
]


def finish(adv, loss, g1, g2, gh, adv_o, loss_o, g1_o, g2_o, gh_o):
    adv_o[...] = jnp.concatenate([adv[i][:, :96] for i in range(4)], axis=1)
    loss_o[0, 0] = loss[0, 0] * (0.5 / 98304)
    g1_o[...] = g1[...]
    g2_o[...] = g2[...]
    gh_o[...] = gh[...]


def shards(features, w_first, w_second, w_head, rewards, discount, trace, episode):
    vmem = pl.BlockSpec(memory_space=pltpu.VMEM)
    smem = pl.BlockSpec(memory_space=pltpu.SMEM)
    hbm = pl.BlockSpec(memory_space=pltpu.HBM)
    shapes = ((16, 1024), (1024, 128), (8, 512))
    parts = pl.pallas_call(
        kernel,
        out_shape=[
            jax.ShapeDtypeStruct(shape, F32) for shape in ((4, 8, 128), (8, 128), *shapes)
        ],
        in_specs=[hbm] * 6 + [smem] * 2,
        out_specs=[vmem] * 5,
        scratch_shapes=[pltpu.VMEM(shape, kind) for shape, kind in SCRATCH]
        + [pltpu.SemaphoreType.DMA((count,)) for count in (RING + 18, SLOTS, 6)],
        compiler_params=pltpu.CompilerParams(
            collective_id=0, has_side_effects=True, vmem_limit_bytes=62 * 2**20
        ),
    )(
        features, w_first, w_second, w_head.T, rewards, episode,
        discount, trace,
    )
    advantages, loss, grad_first, grad_second, grad_head = pl.pallas_call(
        finish,
        out_shape=[
            jax.ShapeDtypeStruct(shape, F32) for shape in ((8, 384), (1, 1), *shapes)
        ],
        in_specs=[vmem, smem, vmem, vmem, vmem],
        out_specs=[vmem, smem, vmem, vmem, vmem],
    )(*parts)
    return advantages, loss[0, 0], grad_first, grad_second, grad_head.T


def solution(mesh):
    placed = (
        P("batch", None),
        P("batch", "hidden"),
        P("hidden", "batch"),
        P("hidden", None),
        P(None, "batch"),
        P(),
        P(),
        P("batch"),
    )
    return jax.shard_map(
        shards,
        mesh=mesh,
        in_specs=placed,
        out_specs=(
            P(None, "batch"),
            P(),
            P("batch", "hidden"),
            P("hidden", "batch"),
            P("hidden", None),
        ),
        check_vma=False,
    )
```

```python
import functools

import jax
import jax.numpy as jnp
from jax import lax
from jax.experimental import pallas as pl
from jax.experimental.pallas import tpu as pltpu
from jax.sharding import PartitionSpec as P

BF16, F32 = jnp.bfloat16, jnp.float32
MESH = pl.DeviceIdType.MESH
SLOTS, RING = 130, 32
EDGE = 192
HALF = (1024 - EDGE) // 2
LOW, HIGH = pl.ds(0, HALF), pl.ds(HALF, HALF)
TOP = pl.ds(2 * HALF, EDGE)
TOPS = (pl.ds(2 * HALF, EDGE // 2), pl.ds(2 * HALF + EDGE // 2, EDGE // 2))


def dot(left, right, dims=((1,), (0,))):
    return lax.dot_general(left, right, (dims, ((), ())), preferred_element_type=F32)


def mod(value, count):
    return lax.rem(value + count, count)


def lane(dx):
    return pl.ds(dx * 128, 128)


class Links:
    def __init__(self, sent, came):
        self.sent, self.came, self.used, self.open = sent, came, 0, []

    def take(self):
        self.used += 1
        return self.used - 1

    def make(self, src, dst, to, k, k_sent):
        return pltpu.make_async_remote_copy(
            src_ref=src,
            dst_ref=dst,
            send_sem=self.sent.at[k_sent],
            recv_sem=self.came.at[k],
            device_id=to,
            device_id_type=MESH,
        )

    def push(self, src, dst, to, land=None, k=None):
        k = self.take() if k is None else k
        turn = len(self.open)
        if turn >= RING:
            self.open[turn - RING].wait_send()
        copy = self.make(src, dst, to, k, turn % RING)
        copy.start()
        self.open.append(copy)
        return copy if land is None else self.make(land, land, to, k, 0)

    def all_of(self, ref, k):
        return self.make(ref, ref, self.peer, k, 0)

    def drain(self):
        for copy in self.open[-RING:]:
            copy.wait_send()


def kernel(
    feat, w1in, w2in, whin, reward_in, number_in, discount_in, trace_in,
    adv_o, loss_o, g1_o, g2_o, gh_o,
    F, FT, W1, W2, WHB, WH, RE, HF, HFT, SP, PS, RA, RB, RL, RR, RZ, PRE, SL2, H2,
    V, ADV, S, BACK, G2, XA, XB, XL, XR, ZA, ZB, ZL, ZR, BKS, BKR, SF,
    G1, YA, YB, YL, YR, UA, UB, UL, UR, GF, GT, GHP, GR, GS, GZ, GX, GY, GC, GH,
    WHS, RWS, EPS, WIN, EZF, EZL, EZR, EXF, EXL, EXR, sent, came, local,
):
    b, j = lax.axis_index("batch"), lax.axis_index("hidden")
    c, m = lax.rem(b, 2), lax.div(b, 2)
    zh, x = lax.rem(m, 4), lax.div(m, 4)
    y, zl = lax.rem(j, 4), lax.div(j, 4)
    r = y * 2 + zl
    link = Links(sent, came)
    push = link.push

    def at(dx=0, dz=0, dc=0, dy=0, dl=0):
        bb = (mod(x + dx, 4) * 4 + mod(zh + dz, 4)) * 2 + mod(c + dc, 2)
        return bb, mod(zl + dl, 2) * 4 + mod(y + dy, 4)

    def beside(step, dc, dy, dl):
        bb = mod(m + step, 16) * 2 + mod(c + dc, 2)
        return bb, mod(zl + dl, 2) * 4 + mod(y + dy, 4)

    link.peer = at(dc=1)
    peers = [(dc, dy, dl) for dc in range(2) for dy in range(4) for dl in range(2)]

    loads = [
        pltpu.make_async_copy(src, dst, local.at[k])
        for k, (src, dst) in enumerate(
            (
                (w1in, WIN),
                (w2in, W2.at[0, :, lane(0)]),
                (feat, F.at[c]),
                (whin, WHS),
                (reward_in, RWS),
                (number_in, EPS.at[0]),
            )
        )
    ]
    for load in loads:
        load.start()

    barrier = pltpu.get_barrier_semaphore()
    partners = [at(dc=dc, dy=dy, dl=dl) for dc, dy, dl in peers[1:]]
    partners += [at(dx=d) for d in (1, 2, 3)] + [at(dz=d) for d in (1, 2, 3)]
    partners += [beside(step, *peer) for step in (1, -1) for peer in peers]
    for partner in partners:
        pl.semaphore_signal(barrier, inc=1, device_id=partner, device_id_type=MESH)
    for load in loads[:3]:
        load.wait()
    pl.semaphore_wait(barrier, len(partners))

    mine, theirs = (
        pl.ds(pl.multiple_of(side * 512, 512), 512) for side in (c, 1 - c)
    )
    w1_sem = link.take()
    w1pair = push(WIN.at[:, theirs], W1.at[x, zh, c], at(dc=1), W1.at[x, zh, 1 - c])
    W1[x, zh, c] = WIN[:, mine]

    def w1_sides(zs):
        own = W1.at[x, zs]
        return [push(own, own, at(dx=dx), W1.at[mod(x - dx, 4), zs]) for dx in (1, 3)]

    def w1_across(zs, sides):
        out = []
        for dx, side in ((1, 0), (3, 1)):
            sides[side].wait_recv()
            part = W1.at[mod(x - dx, 4), zs, side]
            out.append(push(part, part, at(dx=dx), k=w1_sem))
        return out

    w2x = {}

    def w2_to(dz, half, dx):
        key = (dz, 4 - dx, 0 if half is LOW else 1)
        w2x[key] = push(
            W2.at[dz, half, lane(0)], W2.at[dz, half, lane(4 - dx)], at(dx=dx)
        )

    def w2_side(dz, half):
        near = 1 if half is LOW else 3
        w2_to(dz, half, near)
        w2_to(dz, half, 4 - near)

    def w2_across(dz):
        w2x[dz, 3, 0].wait_recv()
        w2x[dz, 2, 0] = push(
            W2.at[dz, LOW, lane(3)], W2.at[dz, LOW, lane(2)], at(dx=1)
        )
        w2x[dz, 1, 1].wait_recv()
        w2x[dz, 2, 1] = push(
            W2.at[dz, HIGH, lane(1)], W2.at[dz, HIGH, lane(2)], at(dx=3)
        )

    def w2_rest(dz, keys=((3, 1), (1, 0), (2, 0), (2, 1))):
        for key in keys:
            w2x[(dz, *key)].wait_recv()

    def w2_z(half, dz):
        return push(W2.at[0, half, lane(0)], W2.at[4 - dz, half, lane(0)], at(dz=dz))

    first, second, w1z, w1x, w1far = [], [], {}, {}, {}

    def w1_start():
        w1pair.wait_recv()
        own = W1.at[x, zh]
        for dz in (1, 3, 2):
            w1z[dz] = push(own, own, at(dz=dz), W1.at[x, mod(zh - dz, 4)])
        w1x[0] = w1_sides(zh)

    def w1_from_z(dz):
        w1z[dz].wait_recv()
        w1x[dz] = w1_sides(mod(zh - dz, 4))

    def w1_far(dz):
        w1far[dz] = w1_across(mod(zh - dz, 4), w1x[dz])

    def w1_done():
        link.all_of(W1.at[0], w1_sem).wait_recv()

    edge = {}

    def edge_x1():
        src = W2.at[0, TOP, lane(0)]
        edge["x3"] = push(src, W2.at[0, TOP, lane(3)], at(dx=1))
        edge["x1"] = push(src, W2.at[0, TOP, lane(1)], at(dx=3))

    def edge_x2():
        edge["x3"].wait_recv()
        src = W2.at[0, TOPS[0], lane(3)]
        edge["x2"] = [push(src, W2.at[0, TOPS[0], lane(2)], at(dx=1))]
        edge["x1"].wait_recv()
        src = W2.at[0, TOPS[1], lane(1)]
        edge["x2"].append(push(src, W2.at[0, TOPS[1], lane(2)], at(dx=3)))

    def edge_z1():
        for got in edge["x2"]:
            got.wait_recv()
        src = W2.at[0, TOP]
        edge["z3"] = push(src, W2.at[3, TOP], at(dz=1))
        edge["z1"] = push(src, W2.at[1, TOP], at(dz=3))

    edge["z2"] = []

    def edge_z2(dz):
        edge["z3" if dz == 3 else "z1"].wait_recv()
        half = TOPS[0 if dz == 3 else 1]
        edge["z2"].append(push(W2.at[dz, half], W2.at[2, half], at(dz=4 - dz)))

    w1_start()
    edge_x1()
    w2_to(0, LOW, 1)
    w2_to(0, HIGH, 3)
    first += [w2_z(LOW, 1), w2_z(HIGH, 3)]
    feat_in = push(F.at[c], F.at[c], at(dc=1), F.at[1 - c])
    w1_from_z(1)
    w2_to(0, HIGH, 1)
    w2_to(0, LOW, 3)
    w1_from_z(3)
    w1_far(0)
    edge_x2()
    w1_from_z(2)
    second += [w2_z(HIGH, 1), w2_z(LOW, 3)]
    for load in loads[3:]:
        load.wait()
    blank = jnp.zeros((8, 32), F32)
    WHB[j] = WHS[...].astype(F32)
    for i in range(4):
        reward = RWS[:, i * 96 : (i + 1) * 96]
        number = jnp.broadcast_to(EPS[:, i * 96 : (i + 1) * 96].astype(F32), (8, 96))
        RE[c, 0, i] = jnp.concatenate([reward, blank], axis=1)
        RE[c, 1, i] = jnp.concatenate([number, blank], axis=1)
    re_in = push(RE.at[c], RE.at[c], at(dc=1), RE.at[1 - c])
    re_sem = link.take()
    re_to = [
        link.make(RE.at[c], RE.at[2], beside(-1, dc, 0, 0), re_sem, RING + dc)
        for dc in range(2)
    ]

    @pl.when(c == 0)
    def _():
        for copy in re_to:
            copy.start()

    wh_sem = link.take()
    for dc, dy, dl in peers[1:8]:
        push(WHB.at[j], WHB.at[j], at(dy=dy, dl=dl), k=wh_sem)
    wh_all = WHB.at[pl.ds(0, 7)]
    wh_in = [link.make(wh_all, wh_all, at(dc=1), wh_sem, 0)]

    w1_far(1)
    edge_z1()
    w1_far(3)
    w1_far(2)
    w2_across(0)
    w2_z2 = []

    def w2_first():
        first[0].wait_recv()
        w2_z2.append(push(W2.at[3, LOW, lane(0)], W2.at[2, LOW, lane(0)], at(dz=1)))
        w2_side(3, LOW)
        first[1].wait_recv()
        w2_z2.append(push(W2.at[1, HIGH, lane(0)], W2.at[2, HIGH, lane(0)], at(dz=3)))
        w2_side(1, HIGH)

    def w2_second():
        second[0].wait_recv()
        w2_side(3, HIGH)
        second[1].wait_recv()
        w2_side(1, LOW)

    def w2_third():
        w2_z2[0].wait_recv()
        w2_side(2, LOW)
        w2_z2[1].wait_recv()
        w2_side(2, HIGH)

    w2_first()
    feat_in.wait_recv()
    w1_done()
    hf_in = []

    def layer_one():
        for n in range(2):
            cols = pl.ds(n * 256, 256)
            into = pl.ds(pl.multiple_of(c * 512 + n * 256, 256), 256)
            there = pl.ds(pl.multiple_of((1 - c) * 512 + n * 256, 256), 256)
            weights = W1[:, :, :, :, cols].reshape(512, 256)
            SP[:, cols] = dot(F[...].reshape(768, 512), weights)

            @pl.loop(0, 12)
            def _(i):
                rows = pl.ds(pl.multiple_of(i * 64, 64), 64)
                value = SP[rows, cols]
                gate = 1.0 / (1.0 + jnp.exp(-value))
                HF[rows, into] = (value * gate).astype(BF16)
                SP[rows, cols] = gate * (1.0 + value * (1.0 - gate))

            src = HF.at[:, into]
            hf_in.append(push(src, src, at(dc=1), HF.at[:, there]))

    layer_one()
    w2_second()

    def product(dz, part=None):
        for n in range(2) if part is None else (part,):
            out = dot(HF[...], W2[dz, :, pl.ds(n * 256, 256)])
            into = pl.ds(dz * 512 + n * 256, 256)
            PS[:, :, into] = out.astype(BF16).reshape(8, 96, 256)

    up, down, over = mod(y + 1, 4), mod(y - 1, 4), mod(y + 2, 4)
    came_rs = {}

    def lanes(dz, part):
        if part is None:
            return pl.ds(dz * 512, 512), pl.ds(0, 512)
        return pl.ds(dz * 512 + part * 256, 256), pl.ds(part * 256, 256)

    def scatter_a(dz, part=None):
        wide, here = lanes(dz, part)
        k = link.take()
        came_rs[dz, part] = [
            push(PS.at[over * 2, :, wide], RA.at[dz, :, here], at(dy=1)),
            push(PS.at[over * 2 + 1, :, wide], RB.at[dz, :, here], at(dy=3)),
            link.all_of(PS.at[pl.ds(0, 4), :, wide], k),
            k,
        ]
        push(PS.at[up * 2 + 1, :, wide], RL.at[dz, 1, :, here], at(dy=1), k=k)
        push(PS.at[down * 2, :, wide], RR.at[dz, 0, :, here], at(dy=3), k=k)

    def scatter_b(dz, part=None):
        wide, here = lanes(dz, part)
        for got, buf, row, dst, dy in (
            (came_rs[dz, part][0], RA, up * 2, RL.at[dz, 0, :, here], 1),
            (came_rs[dz, part][1], RB, down * 2 + 1, RR.at[dz, 1, :, here], 3),
        ):
            got.wait_recv()
            total = PS[row, :, wide].astype(F32) + buf[dz, :, here].astype(F32)
            PS[row, :, wide] = total.astype(BF16)
            push(PS.at[row, :, wide], dst, at(dy=dy), k=came_rs[dz, part][3])

    def scatter_c(dz, part=None):
        wide, here = lanes(dz, part)
        came_rs[dz, part][2].wait_recv()

        def total(side):
            return (
                PS[y * 2 + side, :, wide].astype(F32)
                + RL[dz, side, :, here].astype(F32)
                + RR[dz, side, :, here].astype(F32)
            )

        PS[y * 2 + 1 - zl, :, wide] = total(1 - zl).astype(BF16)
        came_rs[dz, part].append(
            push(PS.at[y * 2 + 1 - zl, :, wide], RZ.at[dz, :, here], at(dl=1))
        )
        PRE[:, wide] = total(zl)

    def scatter_d(dz, part=None):
        wide, here = lanes(dz, part)
        came_rs[dz, part][-1].wait_recv()

        @pl.loop(0, 3)
        def _(i):
            rows = pl.ds(pl.multiple_of(i * 32, 32), 32)
            value = PRE[rows, wide] + RZ[dz, rows, here].astype(F32)
            gate = 1.0 / (1.0 + jnp.exp(-value))
            H2[rows, wide] = (value * gate).astype(BF16)
            SL2[rows, wide] = gate * (1.0 + value * (1.0 - gate))

    for got in hf_in:
        got.wait_recv()
    w2_rest(0)
    product(0)
    scatter_a(0)
    w2_across(3)
    w2_across(1)
    scatter_b(0)
    edge_z2(3)
    w2_rest(3)
    product(3)
    scatter_a(3)
    w2_third()
    edge_z2(1)
    w2_rest(1)
    product(1)
    scatter_a(1)
    scatter_c(0)

    def transposes():
        @pl.loop(0, 4)
        def _(n):
            cols = pl.ds(pl.multiple_of(n * 256, 256), 256)
            HFT[cols, :] = HF[:, cols].astype(F32).T.astype(BF16)

        @pl.loop(0, 2)
        def _(n):
            cols = pl.ds(pl.multiple_of(n * 256, 256), 256)
            FT[cols, :] = F[:, :, cols].reshape(768, 256).astype(F32).T.astype(BF16)

    transposes()
    scatter_b(3)
    w2_across(2)
    for copy in wh_in:
        copy.wait_recv()
    for dz in range(4):
        for dx in range(4):
            mm = mod(x + dx, 4) * 4 + mod(zh + dz, 4)
            group, pair = lax.div(mm, 2), lax.rem(mm, 2)
            even, odd = (
                jnp.where(c == 0, WHB[group, :, lane(2 * p)], WHB[group, :, lane(2 * p + 1)])
                for p in (0, 1)
            )
            WH[:, lane(dz * 4 + dx)] = jnp.where(pair == 0, even, odd).astype(BF16)
    scatter_d(0)
    scatter_b(1)
    w2_rest(2, ((1, 0),))
    for got in edge["z2"]:
        got.wait_recv()
    product(2, 0)
    scatter_a(2, 0)
    w2_rest(2, ((3, 1), (2, 0), (2, 1)))
    product(2, 1)
    scatter_a(2, 1)
    scatter_c(3)
    scatter_c(1)
    scatter_d(3)
    scatter_b(2, 0)
    scatter_b(2, 1)
    scatter_d(1)
    scatter_c(2, 0)
    scatter_c(2, 1)
    scatter_d(2, 0)
    scatter_d(2, 1)

    own_values = dot(WH[...], H2[...], ((1,), (1,)))
    own_v = V.at[c * 12 + r]
    V[c * 12 + r] = jnp.concatenate([own_values, blank], axis=1)
    v_sem = link.take()
    for dc, dy, dl in peers[1:]:
        push(own_v, own_v, at(dc=dc, dy=dy, dl=dl), k=v_sem)
    v_out = [
        link.make(
            own_v, V.at[c * 12 + 8 + lax.rem(r, 4)], beside(-1, *peer), v_sem, RING + 2 + k
        )
        for k, peer in enumerate(peers)
    ]

    @pl.when(r < 4)
    def _():
        for copy in v_out:
            copy.start()

    re_in.wait_recv()
    link.make(RE.at[2], RE.at[2], at(dc=1), re_sem, 0).wait_recv()
    shape = (8, 12 * 128)
    place = lax.rem(lax.broadcasted_iota(jnp.int32, shape, 1), 128)

    def ahead(array, steps):
        return pltpu.roll(array, shape[1] - steps, 1)

    def following(array):
        return jnp.where(place == 95, ahead(array, 33), ahead(array, 1))

    def row_of(kind):
        return jnp.concatenate([RE[i // 4, kind, i % 4] for i in range(12)], axis=1)

    reward, number = row_of(0), row_of(1)
    head_row = lax.broadcasted_iota(jnp.int32, (8, 128), 0)

    def spread(array):
        out = jnp.zeros((8, 128), F32)
        for k in range(8):
            out = jnp.where(head_row == k, array[k], out)
        return out

    rate, decay = spread(discount_in), spread(trace_in)
    discount = jnp.concatenate([rate] * 12, axis=1)
    both = jnp.concatenate([rate * decay] * 12, axis=1)
    keep = jnp.where(following(number) == number, 1.0, 0.0)
    real = place < 96
    factor = jnp.where(real, both * keep, 1.0)
    scale = discount * keep

    v_all = V.at[pl.ds(0, 23)]
    v_in = [link.make(v_all, v_all, at(dc=1), v_sem, 0)]
    for copy in v_in:
        copy.wait_recv()
    value = jnp.concatenate([V[i] + V[12 + i] for i in range(12)], axis=1)
    total = jnp.where(real, reward + scale * following(value) - value, 0.0)
    step = 1
    while step < shape[1]:
        total = total + factor * ahead(total, step)
        factor = factor * ahead(factor, step)
        step *= 2
    for i in range(12):
        ADV[i] = total[:, i * 128 : (i + 1) * 128]

    own = ADV[r]
    slope_t = (-own[:, :96]).astype(BF16)
    slope = (-own).T[:96, :].astype(BF16)
    own_rows = S.at[r]

    def slope_chunk(dz):
        at_dz = pl.ds(dz * 512, 512)
        own_rows[:, at_dz] = (dot(slope, WH[:, at_dz]) * SL2[:, at_dz]).astype(BF16)

    ag = {}
    pair_r = y * 2 + 1 - zl

    def gather_a(dz, part=None):
        wide, _ = lanes(dz, part)
        src = S.at[r, :, wide]
        k, far = link.take(), link.take()
        pair = push(src, src, at(dl=1), S.at[pair_r, :, wide])
        push(src, src, at(dy=1), k=k)
        push(src, src, at(dy=3), k=k)
        ag[dz, part] = pair, k, far

    def gather_b(dz, part=None):
        wide, _ = lanes(dz, part)
        pair, k, _ = ag[dz, part]
        pair.wait_recv()
        src = S.at[pair_r, :, wide]
        push(src, src, at(dy=1), k=k)
        push(src, src, at(dy=3), k=k)

    def gather_c(dz, part=None):
        wide, _ = lanes(dz, part)
        _, k, far = ag[dz, part]
        link.all_of(S.at[pl.ds(0, 4), :, wide], k).wait_recv()
        low, high = S.at[down * 2, :, wide], S.at[up * 2 + 1, :, wide]
        push(low, low, at(dy=1), k=far)
        push(high, high, at(dy=3), k=far)

    def gather_d(dz, part=None):
        wide, _ = lanes(dz, part)
        link.all_of(S.at[pl.ds(0, 2), :, wide], ag[dz, part][2]).wait_recv()

    def grad_part(dz, part):
        wide, here = lanes(dz, part)

        @pl.loop(0, 2)
        def _(n):
            rows = pl.ds(pl.multiple_of(n * 512, 512), 512)
            G2[dz, rows, here] = dot(HFT[rows, :], S[:, :, wide].reshape(768, 256)).astype(BF16)

    def grad_second(dz, side):
        at_dz = pl.ds(dz * 512, 512)

        @pl.loop(0, 2)
        def _(n):
            size = (HALF if side == 0 else HALF + EDGE) // 2
            rows = pl.ds(pl.multiple_of(side * HALF + n * size, 16), size)
            G2[dz, rows, :] = dot(HFT[rows, :], S[:, :, at_dz].reshape(768, 512)).astype(BF16)

    def back_half(dz, side):
        at_dz = pl.ds(dz * 512, 512)

        @pl.loop(0, 2)
        def _(n):
            cols = pl.ds(pl.multiple_of(side * 512 + n * 256, 256), 256)
            part = dot(S[:, :, at_dz].reshape(768, 512), W2[dz, cols, :], ((1,), (1,)))
            BACK[:, cols] = BACK[:, cols] + part

    def back_first(dz, start):
        at_dz = pl.ds(dz * 512, 512)

        @pl.loop(0, 4)
        def _(n):
            cols = pl.ds(pl.multiple_of(n * 256, 256), 256)
            part = dot(S[:, :, at_dz].reshape(768, 512), W2[dz, cols, :], ((1,), (1,)))
            BACK[:, cols] = part if start else BACK[:, cols] + part

    gx, halves = {}, (LOW, HIGH)

    def reduce_far(dz, side):
        src = G2.at[dz, halves[side], lane(2)]
        gx[dz, side] = push(src, (XA, XB)[side].at[dz], at(dx=(1, 3)[side])), link.take()

    def reduce_near(dz, side):
        src = G2.at[dz, halves[side], lane((3, 1)[side])]
        push(src, (XR, XL)[side].at[dz, side], at(dx=(3, 1)[side]), k=gx[dz, side][1])

    def reduce_a(dz, side):
        reduce_far(dz, side)
        reduce_near(dz, side)

    def reduce_b(dz, side):
        gx[dz, side][0].wait_recv()
        dx, half = (1, 3)[side], halves[side]
        block = G2[dz, half, lane(dx)].astype(F32) + (XA, XB)[side][dz].astype(F32)
        G2[dz, half, lane(dx)] = block.astype(BF16)
        src = G2.at[dz, half, lane(dx)]
        push(src, (XL, XR)[side].at[dz, side], at(dx=dx), k=gx[dz, side][1])

    def reduce_c(dz, side, into=None):
        half = halves[side]
        link.all_of(XL.at[dz], gx[dz, side][1]).wait_recv()
        block = (
            G2[dz, half, lane(0)].astype(F32)
            + XL[dz, side].astype(F32)
            + XR[dz, side].astype(F32)
        )
        if into is None:
            G2[dz, half, lane(0)] = block.astype(BF16)
        else:
            into[half, :] = block

    e_far, e_x, e_sem, ex_sem = [], [], link.take(), link.take()

    def edge_far():
        for side in (0, 1):
            src = G2.at[2, TOPS[side], :]
            e_far.append(push(src, EZF.at[side], at(dz=(1, 3)[side])))

    def edge_near(dz):
        buf, near, side = (EZL, 1, 0) if dz == 1 else (EZR, 0, 1)
        push(G2.at[dz, TOPS[near], :], buf.at[near], at(dz=dz), k=e_sem)
        e_far[side].wait_recv()
        block = G2[dz, TOPS[side], :].astype(F32) + EZF[side].astype(F32)
        G2[dz, TOPS[side], :] = block.astype(BF16)
        push(G2.at[dz, TOPS[side], :], buf.at[side], at(dz=dz), k=e_sem)

    def edge_sum():
        link.all_of(G2.at[0, pl.ds(0, 2 * EDGE), :], e_sem).wait_recv()
        for side in (0, 1):
            block = (
                G2[0, TOPS[side], :].astype(F32)
                + EZL[side].astype(F32)
                + EZR[side].astype(F32)
            )
            G2[0, TOPS[side], :] = block.astype(BF16)
            src = G2.at[0, TOPS[side]]
            e_x.append(push(src.at[:, lane(2)], EXF.at[side], at(dx=(1, 3)[side])))
            near = (EXR, EXL)[side].at[side]
            push(src.at[:, lane((3, 1)[side])], near, at(dx=(3, 1)[side]), k=ex_sem)

    def edge_mid():
        for side in (0, 1):
            e_x[side].wait_recv()
            dx = (1, 3)[side]
            block = G2[0, TOPS[side], lane(dx)].astype(F32) + EXF[side].astype(F32)
            G2[0, TOPS[side], lane(dx)] = block.astype(BF16)
            src = G2.at[0, TOPS[side], lane(dx)]
            push(src, (EXL, EXR)[side].at[side], at(dx=dx), k=ex_sem)

    def edge_end():
        link.all_of(G2.at[0, pl.ds(0, 2 * EDGE), lane(0)], ex_sem).wait_recv()
        for side in (0, 1):
            g2_o[TOPS[side], :] = (
                G2[0, TOPS[side], lane(0)].astype(F32)
                + EXL[side].astype(F32)
                + EXR[side].astype(F32)
            )

    z_far, z_sem = [], link.take()

    def reduce_z(dz, side):
        half = halves[side]
        src = G2.at[dz, half, lane(0)]
        if dz == 2:
            z_far.append(push(src, (ZA, ZB)[side], at(dz=(1, 3)[side])))
            return
        if (dz, side) in ((1, 0), (3, 1)):
            z_far[side].wait_recv()
            block = G2[dz, half, lane(0)].astype(F32) + (ZA, ZB)[side][...].astype(F32)
            G2[dz, half, lane(0)] = block.astype(BF16)
        push(src, (ZL if dz == 1 else ZR).at[side], at(dz=dz), k=z_sem)

    slope_chunk(2)
    gather_a(2, 1)
    gather_a(2, 0)
    slope_chunk(1)
    slope_chunk(3)
    slope_chunk(0)
    gather_b(2, 1)
    gather_b(2, 0)
    gather_a(1)

    for i in range(4):
        adv_o[i] = ADV[4 * c + i]
    small = lax.broadcasted_iota(jnp.int32, (8, 128), 1) < 96
    own_loss = jnp.where(small, own * own, 0.0)
    head = dot(slope_t, H2[...])
    for dz in range(4):
        for dx in range(4):
            mm = mod(x + dx, 4) * 4 + mod(zh + dz, 4)
            GHP[lax.div(mm, 2), lax.rem(mm, 2)] = head[:, (dz * 4 + dx) * 128 :][:, :128]
    for g in range(8):
        GHP[g, 2] = own_loss
    gather_c(2, 1)
    gather_c(2, 0)
    gather_a(3)
    gather_b(1)
    gh_sem, gh_all = link.take(), GR.at[pl.ds(0, 7)]
    for dc, dy, dl in peers[1:8]:
        to_j = mod(zl + dl, 2) * 4 + mod(y + dy, 4)
        push(GHP.at[to_j], GR.at[j], at(dy=dy, dl=dl), k=gh_sem)
    gh_in = [link.make(gh_all, gh_all, at(dc=1), gh_sem, 0)]
    GR[j] = GHP[j]
    gather_d(2, 1)
    grad_part(2, 1)
    reduce_far(2, 0)
    reduce_far(2, 1)
    reduce_near(2, 0)
    gather_d(2, 0)
    grad_part(2, 0)
    reduce_near(2, 1)
    edge_far()
    gather_c(1)
    gather_b(3)
    gather_a(0)
    back_first(2, True)
    reduce_b(2, 0)
    reduce_b(2, 1)
    gather_b(0)
    gather_d(1)
    grad_second(1, 1)
    reduce_a(1, 1)
    grad_second(1, 0)
    reduce_a(1, 0)
    gather_c(3)
    back_first(1, False)
    for got in gh_in:
        got.wait_recv()
    GS[...] = functools.reduce(jnp.add, [GR[i] for i in range(8)])
    gz_sem, gx_sem = link.take(), link.take()
    for d in (1, 2, 3):
        push(GS, GZ.at[d - 1], at(dz=d), k=gz_sem)
    gz_in = [link.make(GZ, GZ, at(dz=1), gz_sem, 0)]
    edge_near(1)
    gather_c(0)
    reduce_b(1, 1)
    gather_d(3)
    grad_second(3, 0)
    reduce_a(3, 0)
    grad_second(3, 1)
    reduce_a(3, 1)
    edge_near(3)
    reduce_b(1, 0)
    reduce_c(2, 0)
    reduce_z(2, 0)
    reduce_c(2, 1)
    reduce_z(2, 1)
    back_first(3, False)
    gather_d(0)
    back_half(0, 1 - c)

    @pl.loop(0, 12)
    def _(i):
        rows = pl.ds(pl.multiple_of(i * 64, 64), 64)
        BKS[rows, :] = BACK[rows, theirs].astype(BF16)

    back_in = push(BKS, BKR, at(dc=1))
    back_half(0, c)
    reduce_b(3, 0)
    grad_second(0, 0)
    back_in.wait_recv()

    @pl.loop(0, 12)
    def _(i):
        rows = pl.ds(pl.multiple_of(i * 64, 64), 64)
        back = BACK[rows, mine] + BKR[rows, :].astype(F32)
        SF[rows, :] = (back * SP[rows, :]).astype(BF16)

    @pl.loop(0, 2)
    def _(n):
        rows = pl.ds(pl.multiple_of(n * 256, 256), 256)
        part = dot(FT[rows, :], SF[...]).astype(BF16)
        G1[pl.ds(2 * n, 2)] = part.reshape(2, 4, 32, 512)

    lo, hi = pl.ds(0, 16), pl.ds(16, 16)
    x1, x3, x2 = mod(x + 1, 4), mod(x - 1, 4), mod(x + 2, 4)
    z1, z3, z2 = mod(zh + 1, 4), mod(zh - 1, 4), mod(zh + 2, 4)
    yin = [
        push(G1.at[x2, :, lo], YA, at(dx=1)),
        push(G1.at[x2, :, hi], YB, at(dx=3)),
    ]
    y_sem, u_sem = link.take(), link.take()
    push(G1.at[x1, :, hi], YL.at[1], at(dx=1), k=y_sem)
    push(G1.at[x3, :, lo], YR.at[0], at(dx=3), k=y_sem)
    reduce_b(3, 1)
    grad_second(0, 1)
    for got in gz_in:
        got.wait_recv()
    GY[...] = GS[...] + GZ[0] + GZ[1] + GZ[2]
    for d in (1, 2, 3):
        push(GY, GX.at[d - 1], at(dx=d), k=gx_sem)
    gxs_in = [link.make(GX, GX, at(dx=1), gx_sem, 0)]
    reduce_c(1, 1)
    reduce_z(1, 1)
    reduce_c(1, 0)
    reduce_z(1, 0)
    reduce_c(3, 0)
    reduce_z(3, 0)

    def sums_y():
        for got, buf, row, half, dst, dx in (
            (yin[0], YA, x1, lo, YL.at[0], 1),
            (yin[1], YB, x3, hi, YR.at[1], 3),
        ):
            got.wait_recv()
            block = G1[row, :, half].astype(F32) + buf[...].astype(F32)
            G1[row, :, half] = block.astype(BF16)
            push(G1.at[row, :, half], dst, at(dx=dx), k=y_sem)

    sums_y()
    reduce_a(0, 0)
    reduce_a(0, 1)
    edge_sum()
    for got in gxs_in:
        got.wait_recv()
    heads = GY[...] + GX[0] + GX[1] + GX[2]
    GH[...] = heads
    gc_in = push(GH, GC, at(dc=1))
    reduce_c(3, 1)
    reduce_z(3, 1)
    link.all_of(G1.at[pl.ds(0, 2)], y_sem).wait_recv()
    for side, half in ((0, lo), (1, hi)):
        block = G1[x, :, half].astype(F32) + YL[side].astype(F32) + YR[side].astype(F32)
        G1[x, :, half] = block.astype(BF16)
    uin = [
        push(G1.at[x, z2, lo], UA, at(dz=1)),
        push(G1.at[x, z2, hi], UB, at(dz=3)),
    ]
    push(G1.at[x, z1, hi], UL.at[1], at(dz=1), k=u_sem)
    push(G1.at[x, z3, lo], UR.at[0], at(dz=3), k=u_sem)
    reduce_b(0, 0)
    reduce_b(0, 1)
    edge_mid()
    for got, buf, row, half, dst, dz in (
        (uin[0], UA, z1, lo, UL.at[0], 1),
        (uin[1], UB, z3, hi, UR.at[1], 3),
    ):
        got.wait_recv()
        block = G1[x, row, half].astype(F32) + buf[...].astype(F32)
        G1[x, row, half] = block.astype(BF16)
        push(G1.at[x, row, half], dst, at(dz=dz), k=u_sem)
    link.all_of(G1.at[0, pl.ds(0, 2)], u_sem).wait_recv()
    for side, half in ((0, lo), (1, hi)):
        GF[side] = (
            G1[x, zh, half].astype(F32) + UL[side].astype(F32) + UR[side].astype(F32)
        )
    gt_in = push(GF.at[1 - c], GT, at(dc=1))
    gc_in.wait_recv()
    other = GC[...]
    loss_o[...] = jnp.broadcast_to(jnp.sum(heads[2]), (8, 128))
    for i in range(2):
        gh_o[:, lane(2 * i)] = jnp.where(c == 0, heads[i], other[i])
        gh_o[:, lane(2 * i + 1)] = jnp.where(c == 0, other[i], heads[i])
    reduce_c(0, 0, g2_o)
    reduce_c(0, 1, g2_o)
    edge_end()
    link.all_of(XL.at[pl.ds(0, 2)], z_sem).wait_recv()
    for side, half in ((0, LOW), (1, HIGH)):
        g2_o[half, :] = g2_o[half, :] + ZL[side].astype(F32) + ZR[side].astype(F32)
    gt_in.wait_recv()
    kept, brought = GF[c], GT[...]
    g1_o[:, pl.ds(0, 512)] = jnp.where(c == 0, kept, brought)
    g1_o[:, pl.ds(512, 512)] = jnp.where(c == 0, brought, kept)

    link.drain()

    @pl.when(c == 0)
    def _():
        for copy in re_to:
            copy.wait_send()

    @pl.when(r < 4)
    def _():
        for copy in v_out:
            copy.wait_send()


SCRATCH = [
    ((2, 384, 512), BF16), ((512, 768), BF16), ((4, 4, 2, 16, 512), BF16),
    ((4, 1024, 512), BF16), ((8, 8, 512), F32), ((8, 2048), BF16), ((3, 2, 4, 8, 128), F32),
    ((768, 1024), BF16), ((1024, 768), BF16), ((768, 512), F32), ((8, 96, 2048), BF16),
    ((4, 96, 512), BF16), ((4, 96, 512), BF16), ((4, 2, 96, 512), BF16),
    ((4, 2, 96, 512), BF16), ((4, 96, 512), BF16), ((96, 2048), F32), ((96, 2048), F32),
    ((96, 2048), BF16), ((24, 8, 128), F32), ((12, 8, 128), F32), ((8, 96, 2048), BF16),
    ((768, 1024), F32), ((4, 1024, 512), BF16), ((4, HALF, 128), BF16), ((4, HALF, 128), BF16),
    ((4, 2, HALF, 128), BF16), ((4, 2, HALF, 128), BF16), ((HALF, 128), BF16),
    ((HALF, 128), BF16), ((2, HALF, 128), BF16), ((2, HALF, 128), BF16), ((768, 512), BF16),
    ((768, 512), BF16), ((768, 512), BF16), ((4, 4, 32, 512), BF16), ((4, 16, 512), BF16),
    ((4, 16, 512), BF16), ((2, 4, 16, 512), BF16), ((2, 4, 16, 512), BF16), ((16, 512), BF16),
    ((16, 512), BF16), ((2, 16, 512), BF16), ((2, 16, 512), BF16), ((2, 16, 512), F32),
    ((16, 512), F32), ((8, 3, 8, 128), F32), ((8, 3, 8, 128), F32), ((3, 8, 128), F32),
    ((3, 3, 8, 128), F32), ((3, 3, 8, 128), F32), ((3, 8, 128), F32), ((3, 8, 128), F32),
    ((3, 8, 128), F32), ((8, 512), BF16), ((8, 384), F32), ((1, 384), jnp.int32),
    ((16, 1024), BF16),
    ((2, EDGE // 2, 512), BF16), ((2, EDGE // 2, 512), BF16), ((2, EDGE // 2, 512), BF16),
    ((2, EDGE // 2, 128), BF16), ((2, EDGE // 2, 128), BF16), ((2, EDGE // 2, 128), BF16),
]


def finish(adv, loss, g1, g2, gh, adv_o, loss_o, g1_o, g2_o, gh_o):
    adv_o[...] = jnp.concatenate([adv[i][:, :96] for i in range(4)], axis=1)
    loss_o[0, 0] = loss[0, 0] * (0.5 / 98304)
    g1_o[...] = g1[...]
    g2_o[...] = g2[...]
    gh_o[...] = gh[...]


def shards(features, w_first, w_second, w_head, rewards, discount, trace, episode):
    vmem = pl.BlockSpec(memory_space=pltpu.VMEM)
    smem = pl.BlockSpec(memory_space=pltpu.SMEM)
    hbm = pl.BlockSpec(memory_space=pltpu.HBM)
    shapes = ((16, 1024), (1024, 128), (8, 512))
    parts = pl.pallas_call(
        kernel,
        out_shape=[
            jax.ShapeDtypeStruct(shape, F32) for shape in ((4, 8, 128), (8, 128), *shapes)
        ],
        in_specs=[hbm] * 6 + [smem] * 2,
        out_specs=[vmem] * 5,
        scratch_shapes=[pltpu.VMEM(shape, kind) for shape, kind in SCRATCH]
        + [pltpu.SemaphoreType.DMA((count,)) for count in (RING + 18, SLOTS, 6)],
        compiler_params=pltpu.CompilerParams(
            collective_id=0, has_side_effects=True, vmem_limit_bytes=62 * 2**20
        ),
    )(
        features, w_first, w_second, w_head.T, rewards, episode,
        discount, trace,
    )
    advantages, loss, grad_first, grad_second, grad_head = pl.pallas_call(
        finish,
        out_shape=[
            jax.ShapeDtypeStruct(shape, F32) for shape in ((8, 384), (1, 1), *shapes)
        ],
        in_specs=[vmem, smem, vmem, vmem, vmem],
        out_specs=[vmem, smem, vmem, vmem, vmem],
    )(*parts)
    return advantages, loss[0, 0], grad_first, grad_second, grad_head.T


def solution(mesh):
    placed = (
        P("batch", None),
        P("batch", "hidden"),
        P("hidden", "batch"),
        P("hidden", None),
        P(None, "batch"),
        P(),
        P(),
        P("batch"),
    )
    return jax.shard_map(
        shards,
        mesh=mesh,
        in_specs=placed,
        out_specs=(
            P(None, "batch"),
            P(),
            P("batch", "hidden"),
            P("hidden", "batch"),
            P("hidden", None),
        ),
        check_vma=False,
    )
```
